16 devices in a mesh: dp: 2 (over z), ep: 8 (over y, x, core).
Axes of the slice: x: 2, y: 2, z: 2, core: 2. Of those that a mesh axis runs over, the one named last changes fastest.
Arguments:
- x: bfloat16 [32768, 768], P(('dp', 'ep'))
- gy: bfloat16 [32768, 768], P(('dp', 'ep'))
- idx: int32 [32768], P(('dp', 'ep'))
- w_gate: bfloat16 [768, 32], replicated
- w_up: bfloat16 [32, 768, 3072], P('ep')
- w_down: bfloat16 [32, 3072, 768], P('ep')
Outputs:
- output 1: bfloat16 [32768, 768], P(('dp', 'ep'))
- output 2: bfloat16 [32768, 768], P(('dp', 'ep'))
- output 3: float32 [32, 768, 3072], P('ep')
- output 4: float32 [32, 3072, 768], P('ep')
- output 5: float32 [768, 32], replicated
All inputs are finite; a program needn't handle non-finite values.
Results may differ from the reference program's by a relative error of at most 0.00656847.
Values are sent between devices in bfloat16 or wider.
A program may use at most 1 GiB of HBM per device.

```python
import functools
import jax
import jax.numpy as jnp
from jax import lax

D_MODEL = 768
D_FF = 3072
N_EXPERTS = 32
TOKENS_DEV = 2048
N_DEVICES = 16
TILE_ROWS = 128
N_TOKENS = N_DEVICES * TOKENS_DEV
CAP_ROWS = 4 * TOKENS_DEV // N_EXPERTS
N_TILES = N_TOKENS // TILE_ROWS + N_EXPERTS


def count_profile():
    hot_experts = max(1, N_EXPERTS // 16)
    cold_experts = N_EXPERTS - hot_experts
    rest_rows = TOKENS_DEV - hot_experts * CAP_ROWS
    base_rows = rest_rows // cold_experts
    extra_rows = rest_rows % cold_experts
    return [CAP_ROWS] * hot_experts + [base_rows + 1] * extra_rows + [base_rows] * (cold_experts - extra_rows)


def draw_routing(route_key):
    profile = count_profile()
    rank_table = jnp.array([rank_id for rank_id in range(N_EXPERTS) for copy_num in range(profile[rank_id])], jnp.int32)

    def one_device(dev_key):
        perm_key, shuffle_key = jax.random.split(dev_key)
        expert_perm = jax.random.permutation(perm_key, N_EXPERTS).astype(jnp.int32)
        return jax.random.permutation(shuffle_key, expert_perm[rank_table])

    return jax.vmap(one_device)(jax.random.split(route_key, N_DEVICES)).reshape(N_TOKENS)


def setup_inputs(seed: int = 0) -> dict:
    root_key = jax.random.key(seed)
    k_x, k_gy, k_gate, k_up, k_down, k_route = jax.random.split(root_key, 6)
    x = jax.random.normal(k_x, (N_TOKENS, D_MODEL), jnp.float32).astype(jnp.bfloat16)
    gy = jax.random.normal(k_gy, (N_TOKENS, D_MODEL), jnp.float32).astype(jnp.bfloat16)
    w_gate = (jax.random.normal(k_gate, (D_MODEL, N_EXPERTS), jnp.float32) * D_MODEL ** -0.5).astype(jnp.bfloat16)
    w_up = (jax.random.normal(k_up, (N_EXPERTS, D_MODEL, D_FF), jnp.float32) * D_MODEL ** -0.5).astype(jnp.bfloat16)
    w_down = (jax.random.normal(k_down, (N_EXPERTS, D_FF, D_MODEL), jnp.float32) * D_FF ** -0.5).astype(jnp.bfloat16)
    idx = draw_routing(k_route)
    return {'x': x, 'gy': gy, 'idx': idx, 'w_gate': w_gate, 'w_up': w_up, 'w_down': w_down}


def tile_pass(w_up, w_down, grad_carry, tile_in):
    grad_up, grad_down = grad_carry
    tok_rows, d_out, expert = tile_in
    up_mat = w_up[expert]
    down_mat = w_down[expert]
    pre_act = jnp.dot(tok_rows, up_mat, preferred_element_type=jnp.float32)
    hid_full, gelu_back = jax.vjp(jax.nn.gelu, pre_act)
    hidden = hid_full.astype(jnp.bfloat16)
    y_rows = jnp.dot(hidden, down_mat, preferred_element_type=jnp.float32).astype(jnp.bfloat16)
    d_hidden = jnp.dot(d_out, down_mat.T, preferred_element_type=jnp.float32)
    d_pre = gelu_back(d_hidden)[0].astype(jnp.bfloat16)
    grad_down = grad_down.at[expert].add(jnp.dot(hidden.T, d_out, preferred_element_type=jnp.float32))
    grad_up = grad_up.at[expert].add(jnp.dot(tok_rows.T, d_pre, preferred_element_type=jnp.float32))
    d_rows = jnp.dot(d_pre, up_mat.T, preferred_element_type=jnp.float32).astype(jnp.bfloat16)
    return (grad_up, grad_down), (y_rows, d_rows)


def reference(x, gy, idx, w_gate, w_up, w_down):
    onehot = idx[:, None] == jnp.arange(N_EXPERTS, dtype=jnp.int32)[None, :]
    router_logit = jnp.dot(x, w_gate, preferred_element_type=jnp.float32)
    router_prob = jax.nn.softmax(router_logit, axis=-1)
    gate_val = N_EXPERTS * jnp.sum(jnp.where(onehot, router_prob, 0.0), axis=1)
    expert_count = jnp.sum(onehot, axis=0, dtype=jnp.int32)
    sort_order = jnp.argsort(idx, stable=True)
    sorted_pos = jnp.argsort(sort_order)
    expert_start = jnp.cumsum(expert_count) - expert_count
    tile_count = (expert_count + TILE_ROWS - 1) // TILE_ROWS * TILE_ROWS
    tile_end = jnp.cumsum(tile_count)
    tile_start = tile_end - tile_count
    row_pos = tile_start[idx] + sorted_pos - expert_start[idx]
    tile_first = jnp.arange(N_TILES, dtype=jnp.int32) * TILE_ROWS
    tile_expert = jnp.minimum(jnp.sum(tile_end[None, :] <= tile_first[:, None], axis=1, dtype=jnp.int32), N_EXPERTS - 1)
    gy_full = gy.astype(jnp.float32)
    dy_tok = (gate_val[:, None] * gy_full).astype(jnp.bfloat16)
    rows_buf = jnp.zeros((N_TILES * TILE_ROWS, D_MODEL), x.dtype).at[row_pos].set(x)
    dy_buf = jnp.zeros((N_TILES * TILE_ROWS, D_MODEL), dy_tok.dtype).at[row_pos].set(dy_tok)
    grad_init = (jnp.zeros((N_EXPERTS, D_MODEL, D_FF), jnp.float32), jnp.zeros((N_EXPERTS, D_FF, D_MODEL), jnp.float32))
    tiles_in = (rows_buf.reshape(N_TILES, TILE_ROWS, D_MODEL), dy_buf.reshape(N_TILES, TILE_ROWS, D_MODEL), tile_expert)
    grads, tile_out = lax.scan(functools.partial(tile_pass, w_up, w_down), grad_init, tiles_in)
    grad_up, grad_down = grads
    y_tok = tile_out[0].reshape(N_TILES * TILE_ROWS, D_MODEL)[row_pos]
    dx_expert = tile_out[1].reshape(N_TILES * TILE_ROWS, D_MODEL)[row_pos]
    moe_out = (gate_val[:, None] * y_tok.astype(jnp.float32)).astype(jnp.bfloat16)
    d_gate = jnp.sum(gy_full * y_tok.astype(jnp.float32), axis=1)
    d_logit = ((d_gate * gate_val)[:, None] * (onehot.astype(jnp.float32) - router_prob)).astype(jnp.bfloat16)
    dx_router = jnp.dot(d_logit, w_gate.T, preferred_element_type=jnp.float32)
    grad_x = (dx_expert.astype(jnp.float32) + dx_router).astype(jnp.bfloat16)
    grad_gate = jnp.dot(x.T, d_logit, preferred_element_type=jnp.float32)
    return (moe_out, grad_x, grad_up, grad_down, grad_gate)
```

```python
import jax
import jax.numpy as jnp
from jax import lax
from jax.experimental import pallas as pl
from jax.experimental.pallas import tpu as pltpu
from jax.sharding import PartitionSpec as P


PAD_FACTOR = 4
GROUP = 8
BASE_GROUPS = 7
OVER_GROUPS = 50
MAX_OVER_TILES = 8
TILE_GROUPS = 26
TILE = TILE_GROUPS * GROUP
PERM_TILE = 256
CHUNK = 512
ROW_CHUNK = 256
SQRT_2_PI = 0.7978845608028654
CUBIC = 0.044715
VMEM_BYTES = 67_043_328

F32 = jnp.float32
BF16 = jnp.bfloat16
I32 = jnp.int32


def dot(a, b, dims=((1,), (0,))):
    return lax.dot_general(a, b, (dims, ((), ())), preferred_element_type=F32)


def exclusive_cumsum(v, axis):
    return jnp.cumsum(v, axis=axis) - v


def token_positions(idx, n_experts):
    tok_count = idx.shape[0]
    block = 128
    base_rows = BASE_GROUPS * GROUP
    onehot = (idx[:, None] == jnp.arange(n_experts, dtype=I32)[None, :]).astype(BF16)
    blocks = onehot.reshape(tok_count // block, block, n_experts)
    lower = jnp.tril(jnp.ones((block, block), BF16))
    inclusive = jnp.einsum('ij,bje->bie', lower, blocks, preferred_element_type=F32)
    totals = jnp.sum(blocks.astype(F32), axis=1)
    counts = jnp.sum(totals, axis=0).astype(I32)
    groups = (counts + GROUP - 1) // GROUP
    over = jnp.maximum(groups - BASE_GROUPS, 0)
    over_start = exclusive_cumsum(over, 0)
    rank = inclusive + (exclusive_cumsum(totals, 0) - 1.0)[:, None, :]
    base_at = jnp.arange(n_experts, dtype=F32) * base_rows
    over_at = (n_experts * base_rows - base_rows + over_start * GROUP).astype(F32)
    row = jnp.sum(blocks.astype(F32) * (rank + jnp.where(rank < base_rows, base_at, over_at)), axis=2)
    return groups, row.reshape(tok_count).astype(I32)


def permute_kernel(pos_ref, x_ref, gy_ref, out_ref):
    rows, d_model = out_ref.shape[0], x_ref.shape[1]
    row_id = pl.program_id(0) * rows + lax.broadcasted_iota(I32, (rows, x_ref.shape[0]), 0)
    select = jnp.where(row_id == pos_ref[...], 1.0, 0.0).astype(BF16)
    out_ref[:, :d_model] = dot(select, x_ref[...]).astype(BF16)
    out_ref[:, d_model:] = dot(select, gy_ref[...]).astype(BF16)


def permute_rows(pos, x, gy, first_row, n_rows):
    tok_count, d_model = x.shape
    tile = n_rows if n_rows % PERM_TILE else PERM_TILE
    return pl.pallas_call(
        permute_kernel,
        grid=(n_rows // tile,),
        in_specs=[
            pl.BlockSpec((1, tok_count), lambda i: (0, 0)),
            pl.BlockSpec((tok_count, d_model), lambda i: (0, 0)),
            pl.BlockSpec((tok_count, d_model), lambda i: (0, 0)),
        ],
        out_specs=pl.BlockSpec((tile, 2 * d_model), lambda i: (i, 0)),
        out_shape=jax.ShapeDtypeStruct((n_rows, 2 * d_model), BF16),
        cost_estimate=pl.CostEstimate(flops=4 * n_rows * tok_count * d_model, bytes_accessed=16_000_000, transcendentals=0),
        name='permute',
    )((pos - first_row).reshape(1, tok_count), x, gy)


def unpermute_kernel(pos_ref, base_ref, over_ref, out_ref, dx_ref):
    toks, d_model = out_ref.shape
    n_base = base_ref.shape[0]
    base_id = lax.broadcasted_iota(I32, (toks, n_base), 1)
    over_id = lax.broadcasted_iota(I32, (toks, over_ref.shape[0]), 1) + n_base
    base = jnp.where(base_id == pos_ref[...], 1.0, 0.0).astype(BF16)
    over = jnp.where(over_id == pos_ref[...], 1.0, 0.0).astype(BF16)
    out_ref[...] = (dot(base, base_ref[:, :d_model]) + dot(over, over_ref[:, :d_model])).astype(BF16)
    dx_ref[...] = (dot(base, base_ref[:, d_model:]) + dot(over, over_ref[:, d_model:])).astype(BF16)


def unpermute_rows(pos, base, over):
    n_base, width = base.shape
    tok_count = pos.shape[0]
    d_model = width // 2
    shape = jax.ShapeDtypeStruct((tok_count, d_model), BF16)
    return pl.pallas_call(
        unpermute_kernel,
        grid=(tok_count // PERM_TILE,),
        in_specs=[
            pl.BlockSpec((PERM_TILE, 1), lambda i: (i, 0)),
            pl.BlockSpec(base.shape, lambda i: (0, 0)),
            pl.BlockSpec(over.shape, lambda i: (0, 0)),
        ],
        out_specs=[pl.BlockSpec((PERM_TILE, d_model), lambda i: (i, 0))] * 2,
        out_shape=[shape, shape],
        cost_estimate=pl.CostEstimate(flops=4 * n_base * tok_count * d_model, bytes_accessed=16_000_000, transcendentals=0),
        name='unpermute',
    )(pos.reshape(tok_count, 1), base, over)


def gate(x, wg, expert):
    logit = dot(x, wg)
    unnorm = jnp.exp(logit - jnp.max(logit, axis=1, keepdims=True))
    prob = unnorm / jnp.sum(unnorm, axis=1, keepdims=True)
    onehot = lax.broadcasted_iota(I32, prob.shape, 1) == expert
    gate_val = prob.shape[1] * jnp.sum(jnp.where(onehot, prob, 0.0), axis=1, keepdims=True)
    return prob, onehot, gate_val


def activations(x, dy, w_up, w_down, cols):
    a = dot(x, w_up[:, cols])
    dh = dot(dy, w_down[cols, :], ((1,), (1,)))
    cubic = (SQRT_2_PI * CUBIC) * (a * a)
    half = 0.5 + 0.5 * jnp.tanh(a * (SQRT_2_PI + cubic))
    h = a * half
    slope = half + (h - h * half) * (2.0 * SQRT_2_PI + 6.0 * cubic)
    return h.astype(BF16), (slope * dh).astype(BF16)


def own_rows_step(x, gy, expert, wg_ref, w_up, w_down, store, dwg_ref):
    dy_ref, h_ref, da_ref = store
    prob, onehot, gate_val = gate(x, wg_ref[...], expert)
    gy_full = gy.astype(F32)
    dy = (gate_val * gy_full).astype(BF16)
    dy_ref[...] = dy
    for lo in range(0, h_ref.shape[1], ROW_CHUNK):
        cols = pl.ds(lo, ROW_CHUNK)
        h, da = activations(x, dy, w_up, w_down, cols)
        h_ref[:, cols] = h
        da_ref[:, cols] = da
    y = dot(h_ref[...], w_down[...]).astype(BF16).astype(F32)
    dxe = dot(da_ref[...], w_up[...], ((1,), (1,))).astype(BF16).astype(F32)
    d_gate = jnp.sum(gy_full * y, axis=1, keepdims=True)
    d_logit = ((d_gate * gate_val) * (onehot.astype(F32) - prob)).astype(BF16)
    dwg_ref[...] += dot(x, d_logit, ((0,), (0,)))
    out = (gate_val * y).astype(BF16)
    dx = (dxe + dot(d_logit, wg_ref[...], ((1,), (1,)))).astype(BF16)
    return out, dx


def own_base_kernel(first_ref, rows_ref, wg_ref, up_ref, down_ref, od_ref, dy_ref, h_ref, da_ref, dwg_ref, zero_ref):
    expert = pl.program_id(0)
    d_model = wg_ref.shape[0]

    @pl.when(expert == 0)
    def _():
        dwg_ref[...] = jnp.zeros_like(dwg_ref)

    zero_ref[...] = jnp.zeros_like(zero_ref)
    rows = rows_ref[...].reshape(dy_ref.shape[0], 2 * d_model)
    out, dx = own_rows_step(rows[:, :d_model], rows[:, d_model:], first_ref[0] + expert, wg_ref,
                            up_ref.at[0], down_ref.at[0], (dy_ref, h_ref, da_ref), dwg_ref)
    block = od_ref.shape[:3] + (d_model,)
    od_ref[:, :, :, :d_model] = out.reshape(block)
    od_ref[:, :, :, d_model:] = dx.reshape(block)


def own_base_pass(first_expert, rows, wg, w_up, w_down, over_shape):
    n_src, local, seg, width = rows.shape
    d_model, d_ff = w_up.shape[1], w_up.shape[2]
    tile = n_src * seg
    row_spec = pl.BlockSpec((n_src, 1, seg, width), lambda e, first: (0, e, 0, 0))
    store_spec = lambda cols: pl.BlockSpec((tile, cols), lambda e, first: (e, 0))
    const = lambda e, first: (0, 0)
    rows_of = lambda cols: jax.ShapeDtypeStruct((local * tile, cols), BF16)
    zero_block = (over_shape[0] // local,) + over_shape[1:]
    return pl.pallas_call(
        own_base_kernel,
        grid_spec=pltpu.PrefetchScalarGridSpec(
            num_scalar_prefetch=1,
            grid=(local,),
            in_specs=[
                row_spec,
                pl.BlockSpec(wg.shape, const),
                pl.BlockSpec((1, d_model, d_ff), lambda e, first: (e, 0, 0)),
                pl.BlockSpec((1, d_ff, d_model), lambda e, first: (e, 0, 0)),
            ],
            out_specs=[row_spec, store_spec(d_model), store_spec(d_ff), store_spec(d_ff), pl.BlockSpec(wg.shape, const),
                       pl.BlockSpec(zero_block, lambda e, first: (e, 0, 0))],
        ),
        out_shape=[jax.ShapeDtypeStruct(rows.shape, BF16), rows_of(d_model), rows_of(d_ff), rows_of(d_ff),
                   jax.ShapeDtypeStruct(wg.shape, F32), jax.ShapeDtypeStruct(over_shape, BF16)],
        compiler_params=pltpu.CompilerParams(vmem_limit_bytes=VMEM_BYTES, dimension_semantics=('arbitrary',)),
        cost_estimate=pl.CostEstimate(flops=34_000_000_000, bytes_accessed=80_000_000, transcendentals=6_000_000),
        name='own_base',
    )(first_expert, rows, wg, w_up, w_down)


def group_copies(ids_ref, slot_base, count, hbm, buf, sem, to_hbm):
    def body(g, carry):
        gid = ids_ref[slot_base + g]
        ends = (buf.at[g], hbm.at[gid]) if to_hbm else (hbm.at[gid], buf.at[g])
        pltpu.make_async_copy(*ends, sem).start()
        return carry

    lax.fori_loop(0, count, body, 0)


def group_waits(count, hbm, buf, sem, to_hbm):
    def body(g, carry):
        ends = (buf.at[0], hbm.at[0]) if to_hbm else (hbm.at[0], buf.at[0])
        pltpu.make_async_copy(*ends, sem).wait()
        return carry

    lax.fori_loop(0, count, body, 0)


def tile_rows(buf, count):
    rows = buf[...].reshape(TILE, buf.shape[-1])
    row_id = lax.broadcasted_iota(I32, rows.shape, 0)
    return jnp.where(row_id < count * GROUP, rows, jnp.zeros((), rows.dtype))


def own_over_kernel(tab_ref, ids_ref, first_ref, rows_hbm, wg_ref, up_ref, down_ref, dwg_in, zero_od,
                    od_hbm, x_ref, dy_ref, h_ref, da_ref, dwg_ref, in_buf, out_buf, in_sem, out_sem):
    del zero_od
    step = pl.program_id(0)
    d_model = wg_ref.shape[0]
    slot = step % 2
    count = tab_ref[1, step]

    @pl.when(step == 0)
    def _():
        dwg_ref[...] = dwg_in[...]
        group_copies(ids_ref, 0, count, rows_hbm, in_buf.at[0], in_sem.at[0], False)

    @pl.when(count > 0)
    def _():
        group_waits(count, rows_hbm, in_buf.at[slot], in_sem.at[slot], False)

        @pl.when(step + 1 < pl.num_programs(0))
        def _():
            group_copies(ids_ref, (step + 1) * TILE_GROUPS, tab_ref[1, step + 1], rows_hbm, in_buf.at[1 - slot],
                         in_sem.at[1 - slot], False)

        rows = tile_rows(in_buf.at[slot], count)
        x = rows[:, :d_model]
        x_ref[...] = x
        out, dx = own_rows_step(x, rows[:, d_model:], first_ref[0] + tab_ref[0, step], wg_ref,
                                up_ref.at[0], down_ref.at[0], (dy_ref, h_ref, da_ref), dwg_ref)

        @pl.when(step > 0)
        def _():
            group_waits(tab_ref[1, step - 1], od_hbm, out_buf, out_sem, True)

        out_buf[:, :, :d_model] = out.reshape(TILE_GROUPS, GROUP, d_model)
        out_buf[:, :, d_model:] = dx.reshape(TILE_GROUPS, GROUP, d_model)
        group_copies(ids_ref, step * TILE_GROUPS, count, od_hbm, out_buf, out_sem, True)

        @pl.when(tab_ref[3, step] == 1)
        def _():
            group_waits(count, od_hbm, out_buf, out_sem, True)


def own_over_pass(table, ids, first_expert, rows, wg, w_up, w_down, dwg, zero_od):
    d_model, d_ff = w_up.shape[1], w_up.shape[2]
    width = rows.shape[-1]
    n_tiles = table.shape[1]
    hbm = pl.BlockSpec(memory_space=pl.ANY)
    const = lambda i, tab, ids, first: (0, 0)
    store_spec = lambda cols: pl.BlockSpec((TILE, cols), lambda i, tab, ids, first: (tab[2, i], 0))
    rows_of = lambda cols: jax.ShapeDtypeStruct((n_tiles * TILE, cols), BF16)
    return pl.pallas_call(
        own_over_kernel,
        grid_spec=pltpu.PrefetchScalarGridSpec(
            num_scalar_prefetch=3,
            grid=(n_tiles,),
            in_specs=[
                hbm,
                pl.BlockSpec(wg.shape, const),
                pl.BlockSpec((1, d_model, d_ff), lambda i, tab, ids, first: (tab[0, i], 0, 0)),
                pl.BlockSpec((1, d_ff, d_model), lambda i, tab, ids, first: (tab[0, i], 0, 0)),
                pl.BlockSpec(wg.shape, const),
                hbm,
            ],
            out_specs=[hbm, store_spec(d_model), store_spec(d_model), store_spec(d_ff), store_spec(d_ff),
                       pl.BlockSpec(wg.shape, const)],
            scratch_shapes=[
                pltpu.VMEM((2, TILE_GROUPS, GROUP, width), BF16),
                pltpu.VMEM((TILE_GROUPS, GROUP, width), BF16),
                pltpu.SemaphoreType.DMA((2,)),
                pltpu.SemaphoreType.DMA,
            ],
        ),
        out_shape=[jax.ShapeDtypeStruct(zero_od.shape, BF16), rows_of(d_model), rows_of(d_model), rows_of(d_ff),
                   rows_of(d_ff), jax.ShapeDtypeStruct(dwg.shape, F32)],
        input_output_aliases={8: 0},
        compiler_params=pltpu.CompilerParams(vmem_limit_bytes=VMEM_BYTES, dimension_semantics=('arbitrary',)),
        cost_estimate=pl.CostEstimate(flops=10_000_000_000, bytes_accessed=40_000_000, transcendentals=2_000_000),
        name='own_over',
    )(table, ids, first_expert, rows, wg, w_up, w_down, dwg, zero_od)


OWN_BASE, OWN_OVER, OTHER_BASE, OTHER_OVER = range(4)


def grad_kernel(tab_ref, ids_ref, first_ref, xb_ref, dyb_ref, hb_ref, dab_ref, xo_ref, dyo_ref, ho_ref, dao_ref, base_ref,
                over_hbm, wg_ref, up_hbm, down_hbm, dup_hbm, ddown_hbm,
                dup, ddown, up_buf, down_buf, h_buf, da_buf, in_buf, w_sems, in_sem, out_sems):
    step = pl.program_id(0)
    d_model, d_ff = dup.shape
    expert, kind, last, count = tab_ref[0, step], tab_ref[1, step], tab_ref[2, step], tab_ref[4, step]
    n_local = dup_hbm.shape[0]
    base_rows = h_buf.shape[0]

    def weights(e):
        return (pltpu.make_async_copy(up_hbm.at[e], up_buf, w_sems.at[0]),
                pltpu.make_async_copy(down_hbm.at[e], down_buf, w_sems.at[1]))

    def flush_down(e):
        return pltpu.make_async_copy(ddown, ddown_hbm.at[e], out_sems.at[0])

    def flush_up(e):
        return pltpu.make_async_copy(dup, dup_hbm.at[e], out_sems.at[1])

    def add_down(dy, h_src, add):
        for lo in range(0, d_ff, CHUNK):
            cols = pl.ds(lo, CHUNK)
            term = dot(h_src[:, cols], dy, ((0,), (0,)))
            ddown[cols, :] = ddown[cols, :] + term if add else term

    def add_up(x, da_src, add):
        for lo in range(0, d_ff, CHUNK):
            cols = pl.ds(lo, CHUNK)
            term = dot(x, da_src[:, cols], ((0,), (0,)))
            dup[:, cols] = dup[:, cols] + term if add else term

    def accumulate(x, dy, h_src, da_src):
        add_down(dy, h_src, True)

        @pl.when(last == 1)
        def _():
            flush_down(expert).start()

        add_up(x, da_src, True)

        @pl.when(last == 1)
        def _():
            flush_up(expert).start()

            @pl.when(expert + 1 < n_local)
            def _():
                for copy in weights(expert + 1):
                    copy.start()

            @pl.when(expert + 1 == n_local)
            def _():
                flush_down(expert).wait()
                flush_up(expert).wait()

    @pl.when(kind == OWN_BASE)
    def _():
        @pl.when(expert == 0)
        def _():
            for copy in weights(0):
                copy.start()

        @pl.when(expert > 0)
        def _():
            flush_down(expert - 1).wait()

        add_down(dyb_ref[...], hb_ref, False)

        @pl.when(expert > 0)
        def _():
            flush_up(expert - 1).wait()

        add_up(xb_ref[...].reshape(base_rows, d_model), dab_ref, False)

    @pl.when(kind == OWN_OVER)
    def _():
        add_down(dyo_ref[...], ho_ref, True)
        add_up(xo_ref[...], dao_ref, True)

    def other_rows(rows, n_rows):
        x, gy = rows[:, :d_model], rows[:, d_model:]
        _, _, gate_val = gate(x, wg_ref[...], first_ref[0] + expert)
        dy = (gate_val * gy.astype(F32)).astype(BF16)
        h_dst, da_dst = h_buf.at[:n_rows], da_buf.at[:n_rows]
        for lo in range(0, d_ff, ROW_CHUNK):
            cols = pl.ds(lo, ROW_CHUNK)
            h, da = activations(x, dy, up_buf, down_buf, cols)
            h_dst[:, cols] = h
            da_dst[:, cols] = da
        accumulate(x, dy, h_dst, da_dst)

    @pl.when(kind == OTHER_BASE)
    def _():
        for copy in weights(expert):
            copy.wait()
        other_rows(base_ref[...].reshape(base_rows, 2 * d_model), base_rows)

    @pl.when(kind == OTHER_OVER)
    def _():
        group_copies(ids_ref, tab_ref[5, step] * TILE_GROUPS, count, over_hbm, in_buf, in_sem, False)
        group_waits(count, over_hbm, in_buf, in_sem, False)
        other_rows(tile_rows(in_buf, count), TILE)


def grad_pass(table, ids, first_expert, own_base, base_store, over_store, base, over, wg, w_up, w_down):
    n_src, _, seg, width = base.shape
    d_model, d_ff = w_up.shape[1], w_up.shape[2]
    base_rows = n_src * seg
    base_spec = lambda cols: pl.BlockSpec((base_rows, cols), lambda i, tab, ids, first: (tab[6, i], 0))
    over_spec = lambda cols: pl.BlockSpec((TILE, cols), lambda i, tab, ids, first: (tab[3, i], 0))
    slot_spec = lambda cols, row: pl.BlockSpec((n_src, 1, seg, cols), lambda i, tab, ids, first: (0, tab[row, i], 0, 0))
    hbm = pl.BlockSpec(memory_space=pl.ANY)
    return pl.pallas_call(
        grad_kernel,
        grid_spec=pltpu.PrefetchScalarGridSpec(
            num_scalar_prefetch=3,
            grid=(table.shape[1],),
            in_specs=[
                slot_spec(d_model, 6),
                base_spec(d_model),
                base_spec(d_ff),
                base_spec(d_ff),
                over_spec(d_model),
                over_spec(d_model),
                over_spec(d_ff),
                over_spec(d_ff),
                slot_spec(width, 0),
                hbm,
                pl.BlockSpec(wg.shape, lambda i, tab, ids, first: (0, 0)),
                hbm,
                hbm,
            ],
            out_specs=[hbm, hbm],
            scratch_shapes=[
                pltpu.VMEM((d_model, d_ff), F32),
                pltpu.VMEM((d_ff, d_model), F32),
                pltpu.VMEM((d_model, d_ff), BF16),
                pltpu.VMEM((d_ff, d_model), BF16),
                pltpu.VMEM((base_rows, d_ff), BF16),
                pltpu.VMEM((base_rows, d_ff), BF16),
                pltpu.VMEM((TILE_GROUPS, GROUP, width), BF16),
                pltpu.SemaphoreType.DMA((2,)),
                pltpu.SemaphoreType.DMA,
                pltpu.SemaphoreType.DMA((2,)),
            ],
        ),
        out_shape=[jax.ShapeDtypeStruct(w_up.shape, F32), jax.ShapeDtypeStruct(w_down.shape, F32)],
        compiler_params=pltpu.CompilerParams(vmem_limit_bytes=VMEM_BYTES, dimension_semantics=('arbitrary',)),
        cost_estimate=pl.CostEstimate(flops=70_000_000_000, bytes_accessed=150_000_000, transcendentals=8_000_000),
        name='grad_pass',
    )(table, ids, first_expert, own_base, *base_store, *over_store, base, over, wg, w_up, w_down)


def over_tiles(over, start, max_tiles):
    per_expert = jnp.sum(over, axis=0)
    tiles = (per_expert + TILE_GROUPS - 1) // TILE_GROUPS
    end = jnp.cumsum(tiles)
    step = jnp.arange(max_tiles, dtype=I32)
    expert = jnp.minimum(jnp.sum(step[:, None] >= end[None, :], axis=1, dtype=I32), over.shape[1] - 1)
    pick = (expert[:, None] == jnp.arange(over.shape[1], dtype=I32)[None, :]).astype(I32)
    of = lambda v: jnp.sum(pick * v[None, :], axis=1)
    done = (step - of(end - tiles)) * TILE_GROUPS
    count = jnp.clip(of(per_expert) - done, 0, TILE_GROUPS)
    rank = done[:, None] + jnp.arange(TILE_GROUPS, dtype=I32)[None, :]
    before = exclusive_cumsum(over, 0)
    shift = jnp.sum(pick[:, None, :] * (start - before)[None, :, :], axis=2)
    first = jnp.sum(pick[:, None, :] * before[None, :, :], axis=2)
    size = jnp.sum(pick[:, None, :] * over[None, :, :], axis=2)
    inside = (rank[:, :, None] >= first[:, None, :]) & (rank[:, :, None] < (first + size)[:, None, :])
    gid = jnp.sum(jnp.where(inside, rank[:, :, None] + shift[:, None, :], 0), axis=2)
    return expert, count, gid.reshape(-1), end - tiles, tiles


def grad_table(own_first, own_tiles, other_first, other_tiles, other_count, max_steps):
    n_exp = own_tiles.shape[0]
    one = jnp.ones((n_exp,), I32)
    length = jnp.stack([one, own_tiles, one, other_tiles], axis=1).reshape(-1)
    end = jnp.cumsum(length)
    step = jnp.arange(max_steps, dtype=I32)
    seg = jnp.minimum(jnp.sum(step[:, None] >= end[None, :], axis=1, dtype=I32), 4 * n_exp - 1)
    pick = (seg[:, None] == jnp.arange(4 * n_exp, dtype=I32)[None, :]).astype(I32)
    of = lambda v: jnp.sum(pick * v[None, :], axis=1)
    tile = step - of(end - length)
    expert, kind = seg // 4, seg % 4
    live = step < end[-1]
    last = live & (step + 1 == of(jnp.repeat(end[3::4], 4)))
    last_own = jnp.maximum(jnp.sum(own_tiles) - 1, 0)
    own_tile = jnp.where(kind == OWN_OVER, of(jnp.repeat(own_first, 4)) + tile, of(jnp.repeat(own_first + own_tiles, 4)))
    own_tile = jnp.where(kind == OWN_BASE, of(jnp.repeat(own_first, 4)), own_tile)
    other_tile = jnp.where(kind == OTHER_OVER, of(jnp.repeat(other_first, 4)) + tile, 0)
    tile_pick = (other_tile[:, None] == jnp.arange(other_count.shape[0], dtype=I32)[None, :]).astype(I32)
    count = jnp.sum(tile_pick * other_count[None, :], axis=1)
    next_base = jnp.minimum(expert + (kind > OWN_BASE), n_exp - 1)
    return jnp.stack([expert, jnp.where(live, kind, -1), last.astype(I32), jnp.minimum(own_tile, last_own), count,
                      jnp.minimum(other_tile, other_count.shape[0] - 1), next_base]).astype(I32)


def padded_step(x_loc, gy_loc, idx_loc, w_gate, w_up, w_down, ep_size, dp_size):
    tok_count, d_model = x_loc.shape
    n_experts = w_gate.shape[1]
    local_experts = w_up.shape[0]
    cap_rows = PAD_FACTOR * tok_count // n_experts
    onehot = idx_loc[:, None] == jnp.arange(n_experts, dtype=I32)[None, :]
    expert_count = jnp.sum(onehot, axis=0, dtype=I32)
    sort_order = jnp.argsort(idx_loc, stable=True)
    sorted_pos = jnp.argsort(sort_order)
    expert_start = jnp.cumsum(expert_count) - expert_count
    slot_k = jnp.arange(cap_rows, dtype=I32)
    slot_valid = slot_k[None, :] < expert_count[:, None]
    src_tok = sort_order[jnp.minimum(expert_start[:, None] + slot_k[None, :], tok_count - 1)]
    slot_tok = idx_loc * cap_rows + sorted_pos - expert_start[idx_loc]

    def dispatch(tok_rows):
        picked = jnp.where(slot_valid[:, :, None], tok_rows[src_tok], jnp.zeros((), tok_rows.dtype))
        picked = picked.reshape(ep_size, local_experts, cap_rows, d_model)
        return lax.all_to_all(picked, 'ep', 0, 0, tiled=True)

    def combine(expert_rows):
        returned = lax.all_to_all(expert_rows, 'ep', 1, 0, tiled=True)
        return returned.reshape(n_experts * cap_rows, d_model)[slot_tok]

    router_logit = jnp.dot(x_loc, w_gate, preferred_element_type=F32)
    router_prob = jax.nn.softmax(router_logit, axis=-1)
    gate_val = n_experts * jnp.sum(jnp.where(onehot, router_prob, 0.0), axis=1)
    recv_rows = dispatch(x_loc)
    gy_full = gy_loc.astype(F32)
    dy_tok = (gate_val[:, None] * gy_full).astype(BF16)
    recv_grad = dispatch(dy_tok)

    def one_expert(carry, per_expert):
        rows, grad, up, down = per_expert
        rows, grad = rows.reshape(-1, d_model), grad.reshape(-1, d_model)
        pre_act = dot(rows, up)
        hid_full, gelu_back = jax.vjp(jax.nn.gelu, pre_act)
        hidden = hid_full.astype(BF16)
        out_rows = dot(hidden, down).astype(BF16)
        d_pre = gelu_back(dot(grad, down, ((1,), (1,))))[0].astype(BF16)
        grad_down = dot(hidden, grad, ((0,), (0,)))
        grad_up = dot(rows, d_pre, ((0,), (0,)))
        d_rows = dot(d_pre, up, ((1,), (1,))).astype(BF16)
        shape = (ep_size, cap_rows, d_model)
        return carry, (out_rows.reshape(shape), d_rows.reshape(shape), grad_up, grad_down)

    swap = lambda rows: jnp.swapaxes(rows, 0, 1)
    _, (expert_out, d_rows, grad_up, grad_down) = lax.scan(
        one_expert, 0, (swap(recv_rows), swap(recv_grad), w_up, w_down))
    y_tok = combine(expert_out)
    moe_out = (gate_val[:, None] * y_tok.astype(F32)).astype(BF16)
    dx_expert = combine(d_rows)
    d_gate = jnp.sum(gy_full * y_tok.astype(F32), axis=1)
    d_logit = ((d_gate * gate_val)[:, None] * (onehot.astype(F32) - router_prob)).astype(BF16)
    dx_router = dot(d_logit, w_gate, ((1,), (1,)))
    grad_x = (dx_expert.astype(F32) + dx_router).astype(BF16)
    grad_gate = dot(x_loc, d_logit, ((0,), (0,)))

    def sum_dp(term):
        total = term
        for shift in range(1, dp_size):
            total = total + lax.ppermute(term, 'dp', [(i, (i + shift) % dp_size) for i in range(dp_size)])
        return total

    return (moe_out, grad_x, sum_dp(grad_up), sum_dp(grad_down), lax.psum(grad_gate, ('dp', 'ep')))


def solution(mesh):
    dp_size, ep_size = mesh.shape['dp'], mesh.shape['ep']
    tok_spec = P(('dp', 'ep'), None)
    idx_spec = P(('dp', 'ep'))
    rep_spec = P(None, None)
    exp_spec = P('ep', None, None)
    swap = [(i, (i + 1) % dp_size) for i in range(dp_size)]

    def local_step(x, gy, idx, w_gate, w_up, w_down):
        _, d_model = x.shape
        n_experts = w_gate.shape[1]
        local = w_up.shape[0]
        width = 2 * d_model
        base_rows = BASE_GROUPS * GROUP
        n_base = n_experts * base_rows
        n_over = OVER_GROUPS * GROUP
        max_tiles = MAX_OVER_TILES
        max_steps = 2 * (local + max_tiles)
        dp, ep = lax.axis_index('dp'), lax.axis_index('ep')
        first_expert = (ep * local).astype(I32).reshape(1)

        my_groups, pos = token_positions(idx, n_experts)
        base_sent = permute_rows(pos, x, gy, 0, n_base)
        base = lax.all_to_all(base_sent.reshape(ep_size, local * base_rows, width), 'ep', 0, 0, tiled=True)
        over_sent = permute_rows(pos, x, gy, n_base, n_over).reshape(OVER_GROUPS, GROUP, width)
        all_groups = lax.all_gather(my_groups, ('dp', 'ep')).reshape(dp_size, ep_size, n_experts)
        over = lax.all_gather(over_sent, 'ep').reshape(ep_size * OVER_GROUPS, GROUP, width)
        base_z = lax.ppermute(base, 'dp', swap)
        over_sent_z = lax.ppermute(over_sent, 'dp', swap)
        over_z = lax.all_gather(over_sent_z, 'ep').reshape(over.shape)

        all_over = jnp.maximum(all_groups - BASE_GROUPS, 0)
        owner_over = jnp.sum(all_over, axis=1).reshape(dp_size * ep_size, local)
        owner_tiles = jnp.sum((owner_over + TILE_GROUPS - 1) // TILE_GROUPS, axis=1)
        fits = jnp.all(jnp.sum(all_over, axis=2) <= OVER_GROUPS) & jnp.all(owner_tiles <= max_tiles)
        all_over = jnp.where(fits, all_over, 0)

        def plane_over(plane):
            over = lax.dynamic_index_in_dim(all_over, plane, 0, keepdims=False)
            start = exclusive_cumsum(over, 1) + (jnp.arange(ep_size, dtype=I32) * OVER_GROUPS)[:, None]
            here = lambda t: lax.dynamic_slice_in_dim(t, ep * local, local, 1)
            return over_tiles(here(over), here(start), max_tiles)

        expert, count, ids, own_first, own_tiles = plane_over(dp)
        _, count_z, ids_z, other_first, other_tiles = plane_over((dp + 1) % dp_size)
        gtable = grad_table(own_first, own_tiles, other_first, other_tiles, count_z, max_steps)
        tile_id = jnp.arange(max_tiles, dtype=I32)
        last = jnp.maximum(jnp.sum(own_tiles) - 1, 0)
        table = jnp.stack([expert, count, jnp.minimum(tile_id, last), tile_id == last]).astype(I32)

        slots = (ep_size, local, base_rows, width)
        base = base.reshape(slots)
        od, dy_b, h_b, da_b, dwg, zero_od = own_base_pass(first_expert, base, w_gate, w_up, w_down, over.shape)
        base_back = lax.all_to_all(od.reshape(ep_size, local * base_rows, width), 'ep', 0, 0, tiled=True)
        od_over, x_o, dy_o, h_o, da_o, dwg = own_over_pass(table, ids, first_expert, over, w_gate, w_up, w_down, dwg,
                                                          zero_od)
        over_back = lax.psum_scatter(od_over.reshape(ep_size, OVER_GROUPS, GROUP, width), 'ep', scatter_dimension=0)
        d_up, d_down = grad_pass(gtable, ids_z, first_expert, base, (dy_b, h_b, da_b), (x_o, dy_o, h_o, da_o),
                                 base_z.reshape(slots), over_z, w_gate, w_up, w_down)
        d_gate = lax.psum(dwg, ('dp', 'ep'))
        moe_out, grad_x = unpermute_rows(pos, base_back.reshape(n_base, width), over_back.reshape(n_over, width))
        sparse = (moe_out, grad_x, d_up, d_down, d_gate)

        def dense(carry):
            del carry
            return (jnp.array(True),) + padded_step(x, gy, idx, w_gate, w_up, w_down, ep_size, dp_size)

        return lax.while_loop(lambda carry: jnp.logical_not(carry[0]), dense, (fits,) + sparse)[1:]

    return jax.shard_map(
        local_step, mesh=mesh, in_specs=(tok_spec, tok_spec, idx_spec, rep_spec, exp_spec, exp_spec),
        out_specs=(tok_spec, tok_spec, exp_spec, exp_spec, rep_spec), check_vma=False)
```

```python
import functools

import jax
import jax.numpy as jnp
from jax import lax
from jax.experimental import pallas as pl
from jax.experimental.pallas import tpu as pltpu
from jax.sharding import PartitionSpec as P


PAD_FACTOR = 4
GROUP = 8
BASE_GROUPS = 7
OVER_GROUPS = 50
SENT_GROUPS = OVER_GROUPS + 1
MAX_OVER_TILES = 8
TILE_GROUPS = 26
TILE = TILE_GROUPS * GROUP
PERM_TILE = 256
CHUNK = 512
ROW_CHUNK = 256
CHUNKS = 2
SQRT_2_PI = 0.7978845608028654
CUBIC = 0.044715
VMEM_BYTES = 67_043_328

F32 = jnp.float32
BF16 = jnp.bfloat16
I32 = jnp.int32


def dot(a, b, dims=((1,), (0,))):
    return lax.dot_general(a, b, (dims, ((), ())), preferred_element_type=F32)


def exclusive_cumsum(v, axis):
    return jnp.cumsum(v, axis=axis) - v


def token_positions(idx, n_experts, local):
    tok_count = idx.shape[0]
    block = 128
    base_rows = BASE_GROUPS * GROUP
    onehot = (idx[:, None] == jnp.arange(n_experts, dtype=I32)[None, :]).astype(BF16)
    blocks = onehot.reshape(tok_count // block, block, n_experts)
    lower = jnp.tril(jnp.ones((block, block), BF16))
    inclusive = jnp.einsum('ij,bje->bie', lower, blocks, preferred_element_type=F32)
    totals = jnp.sum(blocks.astype(F32), axis=1)
    counts = jnp.sum(totals, axis=0).astype(I32)
    groups = (counts + GROUP - 1) // GROUP
    over = jnp.maximum(groups - BASE_GROUPS, 0)
    over_start = exclusive_cumsum(over, 0)
    rank = inclusive + (exclusive_cumsum(totals, 0) - 1.0)[:, None, :]
    expert = jnp.arange(n_experts, dtype=I32)
    per_chunk = local // CHUNKS
    slot = (expert % local // per_chunk) * (n_experts // CHUNKS) + expert // local * per_chunk + expert % per_chunk
    base_at = (slot * base_rows).astype(F32)
    over_at = (n_experts * base_rows - base_rows + over_start * GROUP).astype(F32)
    row = jnp.sum(blocks.astype(F32) * (rank + jnp.where(rank < base_rows, base_at, over_at)), axis=2)
    return groups, row.reshape(tok_count).astype(I32)


def permute_kernel(pos_ref, x_ref, gy_ref, *refs):
    *tail, out_ref = refs
    d_model = x_ref.shape[1]
    rows = out_ref.shape[0] - sum(t.shape[0] for t in tail)
    row_id = pl.program_id(0) * rows + lax.broadcasted_iota(I32, (rows, x_ref.shape[0]), 0)
    select = jnp.where(row_id == pos_ref[...], 1.0, 0.0).astype(BF16)
    out_ref[:rows, :d_model] = dot(select, x_ref[...]).astype(BF16)
    out_ref[:rows, d_model:] = dot(select, gy_ref[...]).astype(BF16)
    for t in tail:
        out_ref[rows:, :] = t[...]


def permute_rows(pos, x, gy, first_row, n_rows, *tail):
    tok_count, d_model = x.shape
    tile = n_rows if n_rows % PERM_TILE else PERM_TILE
    extra = sum(t.shape[0] for t in tail)
    return pl.pallas_call(
        permute_kernel,
        grid=(n_rows // tile,),
        in_specs=[
            pl.BlockSpec((1, tok_count), lambda i: (0, 0)),
            pl.BlockSpec((tok_count, d_model), lambda i: (0, 0)),
            pl.BlockSpec((tok_count, d_model), lambda i: (0, 0)),
        ] + [pl.BlockSpec(t.shape, lambda i: (0, 0)) for t in tail],
        out_specs=pl.BlockSpec((tile + extra, 2 * d_model), lambda i: (i, 0)),
        out_shape=jax.ShapeDtypeStruct((n_rows + extra, 2 * d_model), BF16),
        cost_estimate=pl.CostEstimate(flops=4 * n_rows * tok_count * d_model, bytes_accessed=16_000_000, transcendentals=0),
        name='permute',
    )((pos - first_row).reshape(1, tok_count), x, gy, *tail)


def unpermute_kernel(pos_ref, *refs):
    *parts, out_ref, dx_ref = refs
    toks, d_model = out_ref.shape
    first, out, dx = 0, 0.0, 0.0
    for part in parts:
        rows = part[...].reshape(-1, 2 * d_model)
        row_id = lax.broadcasted_iota(I32, (toks, rows.shape[0]), 1) + first
        select = jnp.where(row_id == pos_ref[...], 1.0, 0.0).astype(BF16)
        out += dot(select, rows[:, :d_model])
        dx += dot(select, rows[:, d_model:])
        first += rows.shape[0]
    out_ref[...] = out.astype(BF16)
    dx_ref[...] = dx.astype(BF16)


def unpermute_rows(pos, base, over):
    n_own, n_slot, width = base.shape
    tok_count = pos.shape[0]
    d_model = width // 2
    shape = jax.ShapeDtypeStruct((tok_count, d_model), BF16)
    chunk = (n_own, n_slot // CHUNKS, width)
    return pl.pallas_call(
        unpermute_kernel,
        grid=(tok_count // PERM_TILE,),
        in_specs=[pl.BlockSpec((PERM_TILE, 1), lambda i: (i, 0))]
        + [pl.BlockSpec(chunk, lambda i, c=c: (0, c, 0)) for c in range(CHUNKS)]
        + [pl.BlockSpec(over.shape, lambda i: (0, 0))],
        out_specs=[pl.BlockSpec((PERM_TILE, d_model), lambda i: (i, 0))] * 2,
        out_shape=[shape, shape],
        cost_estimate=pl.CostEstimate(flops=14_000_000_000, bytes_accessed=16_000_000, transcendentals=0),
        name='unpermute',
    )(pos.reshape(tok_count, 1), *[base] * CHUNKS, over)


def gate(x, wg, expert):
    logit = dot(x, wg)
    unnorm = jnp.exp(logit - jnp.max(logit, axis=1, keepdims=True))
    prob = unnorm / jnp.sum(unnorm, axis=1, keepdims=True)
    onehot = lax.broadcasted_iota(I32, prob.shape, 1) == expert
    gate_val = prob.shape[1] * jnp.sum(jnp.where(onehot, prob, 0.0), axis=1, keepdims=True)
    return prob, onehot, gate_val


def activations(x, dy, w_up, w_down, cols):
    a = dot(x, w_up[:, cols])
    dh = dot(dy, w_down[cols, :], ((1,), (1,)))
    cubic = (SQRT_2_PI * CUBIC) * (a * a)
    half = 0.5 + 0.5 * jnp.tanh(a * (SQRT_2_PI + cubic))
    h = a * half
    slope = half + (h - h * half) * (2.0 * SQRT_2_PI + 6.0 * cubic)
    return h.astype(BF16), (slope * dh).astype(BF16)


def own_rows_step(x, gy, expert, wg_ref, w_up, w_down, store, dwg_ref):
    dy_ref, h_ref, da_ref = store
    prob, onehot, gate_val = gate(x, wg_ref[...], expert)
    gy_full = gy.astype(F32)
    dy = (gate_val * gy_full).astype(BF16)
    dy_ref[...] = dy
    for lo in range(0, h_ref.shape[1], ROW_CHUNK):
        cols = pl.ds(lo, ROW_CHUNK)
        h, da = activations(x, dy, w_up, w_down, cols)
        h_ref[:, cols] = h
        da_ref[:, cols] = da
    y = dot(h_ref[...], w_down[...]).astype(BF16).astype(F32)
    dxe = dot(da_ref[...], w_up[...], ((1,), (1,))).astype(BF16).astype(F32)
    d_gate = jnp.sum(gy_full * y, axis=1, keepdims=True)
    d_logit = ((d_gate * gate_val) * (onehot.astype(F32) - prob)).astype(BF16)
    dwg_ref[...] += dot(d_logit, x, ((0,), (0,)))
    out = (gate_val * y).astype(BF16)
    dx = (dxe + dot(d_logit, wg_ref[...], ((1,), (1,)))).astype(BF16)
    return out, dx


def own_base_kernel(first_ref, rows_ref, wg_ref, up_ref, down_ref, dwg_in, *refs):
    od_ref, x_ref, dy_ref, h_ref, da_ref, dwg_ref, zero_ref = refs[-7:]
    step = pl.program_id(0)
    d_model = wg_ref.shape[0]

    @pl.when(step == 0)
    def _():
        dwg_ref[...] = dwg_in[...]

    zero_ref[...] = jnp.zeros_like(zero_ref)
    rows = rows_ref[...].reshape(dy_ref.shape[0], 2 * d_model)
    x = rows[:, :d_model]
    x_ref[...] = x
    out, dx = own_rows_step(x, rows[:, d_model:], first_ref[0] + step, wg_ref, up_ref.at[0], down_ref.at[0],
                            (dy_ref, h_ref, da_ref), dwg_ref)
    block = od_ref.shape[:3] + (d_model,)
    od_ref[:, :, :, :d_model] = out.reshape(block)
    od_ref[:, :, :, d_model:] = dx.reshape(block)


def own_base_pass(first_expert, chunk, rows, wg, w_up, w_down, dwg, stores, over_shape):
    n_src, count, seg, width = rows.shape
    local, d_model, d_ff = w_up.shape
    tile = n_src * seg
    lead = chunk * count
    row_spec = lambda at: pl.BlockSpec((n_src, 1, seg, width), lambda e, first: (0, at + e, 0, 0))
    store_spec = lambda cols: pl.BlockSpec((tile, cols), lambda e, first: (lead + e, 0))
    const = lambda e, first: (0, 0)
    rows_of = lambda cols: jax.ShapeDtypeStruct((local * tile, cols), BF16)
    zero_block = (over_shape[0] // local,) + over_shape[1:]
    kept = [] if stores is None else list(stores)
    return pl.pallas_call(
        own_base_kernel,
        grid_spec=pltpu.PrefetchScalarGridSpec(
            num_scalar_prefetch=1,
            grid=(count,),
            in_specs=[
                row_spec(0),
                pl.BlockSpec(wg.shape, const),
                pl.BlockSpec((1, d_model, d_ff), lambda e, first: (lead + e, 0, 0)),
                pl.BlockSpec((1, d_ff, d_model), lambda e, first: (lead + e, 0, 0)),
                pl.BlockSpec(dwg.shape, const),
            ] + [pl.BlockSpec(memory_space=pl.ANY)] * len(kept),
            out_specs=[row_spec(lead), store_spec(d_model), store_spec(d_model), store_spec(d_ff), store_spec(d_ff),
                       pl.BlockSpec(dwg.shape, const), pl.BlockSpec(zero_block, lambda e, first: (lead + e, 0, 0))],
        ),
        out_shape=[jax.ShapeDtypeStruct((n_src, local, seg, width), BF16), rows_of(d_model), rows_of(d_model), rows_of(d_ff), rows_of(d_ff),
                   jax.ShapeDtypeStruct(dwg.shape, F32), jax.ShapeDtypeStruct(over_shape, BF16)],
        input_output_aliases={6 + i: o for i, o in zip(range(len(kept)), (0, 1, 2, 3, 4, 6))},
        compiler_params=pltpu.CompilerParams(vmem_limit_bytes=VMEM_BYTES, dimension_semantics=('arbitrary',)),
        cost_estimate=pl.CostEstimate(flops=8_500_000_000 * count, bytes_accessed=20_000_000 * count,
                                      transcendentals=1_500_000 * count),
        name='own_base',
    )(first_expert + lead, rows, wg, w_up, w_down, dwg, *kept)


def group_copies(ids_ref, slot_base, count, hbm, buf, sem, to_hbm):
    def body(g, carry):
        gid = ids_ref[slot_base + g]
        ends = (buf.at[g], hbm.at[gid]) if to_hbm else (hbm.at[gid], buf.at[g])
        pltpu.make_async_copy(*ends, sem).start()
        return carry

    lax.fori_loop(0, count, body, 0)


def group_waits(count, hbm, buf, sem, to_hbm):
    def body(g, carry):
        ends = (buf.at[0], hbm.at[0]) if to_hbm else (hbm.at[0], buf.at[0])
        pltpu.make_async_copy(*ends, sem).wait()
        return carry

    lax.fori_loop(0, count, body, 0)


def tile_rows(buf, count):
    rows = buf[...].reshape(TILE, buf.shape[-1])
    row_id = lax.broadcasted_iota(I32, rows.shape, 0)
    return jnp.where(row_id < count * GROUP, rows, jnp.zeros((), rows.dtype))


def own_over_kernel(tab_ref, ids_ref, back_ids_ref, first_ref, rows_hbm, wg_ref, up_ref, down_ref, dwg_in, zero_od,
                    od_hbm, x_ref, dy_ref, h_ref, da_ref, dwg_ref, in_buf, out_buf, in_sem, out_sem):
    del zero_od
    step = pl.program_id(0)
    d_model = wg_ref.shape[0]
    slot = step % 2
    count = tab_ref[1, step]

    @pl.when(step == 0)
    def _():
        dwg_ref[...] = dwg_in[...]
        group_copies(ids_ref, 0, count, rows_hbm, in_buf.at[0], in_sem.at[0], False)

    @pl.when(count > 0)
    def _():
        group_waits(count, rows_hbm, in_buf.at[slot], in_sem.at[slot], False)

        @pl.when(step + 1 < pl.num_programs(0))
        def _():
            group_copies(ids_ref, (step + 1) * TILE_GROUPS, tab_ref[1, step + 1], rows_hbm, in_buf.at[1 - slot],
                         in_sem.at[1 - slot], False)

        rows = tile_rows(in_buf.at[slot], count)
        x = rows[:, :d_model]
        x_ref[...] = x
        out, dx = own_rows_step(x, rows[:, d_model:], first_ref[0] + tab_ref[0, step], wg_ref,
                                up_ref.at[0], down_ref.at[0], (dy_ref, h_ref, da_ref), dwg_ref)

        @pl.when(step > 0)
        def _():
            group_waits(tab_ref[1, step - 1], od_hbm, out_buf, out_sem, True)

        out_buf[:, :, :d_model] = out.reshape(TILE_GROUPS, GROUP, d_model)
        out_buf[:, :, d_model:] = dx.reshape(TILE_GROUPS, GROUP, d_model)
        group_copies(back_ids_ref, step * TILE_GROUPS, count, od_hbm, out_buf, out_sem, True)

        @pl.when(tab_ref[3, step] == 1)
        def _():
            group_waits(count, od_hbm, out_buf, out_sem, True)


def own_over_pass(table, ids, back_ids, first_expert, rows, wg, w_up, w_down, dwg, zero_od):
    d_model, d_ff = w_up.shape[1], w_up.shape[2]
    width = rows.shape[-1]
    n_tiles = table.shape[1]
    hbm = pl.BlockSpec(memory_space=pl.ANY)
    const = lambda i, tab, ids, back, first: (0, 0)
    store_spec = lambda cols: pl.BlockSpec((TILE, cols), lambda i, tab, ids, back, first: (tab[2, i], 0))
    rows_of = lambda cols: jax.ShapeDtypeStruct((n_tiles * TILE, cols), BF16)
    return pl.pallas_call(
        own_over_kernel,
        grid_spec=pltpu.PrefetchScalarGridSpec(
            num_scalar_prefetch=4,
            grid=(n_tiles,),
            in_specs=[
                hbm,
                pl.BlockSpec(wg.shape, const),
                pl.BlockSpec((1, d_model, d_ff), lambda i, tab, ids, back, first: (tab[0, i], 0, 0)),
                pl.BlockSpec((1, d_ff, d_model), lambda i, tab, ids, back, first: (tab[0, i], 0, 0)),
                pl.BlockSpec(dwg.shape, const),
                hbm,
            ],
            out_specs=[hbm, store_spec(d_model), store_spec(d_model), store_spec(d_ff), store_spec(d_ff),
                       pl.BlockSpec(dwg.shape, const)],
            scratch_shapes=[
                pltpu.VMEM((2, TILE_GROUPS, GROUP, width), BF16),
                pltpu.VMEM((TILE_GROUPS, GROUP, width), BF16),
                pltpu.SemaphoreType.DMA((2,)),
                pltpu.SemaphoreType.DMA,
            ],
        ),
        out_shape=[jax.ShapeDtypeStruct(zero_od.shape, BF16), rows_of(d_model), rows_of(d_model), rows_of(d_ff),
                   rows_of(d_ff), jax.ShapeDtypeStruct(dwg.shape, F32)],
        input_output_aliases={9: 0},
        compiler_params=pltpu.CompilerParams(vmem_limit_bytes=VMEM_BYTES, dimension_semantics=('arbitrary',)),
        cost_estimate=pl.CostEstimate(flops=10_000_000_000, bytes_accessed=40_000_000, transcendentals=2_000_000),
        name='own_over',
    )(table, ids, back_ids, first_expert, rows, wg, w_up, w_down, dwg, zero_od)


OWN_BASE, OWN_OVER, OTHER_BASE, OTHER_OVER = range(4)


def grad_kernel(tab_ref, ids_ref, first_ref, xb_ref, dyb_ref, hb_ref, dab_ref, xo_ref, dyo_ref, ho_ref, dao_ref, *refs):
    *base_hbm, over_hbm, wg_ref, up_hbm, down_hbm, dup_hbm, ddown_hbm = refs[:-12]
    dup, ddown, up_buf, down_buf, h_buf, da_buf, base_buf, in_buf, w_sems, base_sem, in_sem, out_sems = refs[-12:]
    step = pl.program_id(0)
    d_model, d_ff = dup.shape
    expert, kind, last, count = tab_ref[0, step], tab_ref[1, step], tab_ref[2, step], tab_ref[4, step]
    n_local = dup_hbm.shape[0]
    base_rows = h_buf.shape[0]

    def weights(e):
        return (pltpu.make_async_copy(up_hbm.at[e], up_buf, w_sems.at[0]),
                pltpu.make_async_copy(down_hbm.at[e], down_buf, w_sems.at[1]))

    def flush_down(e):
        return pltpu.make_async_copy(ddown, ddown_hbm.at[e], out_sems.at[0])

    def flush_up(e):
        return pltpu.make_async_copy(dup, dup_hbm.at[e], out_sems.at[1])

    def add_down(dy, h_src, add):
        for lo in range(0, d_ff, CHUNK):
            cols = pl.ds(lo, CHUNK)
            term = dot(h_src[:, cols], dy, ((0,), (0,)))
            ddown[cols, :] = ddown[cols, :] + term if add else term

    def add_up(x, da_src, add):
        for lo in range(0, d_ff, CHUNK):
            cols = pl.ds(lo, CHUNK)
            term = dot(x, da_src[:, cols], ((0,), (0,)))
            dup[:, cols] = dup[:, cols] + term if add else term

    def accumulate(x, dy, h_src, da_src):
        add_down(dy, h_src, True)

        @pl.when(last == 1)
        def _():
            flush_down(expert).start()

        add_up(x, da_src, True)

        @pl.when(last == 1)
        def _():
            flush_up(expert).start()

            @pl.when(expert + 1 < n_local)
            def _():
                for copy in weights(expert + 1):
                    copy.start()

            @pl.when(expert + 1 == n_local)
            def _():
                flush_down(expert).wait()
                flush_up(expert).wait()

    def base_copy(e):
        chunk = base_hbm[e // base_hbm[0].shape[1]]
        return pltpu.make_async_copy(chunk.at[:, e % chunk.shape[1]], base_buf, base_sem)

    @pl.when(kind == OWN_BASE)
    def _():
        for e in range(n_local):
            @pl.when(expert == e)
            def _():
                base_copy(e).start()

        @pl.when(expert == 0)
        def _():
            for copy in weights(0):
                copy.start()

        @pl.when(expert > 0)
        def _():
            flush_down(expert - 1).wait()

        add_down(dyb_ref[...], hb_ref, False)

        @pl.when(expert > 0)
        def _():
            flush_up(expert - 1).wait()

        add_up(xb_ref[...], dab_ref, False)

    @pl.when(kind == OWN_OVER)
    def _():
        add_down(dyo_ref[...], ho_ref, True)
        add_up(xo_ref[...], dao_ref, True)

    def other_rows(rows, n_rows):
        x, gy = rows[:, :d_model], rows[:, d_model:]
        _, _, gate_val = gate(x, wg_ref[...], first_ref[0] + expert)
        dy = (gate_val * gy.astype(F32)).astype(BF16)
        h_dst, da_dst = h_buf.at[:n_rows], da_buf.at[:n_rows]
        for lo in range(0, d_ff, ROW_CHUNK):
            cols = pl.ds(lo, ROW_CHUNK)
            h, da = activations(x, dy, up_buf, down_buf, cols)
            h_dst[:, cols] = h
            da_dst[:, cols] = da
        accumulate(x, dy, h_dst, da_dst)

    @pl.when(kind == OTHER_BASE)
    def _():
        for copy in weights(expert):
            copy.wait()
        base_copy(0).wait()
        other_rows(base_buf[...].reshape(base_rows, 2 * d_model), base_rows)

    @pl.when(kind == OTHER_OVER)
    def _():
        group_copies(ids_ref, tab_ref[5, step] * TILE_GROUPS, count, over_hbm, in_buf, in_sem, False)
        group_waits(count, over_hbm, in_buf, in_sem, False)
        other_rows(tile_rows(in_buf, count), TILE)


def grad_pass(table, ids, first_expert, base_store, over_store, base, over, wg, w_up, w_down):
    n_src, _, seg, width = base[0].shape
    d_model, d_ff = w_up.shape[1], w_up.shape[2]
    base_rows = n_src * seg
    base_spec = lambda cols: pl.BlockSpec((base_rows, cols), lambda i, tab, ids, first: (tab[6, i], 0))
    over_spec = lambda cols: pl.BlockSpec((TILE, cols), lambda i, tab, ids, first: (tab[3, i], 0))
    hbm = pl.BlockSpec(memory_space=pl.ANY)
    return pl.pallas_call(
        grad_kernel,
        grid_spec=pltpu.PrefetchScalarGridSpec(
            num_scalar_prefetch=3,
            grid=(table.shape[1],),
            in_specs=[
                base_spec(d_model),
                base_spec(d_model),
                base_spec(d_ff),
                base_spec(d_ff),
                over_spec(d_model),
                over_spec(d_model),
                over_spec(d_ff),
                over_spec(d_ff),
                *[hbm for _ in base],
                hbm,
                pl.BlockSpec(wg.shape, lambda i, tab, ids, first: (0, 0)),
                hbm,
                hbm,
            ],
            out_specs=[hbm, hbm],
            scratch_shapes=[
                pltpu.VMEM((d_model, d_ff), F32),
                pltpu.VMEM((d_ff, d_model), F32),
                pltpu.VMEM((d_model, d_ff), BF16),
                pltpu.VMEM((d_ff, d_model), BF16),
                pltpu.VMEM((base_rows, d_ff), BF16),
                pltpu.VMEM((base_rows, d_ff), BF16),
                pltpu.VMEM((n_src, seg, width), BF16),
                pltpu.VMEM((TILE_GROUPS, GROUP, width), BF16),
                pltpu.SemaphoreType.DMA((2,)),
                pltpu.SemaphoreType.DMA,
                pltpu.SemaphoreType.DMA,
                pltpu.SemaphoreType.DMA((2,)),
            ],
        ),
        out_shape=[jax.ShapeDtypeStruct(w_up.shape, F32), jax.ShapeDtypeStruct(w_down.shape, F32)],
        compiler_params=pltpu.CompilerParams(vmem_limit_bytes=VMEM_BYTES, dimension_semantics=('arbitrary',)),
        cost_estimate=pl.CostEstimate(flops=70_000_000_000, bytes_accessed=150_000_000, transcendentals=8_000_000),
        name='grad_pass',
    )(table, ids, first_expert, *base_store, *over_store, *base, over, wg, w_up, w_down)


def overflow_spans(count_ref, local):
    groups = jnp.sum(count_ref[...].astype(F32), axis=(1, 2))
    over = jnp.maximum(groups - BASE_GROUPS, 0.0)
    lanes = over.shape[1]
    row, col = (lax.broadcasted_iota(I32, (lanes, lanes), d) for d in (0, 1))
    start = dot(over.astype(BF16), jnp.where(row < col, 1.0, 0.0).astype(BF16))
    tiles = jnp.ceil(jnp.sum(over, axis=0, keepdims=True) * (1.0 / TILE_GROUPS) - 1e-3)
    owner = dot(jnp.broadcast_to(tiles, over.shape).astype(BF16), jnp.where(row // local == col, 1.0, 0.0).astype(BF16))
    excess = jnp.max(jnp.maximum(start + over - OVER_GROUPS, owner - MAX_OVER_TILES))
    first = jnp.minimum(start, OVER_GROUPS)
    size = jnp.minimum(start + over, OVER_GROUPS) - first
    return size.astype(I32), first.astype(I32), excess


def fill_tiles(n_src, local, lead, size, first, write):
    firsts, tile = [], jnp.int32(0)
    for e in range(local):
        base = tile * TILE_GROUPS

        def per_source(s, at, e=e, base=base):
            begin = first[s, lead + e]

            def per_group(g, at):
                @pl.when(base + at < MAX_OVER_TILES * TILE_GROUPS)
                def _():
                    write(base + at, s, begin + g)

                return at + 1

            return lax.fori_loop(0, size[s, lead + e], per_group, at)

        total = lax.fori_loop(0, n_src, per_source, jnp.int32(0))
        tiles = jnp.minimum(lax.div(total + (TILE_GROUPS - 1), jnp.int32(TILE_GROUPS)), MAX_OVER_TILES - tile)
        firsts.append((tile, tiles, total))
        tile = tile + tiles
    return firsts, tile


def to_scalars(pairs, sems):
    copies = [pltpu.make_async_copy(v, m, sems.at[i]) for i, (v, m) in enumerate(pairs)]
    for copy in copies:
        copy.start()
    for copy in copies:
        copy.wait()


def own_plan_kernel(local, lead_ref, count_ref, tab_ref, ids_ref, back_ref, size_v, first_v, size_s, first_s, sems):
    size_v[...], first_v[...], _ = overflow_spans(count_ref, local)
    to_scalars([(size_v, size_s), (first_v, first_s)], sems)

    def write(at, s, g):
        ids_ref[at] = s * SENT_GROUPS + g
        back_ref[at] = s * OVER_GROUPS + g

    spans, n_tiles = fill_tiles(count_ref.shape[0], local, lead_ref[0], size_s, first_s, write)
    last = jnp.maximum(n_tiles - 1, 0)
    for t in range(MAX_OVER_TILES):
        tab_ref[0, t] = local - 1
        tab_ref[1, t] = 0
        tab_ref[2, t] = jnp.minimum(t, last)
        tab_ref[3, t] = (last == t).astype(I32)
    for e, (tile, tiles, total) in enumerate(spans):
        def body(k, left, e=e, tile=tile):
            tab_ref[0, tile + k] = e
            tab_ref[1, tile + k] = jnp.minimum(left, TILE_GROUPS)
            return left - TILE_GROUPS

        lax.fori_loop(0, tiles, body, total)


def grad_plan_kernel(local, lead_ref, own_ref, other_ref, tab_ref, ids_ref, fits_ref, size_v, first_v, size_s, first_s, sems):
    n_src = own_ref.shape[0]
    size_v[0], first_v[0], own_excess = overflow_spans(own_ref, local)
    size_v[1], first_v[1], other_excess = overflow_spans(other_ref, local)
    to_scalars([(size_v, size_s), (first_v, first_s)], sems)
    fits_ref[0] = (jnp.maximum(own_excess, other_excess) <= 0.0).astype(I32)

    def write(at, s, g):
        ids_ref[at] = s * SENT_GROUPS + g

    own, _ = fill_tiles(n_src, local, lead_ref[0], size_s.at[0], first_s.at[0], lambda at, s, g: None)
    other, _ = fill_tiles(n_src, local, lead_ref[0], size_s.at[1], first_s.at[1], write)
    max_steps = tab_ref.shape[1]
    for t in range(max_steps):
        tab_ref[1, t] = -1
        tab_ref[2, t] = 0
    step = jnp.int32(0)
    own_at = jnp.int32(0)

    def emit(step, expert, kind, own_tile, groups, other_tile, next_base):
        tab_ref[0, step] = expert
        tab_ref[1, step] = kind
        tab_ref[3, step] = jnp.clip(own_tile, 0, MAX_OVER_TILES - 1)
        tab_ref[4, step] = groups
        tab_ref[5, step] = other_tile
        tab_ref[6, step] = next_base

    for e in range(local):
        own_tile, own_tiles, _ = own[e]
        other_tile, other_tiles, total = other[e]
        after = min(e + 1, local - 1)
        emit(step, e, OWN_BASE, own_tile, 0, 0, e)

        def own_body(k, c, e=e, step=step, own_tile=own_tile, after=after):
            emit(step + 1 + k, e, OWN_OVER, own_tile + k, 0, 0, after)
            return c

        lax.fori_loop(0, own_tiles, own_body, 0)
        step = step + 1 + own_tiles
        own_at = own_tile + own_tiles
        emit(step, e, OTHER_BASE, own_at, 0, 0, after)

        def other_body(k, left, e=e, step=step, own_at=own_at, other_tile=other_tile, after=after):
            emit(step + 1 + k, e, OTHER_OVER, own_at, jnp.minimum(left, TILE_GROUPS), other_tile + k, after)
            return left - TILE_GROUPS

        lax.fori_loop(0, other_tiles, other_body, total)
        step = step + 1 + other_tiles
        tab_ref[2, step - 1] = 1

    def rest(t, c):
        emit(t, local - 1, -1, own_at, 0, 0, local - 1)
        return c

    lax.fori_loop(step, max_steps, rest, 0)


def plan_call(kernel, local, lead, counts, out_shapes, planes):
    n_src = counts[0].shape[0]
    smem = pl.BlockSpec(memory_space=pltpu.SMEM)
    spec = pl.BlockSpec((n_src, 1, GROUP, 128), lambda i: (0, OVER_GROUPS, 0, 0))
    shape = (n_src, 128) if planes == 1 else (planes, n_src, 128)
    return pl.pallas_call(
        functools.partial(kernel, local),
        grid=(1,),
        in_specs=[smem] + [spec] * len(counts),
        out_specs=[smem] * len(out_shapes),
        out_shape=[jax.ShapeDtypeStruct(o, I32) for o in out_shapes],
        scratch_shapes=[pltpu.VMEM(shape, I32), pltpu.VMEM(shape, I32), pltpu.SMEM(shape, I32), pltpu.SMEM(shape, I32),
                        pltpu.SemaphoreType.DMA((2,))],
    )(lead, *counts)


def padded_step(x_loc, gy_loc, idx_loc, w_gate, w_up, w_down, ep_size, dp_size):
    tok_count, d_model = x_loc.shape
    n_experts = w_gate.shape[1]
    local_experts = w_up.shape[0]
    cap_rows = PAD_FACTOR * tok_count // n_experts
    onehot = idx_loc[:, None] == jnp.arange(n_experts, dtype=I32)[None, :]
    expert_count = jnp.sum(onehot, axis=0, dtype=I32)
    sort_order = jnp.argsort(idx_loc, stable=True)
    sorted_pos = jnp.argsort(sort_order)
    expert_start = jnp.cumsum(expert_count) - expert_count
    slot_k = jnp.arange(cap_rows, dtype=I32)
    slot_valid = slot_k[None, :] < expert_count[:, None]
    src_tok = sort_order[jnp.minimum(expert_start[:, None] + slot_k[None, :], tok_count - 1)]
    slot_tok = idx_loc * cap_rows + sorted_pos - expert_start[idx_loc]

    def dispatch(tok_rows):
        picked = jnp.where(slot_valid[:, :, None], tok_rows[src_tok], jnp.zeros((), tok_rows.dtype))
        picked = picked.reshape(ep_size, local_experts, cap_rows, d_model)
        return lax.all_to_all(picked, 'ep', 0, 0, tiled=True)

    def combine(expert_rows):
        returned = lax.all_to_all(expert_rows, 'ep', 1, 0, tiled=True)
        return returned.reshape(n_experts * cap_rows, d_model)[slot_tok]

    router_logit = jnp.dot(x_loc, w_gate, preferred_element_type=F32)
    router_prob = jax.nn.softmax(router_logit, axis=-1)
    gate_val = n_experts * jnp.sum(jnp.where(onehot, router_prob, 0.0), axis=1)
    recv_rows = dispatch(x_loc)
    gy_full = gy_loc.astype(F32)
    dy_tok = (gate_val[:, None] * gy_full).astype(BF16)
    recv_grad = dispatch(dy_tok)

    def one_expert(carry, per_expert):
        rows, grad, up, down = per_expert
        rows, grad = rows.reshape(-1, d_model), grad.reshape(-1, d_model)
        pre_act = dot(rows, up)
        hid_full, gelu_back = jax.vjp(jax.nn.gelu, pre_act)
        hidden = hid_full.astype(BF16)
        out_rows = dot(hidden, down).astype(BF16)
        d_pre = gelu_back(dot(grad, down, ((1,), (1,))))[0].astype(BF16)
        grad_down = dot(hidden, grad, ((0,), (0,)))
        grad_up = dot(rows, d_pre, ((0,), (0,)))
        d_rows = dot(d_pre, up, ((1,), (1,))).astype(BF16)
        shape = (ep_size, cap_rows, d_model)
        return carry, (out_rows.reshape(shape), d_rows.reshape(shape), grad_up, grad_down)

    swap = lambda rows: jnp.swapaxes(rows, 0, 1)
    _, (expert_out, d_rows, grad_up, grad_down) = lax.scan(
        one_expert, 0, (swap(recv_rows), swap(recv_grad), w_up, w_down))
    y_tok = combine(expert_out)
    moe_out = (gate_val[:, None] * y_tok.astype(F32)).astype(BF16)
    dx_expert = combine(d_rows)
    d_gate = jnp.sum(gy_full * y_tok.astype(F32), axis=1)
    d_logit = ((d_gate * gate_val)[:, None] * (onehot.astype(F32) - router_prob)).astype(BF16)
    dx_router = dot(d_logit, w_gate, ((1,), (1,)))
    grad_x = (dx_expert.astype(F32) + dx_router).astype(BF16)
    grad_gate = dot(x_loc, d_logit, ((0,), (0,)))

    def sum_dp(term):
        total = term
        for shift in range(1, dp_size):
            total = total + lax.ppermute(term, 'dp', [(i, (i + shift) % dp_size) for i in range(dp_size)])
        return total

    return (moe_out, grad_x, sum_dp(grad_up), sum_dp(grad_down), lax.psum(grad_gate, ('dp', 'ep')))


def solution(mesh):
    dp_size, ep_size = mesh.shape['dp'], mesh.shape['ep']
    tok_spec = P(('dp', 'ep'), None)
    idx_spec = P(('dp', 'ep'))
    rep_spec = P(None, None)
    exp_spec = P('ep', None, None)
    swap = [(i, (i + 1) % dp_size) for i in range(dp_size)]

    def local_step(x, gy, idx, w_gate, w_up, w_down):
        _, d_model = x.shape
        n_experts = w_gate.shape[1]
        local = w_up.shape[0]
        width = 2 * d_model
        base_rows = BASE_GROUPS * GROUP
        n_base = n_experts * base_rows
        n_over = OVER_GROUPS * GROUP
        ep = lax.axis_index('ep')
        first_expert = (ep * local).astype(I32).reshape(1)

        my_groups, pos = token_positions(idx, n_experts, local)
        chunk_rows = n_base // CHUNKS
        slots = (ep_size, local // CHUNKS, base_rows, width)
        base, base_z = [], []
        for c in range(CHUNKS):
            sent = permute_rows(pos, x, gy, c * chunk_rows, chunk_rows)
            base.append(lax.all_to_all(sent.reshape(ep_size, -1, width), 'ep', 0, 0, tiled=True))
            base_z.append(lax.ppermute(base[c], 'dp', swap).reshape(slots))
        marks = jnp.pad(my_groups.astype(BF16)[None, :], ((0, GROUP - 1), (0, width - n_experts)))
        over_sent = permute_rows(pos, x, gy, n_base, n_over, marks).reshape(SENT_GROUPS, GROUP, width)
        over = lax.all_gather(over_sent, 'ep')
        over_sent_z = lax.ppermute(over_sent, 'dp', swap)
        over_z = lax.all_gather(over_sent_z, 'ep')

        n_ids = MAX_OVER_TILES * TILE_GROUPS
        table, ids, back_ids = plan_call(own_plan_kernel, local, first_expert, [over],
                                         [(4, MAX_OVER_TILES), (n_ids,), (n_ids,)], 1)
        gtable, ids_z, fits = plan_call(grad_plan_kernel, local, first_expert, [over, over_z],
                                        [(7, 2 * (local + MAX_OVER_TILES)), (n_ids,), (1,)], 2)
        over_shape = (ep_size * OVER_GROUPS, GROUP, width)
        over = over.reshape(-1, GROUP, width)
        over_z = over_z.reshape(-1, GROUP, width)
        dwg = jnp.zeros((n_experts, d_model), F32)
        stores = None
        for c in range(CHUNKS):
            kept = own_base_pass(first_expert, c, base[c].reshape(slots), w_gate, w_up, w_down, dwg, stores, over_shape)
            dwg = kept[5]
            stores = kept[:5] + kept[6:]
        od, *base_store, zero_od = stores
        base_back = lax.all_to_all(od.reshape(ep_size, -1, width), 'ep', 0, 0, tiled=True)
        od_over, x_o, dy_o, h_o, da_o, dwg = own_over_pass(table, ids, back_ids, first_expert, over, w_gate, w_up, w_down,
                                                          dwg, zero_od)
        over_back = lax.psum_scatter(od_over.reshape(ep_size, OVER_GROUPS, GROUP, width), 'ep', scatter_dimension=0)
        d_up, d_down = grad_pass(gtable, ids_z, first_expert, base_store, (x_o, dy_o, h_o, da_o), base_z, over_z,
                                 w_gate, w_up, w_down)
        d_gate = jnp.sum(lax.all_gather(dwg, ('dp', 'ep')), axis=0).T
        moe_out, grad_x = unpermute_rows(pos, base_back, over_back.reshape(n_over, width))
        sparse = (moe_out, grad_x, d_up, d_down, d_gate)

        def dense(carry):
            del carry
            return (jnp.array(True),) + padded_step(x, gy, idx, w_gate, w_up, w_down, ep_size, dp_size)

        return lax.while_loop(lambda carry: jnp.logical_not(carry[0]), dense, (fits[0] == 1,) + sparse)[1:]

    return jax.shard_map(
        local_step, mesh=mesh, in_specs=(tok_spec, tok_spec, idx_spec, rep_spec, exp_spec, exp_spec),
        out_specs=(tok_spec, tok_spec, exp_spec, exp_spec, rep_spec), check_vma=False)
```

```python
import functools

import jax
import jax.numpy as jnp
from jax import lax
from jax.experimental import pallas as pl
from jax.experimental.pallas import tpu as pltpu
from jax.sharding import PartitionSpec as P


PAD_FACTOR = 4
GROUP = 8
BASE_GROUPS = 7
OVER_GROUPS = 50
SENT_GROUPS = OVER_GROUPS + 1
MAX_OVER_TILES = 8
RUNS = 8
RUN_SIZES = (16, 8, 4, 2, 1)
TILE_GROUPS = 26
TILE = TILE_GROUPS * GROUP
PERM_TILE = 256
CHUNK = 512
ROW_CHUNK = 256
CHUNKS = 2
SQRT_2_PI = 0.7978845608028654
CUBIC = 0.044715
VMEM_BYTES = 67_043_328

F32 = jnp.float32
BF16 = jnp.bfloat16
I32 = jnp.int32


def dot(a, b, dims=((1,), (0,))):
    return lax.dot_general(a, b, (dims, ((), ())), preferred_element_type=F32)


def exclusive_cumsum(v, axis):
    return jnp.cumsum(v, axis=axis) - v


def token_positions(idx, n_experts, local):
    tok_count = idx.shape[0]
    block = 128
    base_rows = BASE_GROUPS * GROUP
    onehot = (idx[:, None] == jnp.arange(n_experts, dtype=I32)[None, :]).astype(BF16)
    blocks = onehot.reshape(tok_count // block, block, n_experts)
    lower = jnp.tril(jnp.ones((block, block), BF16))
    inclusive = jnp.einsum('ij,bje->bie', lower, blocks, preferred_element_type=F32)
    totals = jnp.sum(blocks.astype(F32), axis=1)
    counts = jnp.sum(totals, axis=0).astype(I32)
    groups = (counts + GROUP - 1) // GROUP
    over = jnp.maximum(groups - BASE_GROUPS, 0)
    over_start = exclusive_cumsum(over, 0)
    rank = inclusive + (exclusive_cumsum(totals, 0) - 1.0)[:, None, :]
    expert = jnp.arange(n_experts, dtype=I32)
    per_chunk = local // CHUNKS
    slot = (expert % local // per_chunk) * (n_experts // CHUNKS) + expert // local * per_chunk + expert % per_chunk
    base_at = (slot * base_rows).astype(F32)
    over_at = (n_experts * base_rows - base_rows + over_start * GROUP).astype(F32)
    row = jnp.sum(blocks.astype(F32) * (rank + jnp.where(rank < base_rows, base_at, over_at)), axis=2)
    return groups, row.reshape(tok_count).astype(I32)


def permute_kernel(pos_ref, x_ref, gy_ref, *refs):
    *tail, out_ref = refs
    d_model = x_ref.shape[1]
    rows = out_ref.shape[0] - sum(t.shape[0] for t in tail)
    row_id = pl.program_id(0) * rows + lax.broadcasted_iota(I32, (rows, x_ref.shape[0]), 0)
    select = jnp.where(row_id == pos_ref[...], 1.0, 0.0).astype(BF16)
    out_ref[:rows, :d_model] = dot(select, x_ref[...]).astype(BF16)
    out_ref[:rows, d_model:] = dot(select, gy_ref[...]).astype(BF16)
    for t in tail:
        out_ref[rows:, :] = t[...]


def permute_rows(pos, x, gy, first_row, n_rows, *tail):
    tok_count, d_model = x.shape
    tile = n_rows if n_rows % PERM_TILE else PERM_TILE
    extra = sum(t.shape[0] for t in tail)
    return pl.pallas_call(
        permute_kernel,
        grid=(n_rows // tile,),
        in_specs=[
            pl.BlockSpec((1, tok_count), lambda i: (0, 0)),
            pl.BlockSpec((tok_count, d_model), lambda i: (0, 0)),
            pl.BlockSpec((tok_count, d_model), lambda i: (0, 0)),
        ] + [pl.BlockSpec(t.shape, lambda i: (0, 0)) for t in tail],
        out_specs=pl.BlockSpec((tile + extra, 2 * d_model), lambda i: (i, 0)),
        out_shape=jax.ShapeDtypeStruct((n_rows + extra, 2 * d_model), BF16),
        cost_estimate=pl.CostEstimate(flops=4 * n_rows * tok_count * d_model, bytes_accessed=16_000_000, transcendentals=0),
        name='permute',
    )((pos - first_row).reshape(1, tok_count), x, gy, *tail)


def unpermute_kernel(pos_ref, *refs):
    *parts, out_ref, dx_ref = refs
    toks, d_model = out_ref.shape
    pos = jnp.transpose(jnp.broadcast_to(pos_ref[...], (8, toks)))[:, :1]
    first, out, dx = 0, 0.0, 0.0
    for part in parts:
        rows = part[...].reshape(-1, 2 * d_model)
        row_id = lax.broadcasted_iota(I32, (toks, rows.shape[0]), 1) + first
        select = jnp.where(row_id == pos, 1.0, 0.0).astype(BF16)
        out += dot(select, rows[:, :d_model])
        dx += dot(select, rows[:, d_model:])
        first += rows.shape[0]
    out_ref[...] = out.astype(BF16)
    dx_ref[...] = dx.astype(BF16)


def unpermute_rows(pos, base, over):
    n_own, n_slot, width = base.shape
    tok_count = pos.shape[0]
    d_model = width // 2
    shape = jax.ShapeDtypeStruct((tok_count, d_model), BF16)
    chunk = (n_own, n_slot // CHUNKS, width)
    return pl.pallas_call(
        unpermute_kernel,
        grid=(tok_count // PERM_TILE,),
        in_specs=[pl.BlockSpec((1, PERM_TILE), lambda i: (0, i))]
        + [pl.BlockSpec(chunk, lambda i, c=c: (0, c, 0)) for c in range(CHUNKS)]
        + [pl.BlockSpec(over.shape, lambda i: (0, 0))],
        out_specs=[pl.BlockSpec((PERM_TILE, d_model), lambda i: (i, 0))] * 2,
        out_shape=[shape, shape],
        cost_estimate=pl.CostEstimate(flops=14_000_000_000, bytes_accessed=16_000_000, transcendentals=0),
        name='unpermute',
    )(pos.reshape(1, tok_count), *[base] * CHUNKS, over)


def gate(x, wg, expert):
    logit = dot(x, wg)
    unnorm = jnp.exp(logit - jnp.max(logit, axis=1, keepdims=True))
    prob = unnorm / jnp.sum(unnorm, axis=1, keepdims=True)
    onehot = lax.broadcasted_iota(I32, prob.shape, 1) == expert
    gate_val = prob.shape[1] * jnp.sum(jnp.where(onehot, prob, 0.0), axis=1, keepdims=True)
    return prob, onehot, gate_val


def activations(x, dy, w_up, w_down, cols):
    a = dot(x, w_up[:, cols])
    dh = dot(dy, w_down[cols, :], ((1,), (1,)))
    cubic = (SQRT_2_PI * CUBIC) * (a * a)
    half = 0.5 + 0.5 * jnp.tanh(a * (SQRT_2_PI + cubic))
    h = a * half
    slope = half + (h - h * half) * (2.0 * SQRT_2_PI + 6.0 * cubic)
    return h.astype(BF16), (slope * dh).astype(BF16)


def own_rows_step(x, gy, expert, wg_ref, w_up, w_down, store, dwg_ref):
    dy_ref, h_ref, da_ref = store
    prob, onehot, gate_val = gate(x, wg_ref[...], expert)
    gy_full = gy.astype(F32)
    dy = (gate_val * gy_full).astype(BF16)
    dy_ref[...] = dy
    for lo in range(0, h_ref.shape[1], ROW_CHUNK):
        cols = pl.ds(lo, ROW_CHUNK)
        h, da = activations(x, dy, w_up, w_down, cols)
        h_ref[:, cols] = h
        da_ref[:, cols] = da
    y = dot(h_ref[...], w_down[...]).astype(BF16).astype(F32)
    dxe = dot(da_ref[...], w_up[...], ((1,), (1,))).astype(BF16).astype(F32)
    d_gate = jnp.sum(gy_full * y, axis=1, keepdims=True)
    d_logit = ((d_gate * gate_val) * (onehot.astype(F32) - prob)).astype(BF16)
    dwg_ref[...] += dot(d_logit, x, ((0,), (0,)))
    out = (gate_val * y).astype(BF16)
    dx = (dxe + dot(d_logit, wg_ref[...], ((1,), (1,)))).astype(BF16)
    return out, dx


def own_base_kernel(first_ref, rows_ref, wg_ref, up_ref, down_ref, dwg_in, *refs):
    od_ref, x_ref, dy_ref, h_ref, da_ref, dwg_ref, zero_ref = refs[-7:]
    step = pl.program_id(0)
    d_model = wg_ref.shape[0]

    @pl.when(step == 0)
    def _():
        dwg_ref[...] = dwg_in[...]

    zero_ref[...] = jnp.zeros_like(zero_ref)
    rows = rows_ref[...].reshape(dy_ref.shape[0], 2 * d_model)
    x = rows[:, :d_model]
    x_ref[...] = x
    out, dx = own_rows_step(x, rows[:, d_model:], first_ref[0] + step, wg_ref, up_ref.at[0], down_ref.at[0],
                            (dy_ref, h_ref, da_ref), dwg_ref)
    block = od_ref.shape[:3] + (d_model,)
    od_ref[:, :, :, :d_model] = out.reshape(block)
    od_ref[:, :, :, d_model:] = dx.reshape(block)


def own_base_pass(first_expert, chunk, rows, wg, w_up, w_down, dwg, stores, over_shape):
    n_src, count, seg, width = rows.shape
    local, d_model, d_ff = w_up.shape
    tile = n_src * seg
    lead = chunk * count
    row_spec = lambda at: pl.BlockSpec((n_src, 1, seg, width), lambda e, first: (0, at + e, 0, 0))
    store_spec = lambda cols: pl.BlockSpec((tile, cols), lambda e, first: (lead + e, 0))
    const = lambda e, first: (0, 0)
    rows_of = lambda cols: jax.ShapeDtypeStruct((local * tile, cols), BF16)
    zero_block = (over_shape[0] // local,) + over_shape[1:]
    kept = [] if stores is None else list(stores)
    return pl.pallas_call(
        own_base_kernel,
        grid_spec=pltpu.PrefetchScalarGridSpec(
            num_scalar_prefetch=1,
            grid=(count,),
            in_specs=[
                row_spec(0),
                pl.BlockSpec(wg.shape, const),
                pl.BlockSpec((1, d_model, d_ff), lambda e, first: (lead + e, 0, 0)),
                pl.BlockSpec((1, d_ff, d_model), lambda e, first: (lead + e, 0, 0)),
                pl.BlockSpec(dwg.shape, const),
            ] + [pl.BlockSpec(memory_space=pl.ANY)] * len(kept),
            out_specs=[row_spec(lead), store_spec(d_model), store_spec(d_model), store_spec(d_ff), store_spec(d_ff),
                       pl.BlockSpec(dwg.shape, const), pl.BlockSpec(zero_block, lambda e, first: (lead + e, 0, 0))],
        ),
        out_shape=[jax.ShapeDtypeStruct((n_src, local, seg, width), BF16), rows_of(d_model), rows_of(d_model), rows_of(d_ff), rows_of(d_ff),
                   jax.ShapeDtypeStruct(dwg.shape, F32), jax.ShapeDtypeStruct(over_shape, BF16)],
        input_output_aliases={6 + i: o for i, o in zip(range(len(kept)), (0, 1, 2, 3, 4, 6))},
        compiler_params=pltpu.CompilerParams(vmem_limit_bytes=VMEM_BYTES, dimension_semantics=('arbitrary',)),
        cost_estimate=pl.CostEstimate(flops=8_500_000_000 * count, bytes_accessed=20_000_000 * count,
                                      transcendentals=1_500_000 * count),
        name='own_base',
    )(first_expert + lead, rows, wg, w_up, w_down, dwg, *kept)


def run_copies(runs_ref, tile, n_runs, hbm, buf, sem, to_hbm):
    def body(r, carry):
        at = (tile * RUNS + r) * 3
        first, left, slot = runs_ref[at], runs_ref[at + 1], runs_ref[at + 2]
        for size in RUN_SIZES:
            take = left >= size

            @pl.when(take)
            def _(first=first, slot=slot, size=size):
                ends = (hbm.at[pl.ds(first, size)], buf.at[pl.ds(slot, size)])
                pltpu.make_async_copy(*(ends[::-1] if to_hbm else ends), sem).start()

            step = jnp.where(take, size, 0)
            first, slot, left = first + step, slot + step, left - step
        return carry

    lax.fori_loop(0, n_runs, body, 0)


def run_waits(count, hbm, buf, sem, to_hbm):
    for size in RUN_SIZES:
        @pl.when((count & size) != 0)
        def _(size=size):
            ends = (hbm.at[pl.ds(0, size)], buf.at[pl.ds(0, size)])
            pltpu.make_async_copy(*(ends[::-1] if to_hbm else ends), sem).wait()


def tile_rows(buf, count):
    rows = buf[...].reshape(TILE, buf.shape[-1])
    row_id = lax.broadcasted_iota(I32, rows.shape, 0)
    return jnp.where(row_id < count * GROUP, rows, jnp.zeros((), rows.dtype))


def own_over_kernel(tab_ref, runs_ref, first_ref, rows_hbm, wg_ref, up_ref, down_ref, dwg_in, zero_od,
                    od_hbm, x_ref, dy_ref, h_ref, da_ref, dwg_ref, in_buf, out_buf, in_sem, out_sem):
    del zero_od
    step = pl.program_id(0)
    d_model = wg_ref.shape[0]
    slot = step % 2
    count = tab_ref[1, step]

    @pl.when(step == 0)
    def _():
        dwg_ref[...] = dwg_in[...]
        run_copies(runs_ref, 0, tab_ref[4, 0], rows_hbm, in_buf.at[0], in_sem.at[0], False)

    @pl.when(count > 0)
    def _():
        run_waits(count, rows_hbm, in_buf.at[slot], in_sem.at[slot], False)

        @pl.when(step + 1 < pl.num_programs(0))
        def _():
            run_copies(runs_ref, step + 1, tab_ref[4, step + 1], rows_hbm, in_buf.at[1 - slot], in_sem.at[1 - slot], False)

        rows = tile_rows(in_buf.at[slot], count)
        x = rows[:, :d_model]
        x_ref[...] = x
        out, dx = own_rows_step(x, rows[:, d_model:], first_ref[0] + tab_ref[0, step], wg_ref,
                                up_ref.at[0], down_ref.at[0], (dy_ref, h_ref, da_ref), dwg_ref)

        @pl.when(step > 0)
        def _():
            run_waits(tab_ref[1, step - 1], od_hbm, out_buf, out_sem, True)

        out_buf[:, :, :d_model] = out.reshape(TILE_GROUPS, GROUP, d_model)
        out_buf[:, :, d_model:] = dx.reshape(TILE_GROUPS, GROUP, d_model)
        run_copies(runs_ref, step, tab_ref[4, step], od_hbm, out_buf, out_sem, True)

        @pl.when(tab_ref[3, step] == 1)
        def _():
            run_waits(count, od_hbm, out_buf, out_sem, True)


def own_over_pass(table, runs, first_expert, rows, wg, w_up, w_down, dwg, zero_od):
    d_model, d_ff = w_up.shape[1], w_up.shape[2]
    width = rows.shape[-1]
    n_tiles = table.shape[1]
    hbm = pl.BlockSpec(memory_space=pl.ANY)
    const = lambda i, tab, runs, first: (0, 0)
    store_spec = lambda cols: pl.BlockSpec((TILE, cols), lambda i, tab, runs, first: (tab[2, i], 0))
    rows_of = lambda cols: jax.ShapeDtypeStruct((n_tiles * TILE, cols), BF16)
    return pl.pallas_call(
        own_over_kernel,
        grid_spec=pltpu.PrefetchScalarGridSpec(
            num_scalar_prefetch=3,
            grid=(n_tiles,),
            in_specs=[
                hbm,
                pl.BlockSpec(wg.shape, const),
                pl.BlockSpec((1, d_model, d_ff), lambda i, tab, runs, first: (tab[0, i], 0, 0)),
                pl.BlockSpec((1, d_ff, d_model), lambda i, tab, runs, first: (tab[0, i], 0, 0)),
                pl.BlockSpec(dwg.shape, const),
                hbm,
            ],
            out_specs=[hbm, store_spec(d_model), store_spec(d_model), store_spec(d_ff), store_spec(d_ff),
                       pl.BlockSpec(dwg.shape, const)],
            scratch_shapes=[
                pltpu.VMEM((2, TILE_GROUPS, GROUP, width), BF16),
                pltpu.VMEM((TILE_GROUPS, GROUP, width), BF16),
                pltpu.SemaphoreType.DMA((2,)),
                pltpu.SemaphoreType.DMA,
            ],
        ),
        out_shape=[jax.ShapeDtypeStruct(zero_od.shape, BF16), rows_of(d_model), rows_of(d_model), rows_of(d_ff),
                   rows_of(d_ff), jax.ShapeDtypeStruct(dwg.shape, F32)],
        input_output_aliases={8: 0},
        compiler_params=pltpu.CompilerParams(vmem_limit_bytes=VMEM_BYTES, dimension_semantics=('arbitrary',)),
        cost_estimate=pl.CostEstimate(flops=10_000_000_000, bytes_accessed=40_000_000, transcendentals=2_000_000),
        name='own_over',
    )(table, runs, first_expert, rows, wg, w_up, w_down, dwg, zero_od)


OWN_BASE, OWN_OVER, OTHER_BASE, OTHER_OVER = range(4)


def grad_kernel(tab_ref, runs_ref, first_ref, xb_ref, dyb_ref, hb_ref, dab_ref, xo_ref, dyo_ref, ho_ref, dao_ref, *refs):
    *base_hbm, over_hbm, wg_ref, up_hbm, down_hbm, dup_hbm, ddown_hbm = refs[:-12]
    dup, ddown, up_buf, down_buf, h_buf, da_buf, base_buf, in_buf, w_sems, base_sem, in_sem, out_sems = refs[-12:]
    step = pl.program_id(0)
    d_model, d_ff = dup.shape
    expert, kind, last, count = tab_ref[0, step], tab_ref[1, step], tab_ref[2, step], tab_ref[4, step]
    n_local = dup_hbm.shape[0]
    base_rows = h_buf.shape[0]

    def weights(e):
        return (pltpu.make_async_copy(up_hbm.at[e], up_buf, w_sems.at[0]),
                pltpu.make_async_copy(down_hbm.at[e], down_buf, w_sems.at[1]))

    def flush_down(e):
        return pltpu.make_async_copy(ddown, ddown_hbm.at[e], out_sems.at[0])

    def flush_up(e):
        return pltpu.make_async_copy(dup, dup_hbm.at[e], out_sems.at[1])

    def add_down(dy, h_src, add):
        for lo in range(0, d_ff, CHUNK):
            cols = pl.ds(lo, CHUNK)
            term = dot(h_src[:, cols], dy, ((0,), (0,)))
            ddown[cols, :] = ddown[cols, :] + term if add else term

    def add_up(x, da_src, add):
        for lo in range(0, d_ff, CHUNK):
            cols = pl.ds(lo, CHUNK)
            term = dot(x, da_src[:, cols], ((0,), (0,)))
            dup[:, cols] = dup[:, cols] + term if add else term

    def accumulate(x, dy, h_src, da_src):
        add_down(dy, h_src, True)

        @pl.when(last == 1)
        def _():
            flush_down(expert).start()

        add_up(x, da_src, True)

        @pl.when(last == 1)
        def _():
            flush_up(expert).start()

            @pl.when(expert + 1 < n_local)
            def _():
                for copy in weights(expert + 1):
                    copy.start()

            @pl.when(expert + 1 == n_local)
            def _():
                flush_down(expert).wait()
                flush_up(expert).wait()

    def base_copy(e):
        chunk = base_hbm[e // base_hbm[0].shape[1]]
        return pltpu.make_async_copy(chunk.at[:, e % chunk.shape[1]], base_buf, base_sem)

    ahead = step + 1
    ahead_at = jnp.minimum(ahead, pl.num_programs(0) - 1)

    @pl.when((ahead < pl.num_programs(0)) & (tab_ref[1, ahead_at] == OTHER_OVER))
    def _():
        run_copies(runs_ref, tab_ref[5, ahead_at], tab_ref[7, ahead_at], over_hbm, in_buf.at[ahead % 2], in_sem.at[ahead % 2],
                   False)

    @pl.when(kind == OWN_BASE)
    def _():
        for e in range(n_local):
            @pl.when(expert == e)
            def _():
                base_copy(e).start()

        @pl.when(expert == 0)
        def _():
            for copy in weights(0):
                copy.start()

        @pl.when(expert > 0)
        def _():
            flush_down(expert - 1).wait()

        add_down(dyb_ref[...], hb_ref, False)

        @pl.when(expert > 0)
        def _():
            flush_up(expert - 1).wait()

        add_up(xb_ref[...], dab_ref, False)

    @pl.when(kind == OWN_OVER)
    def _():
        add_down(dyo_ref[...], ho_ref, True)
        add_up(xo_ref[...], dao_ref, True)

    def other_rows(rows, n_rows):
        x, gy = rows[:, :d_model], rows[:, d_model:]
        _, _, gate_val = gate(x, wg_ref[...], first_ref[0] + expert)
        dy = (gate_val * gy.astype(F32)).astype(BF16)
        h_dst, da_dst = h_buf.at[:n_rows], da_buf.at[:n_rows]
        for lo in range(0, d_ff, ROW_CHUNK):
            cols = pl.ds(lo, ROW_CHUNK)
            h, da = activations(x, dy, up_buf, down_buf, cols)
            h_dst[:, cols] = h
            da_dst[:, cols] = da
        accumulate(x, dy, h_dst, da_dst)

    @pl.when(kind == OTHER_BASE)
    def _():
        for copy in weights(expert):
            copy.wait()
        base_copy(0).wait()
        other_rows(base_buf[...].reshape(base_rows, 2 * d_model), base_rows)

    @pl.when(kind == OTHER_OVER)
    def _():
        run_waits(count, over_hbm, in_buf.at[step % 2], in_sem.at[step % 2], False)
        other_rows(tile_rows(in_buf.at[step % 2], count), TILE)


def grad_pass(table, ids, first_expert, base_store, over_store, base, over, wg, w_up, w_down):
    n_src, _, seg, width = base[0].shape
    d_model, d_ff = w_up.shape[1], w_up.shape[2]
    base_rows = n_src * seg
    base_spec = lambda cols: pl.BlockSpec((base_rows, cols), lambda i, tab, ids, first: (tab[6, i], 0))
    over_spec = lambda cols: pl.BlockSpec((TILE, cols), lambda i, tab, ids, first: (tab[3, i], 0))
    hbm = pl.BlockSpec(memory_space=pl.ANY)
    return pl.pallas_call(
        grad_kernel,
        grid_spec=pltpu.PrefetchScalarGridSpec(
            num_scalar_prefetch=3,
            grid=(table.shape[1],),
            in_specs=[
                base_spec(d_model),
                base_spec(d_model),
                base_spec(d_ff),
                base_spec(d_ff),
                over_spec(d_model),
                over_spec(d_model),
                over_spec(d_ff),
                over_spec(d_ff),
                *[hbm for _ in base],
                hbm,
                pl.BlockSpec(wg.shape, lambda i, tab, ids, first: (0, 0)),
                hbm,
                hbm,
            ],
            out_specs=[hbm, hbm],
            scratch_shapes=[
                pltpu.VMEM((d_model, d_ff), F32),
                pltpu.VMEM((d_ff, d_model), F32),
                pltpu.VMEM((d_model, d_ff), BF16),
                pltpu.VMEM((d_ff, d_model), BF16),
                pltpu.VMEM((base_rows, d_ff), BF16),
                pltpu.VMEM((base_rows, d_ff), BF16),
                pltpu.VMEM((n_src, seg, width), BF16),
                pltpu.VMEM((2, TILE_GROUPS, GROUP, width), BF16),
                pltpu.SemaphoreType.DMA((2,)),
                pltpu.SemaphoreType.DMA,
                pltpu.SemaphoreType.DMA((2,)),
                pltpu.SemaphoreType.DMA((2,)),
            ],
        ),
        out_shape=[jax.ShapeDtypeStruct(w_up.shape, F32), jax.ShapeDtypeStruct(w_down.shape, F32)],
        compiler_params=pltpu.CompilerParams(vmem_limit_bytes=VMEM_BYTES, dimension_semantics=('arbitrary',)),
        cost_estimate=pl.CostEstimate(flops=70_000_000_000, bytes_accessed=150_000_000, transcendentals=8_000_000),
        name='grad_pass',
    )(table, ids, first_expert, *base_store, *over_store, *base, over, wg, w_up, w_down)


def overflow_spans(count_ref, local):
    groups = jnp.sum(count_ref[...].astype(F32), axis=(1, 2))
    over = jnp.maximum(groups - BASE_GROUPS, 0.0)
    lanes = over.shape[1]
    row, col = (lax.broadcasted_iota(I32, (lanes, lanes), d) for d in (0, 1))
    start = dot(over.astype(BF16), jnp.where(row < col, 1.0, 0.0).astype(BF16))
    tiles = jnp.ceil(jnp.sum(over, axis=0, keepdims=True) * (1.0 / TILE_GROUPS) - 1e-3)
    owner = dot(jnp.broadcast_to(tiles, over.shape).astype(BF16), jnp.where(row // local == col, 1.0, 0.0).astype(BF16))
    excess = jnp.max(jnp.maximum(start + over - OVER_GROUPS, owner - MAX_OVER_TILES))
    first = jnp.minimum(start, OVER_GROUPS)
    size = jnp.minimum(start + over, OVER_GROUPS) - first
    return size.astype(I32), first.astype(I32), excess


def fill_tiles(n_src, local, lead, size, first, runs, n_runs, count):
    for t in range(MAX_OVER_TILES):
        n_runs[t] = 0
        count[t] = 0

    def put(tile, slot, begin, groups):
        @pl.when((groups > 0) & (tile < MAX_OVER_TILES))
        def _():
            at = (tile * RUNS + n_runs[tile]) * 3
            runs[at] = begin
            runs[at + 1] = groups
            runs[at + 2] = slot
            n_runs[tile] = n_runs[tile] + 1
            count[tile] = count[tile] + groups

    spans, tile = [], jnp.int32(0)
    for e in range(local):
        def per_source(s, where, e=e):
            tile, slot = where
            groups = size[s, lead + e]
            begin = s * SENT_GROUPS + first[s, lead + e]
            head = jnp.minimum(groups, TILE_GROUPS - slot)
            rest = groups - head
            put(tile, slot, begin, head)
            put(tile + 1, 0, begin + head, rest)
            full = (slot + head == TILE_GROUPS).astype(I32)
            return tile + full, jnp.where(full == 1, rest, slot + head)

        end, slot = lax.fori_loop(0, n_src, per_source, (tile, jnp.int32(0)))
        end = jnp.minimum(end + (slot > 0).astype(I32), MAX_OVER_TILES)
        spans.append((tile, end - tile))
        tile = end
    return spans, tile


def to_scalars(pairs, sems):
    copies = [pltpu.make_async_copy(v, m, sems.at[i]) for i, (v, m) in enumerate(pairs)]
    for copy in copies:
        copy.start()
    for copy in copies:
        copy.wait()


def own_plan_kernel(local, lead_ref, count_ref, tab_ref, runs_ref, size_v, first_v, size_s, first_s, n_runs, count, sems):
    size_v[...], first_v[...], _ = overflow_spans(count_ref, local)
    to_scalars([(size_v, size_s), (first_v, first_s)], sems)
    spans, n_tiles = fill_tiles(count_ref.shape[0], local, lead_ref[0], size_s, first_s, runs_ref, n_runs.at[0], count.at[0])
    last = jnp.maximum(n_tiles - 1, 0)
    for t in range(MAX_OVER_TILES):
        tab_ref[0, t] = local - 1
        tab_ref[1, t] = count[0, t]
        tab_ref[2, t] = jnp.minimum(t, last)
        tab_ref[3, t] = (last == t).astype(I32)
        tab_ref[4, t] = n_runs[0, t]
    for e, (tile, tiles) in enumerate(spans):
        def body(k, c, e=e, tile=tile):
            tab_ref[0, tile + k] = e
            return c

        lax.fori_loop(0, tiles, body, 0)


def grad_plan_kernel(local, lead_ref, own_ref, other_ref, tab_ref, runs_ref, fits_ref, size_v, first_v, size_s, first_s,
                     n_runs, count, sems):
    n_src = own_ref.shape[0]
    size_v[0], first_v[0], own_excess = overflow_spans(own_ref, local)
    size_v[1], first_v[1], other_excess = overflow_spans(other_ref, local)
    to_scalars([(size_v, size_s), (first_v, first_s)], sems)
    fits_ref[0] = (jnp.maximum(own_excess, other_excess) <= 0.0).astype(I32)
    lead = lead_ref[0]
    own, n_tiles = fill_tiles(n_src, local, lead, size_s.at[0], first_s.at[0], runs_ref, n_runs.at[0], count.at[0])
    other, _ = fill_tiles(n_src, local, lead, size_s.at[1], first_s.at[1], runs_ref, n_runs.at[1], count.at[1])
    max_steps = tab_ref.shape[1]

    def emit(step, expert, kind, own_tile, other_tile, next_base):
        over = (kind == OTHER_OVER).astype(I32) if not isinstance(kind, int) else int(kind == OTHER_OVER)
        tab_ref[0, step] = expert
        tab_ref[1, step] = kind
        tab_ref[2, step] = 0
        tab_ref[3, step] = jnp.clip(own_tile, 0, MAX_OVER_TILES - 1)
        tab_ref[4, step] = count[1, other_tile] * over
        tab_ref[5, step] = other_tile
        tab_ref[6, step] = next_base
        tab_ref[7, step] = n_runs[1, other_tile] * over

    step = jnp.int32(0)
    for e in range(local):
        own_tile, own_tiles = own[e]
        other_tile, other_tiles = other[e]
        after = min(e + 1, local - 1)
        emit(step, e, OWN_BASE, own_tile, 0, e)

        def own_body(k, c, e=e, step=step, own_tile=own_tile, after=after):
            emit(step + 1 + k, e, OWN_OVER, own_tile + k, 0, after)
            return c

        lax.fori_loop(0, own_tiles, own_body, 0)
        step = step + 1 + own_tiles
        own_at = own_tile + own_tiles
        emit(step, e, OTHER_BASE, own_at, 0, after)

        def other_body(k, c, e=e, step=step, own_at=own_at, other_tile=other_tile, after=after):
            emit(step + 1 + k, e, OTHER_OVER, own_at, other_tile + k, after)
            return c

        lax.fori_loop(0, other_tiles, other_body, 0)
        step = step + 1 + other_tiles
        tab_ref[2, step - 1] = 1

    def dead(t, c):
        emit(t, local - 1, -1, n_tiles - 1, 0, local - 1)
        return c

    lax.fori_loop(step, max_steps, dead, 0)


def plan_call(kernel, local, lead, counts, out_shapes, planes):
    n_src = counts[0].shape[0]
    smem = pl.BlockSpec(memory_space=pltpu.SMEM)
    spec = pl.BlockSpec((n_src, 1, GROUP, 128), lambda i: (0, OVER_GROUPS, 0, 0))
    shape = (n_src, 128) if planes == 1 else (planes, n_src, 128)
    return pl.pallas_call(
        functools.partial(kernel, local),
        grid=(1,),
        in_specs=[smem] + [spec] * len(counts),
        out_specs=[smem] * len(out_shapes),
        out_shape=[jax.ShapeDtypeStruct(o, I32) for o in out_shapes],
        scratch_shapes=[pltpu.VMEM(shape, I32), pltpu.VMEM(shape, I32), pltpu.SMEM(shape, I32), pltpu.SMEM(shape, I32),
                        pltpu.SMEM((planes, MAX_OVER_TILES), I32), pltpu.SMEM((planes, MAX_OVER_TILES), I32),
                        pltpu.SemaphoreType.DMA((2,))],
    )(lead, *counts)


def padded_step(x_loc, gy_loc, idx_loc, w_gate, w_up, w_down, ep_size, dp_size):
    tok_count, d_model = x_loc.shape
    n_experts = w_gate.shape[1]
    local_experts = w_up.shape[0]
    cap_rows = PAD_FACTOR * tok_count // n_experts
    onehot = idx_loc[:, None] == jnp.arange(n_experts, dtype=I32)[None, :]
    expert_count = jnp.sum(onehot, axis=0, dtype=I32)
    sort_order = jnp.argsort(idx_loc, stable=True)
    sorted_pos = jnp.argsort(sort_order)
    expert_start = jnp.cumsum(expert_count) - expert_count
    slot_k = jnp.arange(cap_rows, dtype=I32)
    slot_valid = slot_k[None, :] < expert_count[:, None]
    src_tok = sort_order[jnp.minimum(expert_start[:, None] + slot_k[None, :], tok_count - 1)]
    slot_tok = idx_loc * cap_rows + sorted_pos - expert_start[idx_loc]

    def dispatch(tok_rows):
        picked = jnp.where(slot_valid[:, :, None], tok_rows[src_tok], jnp.zeros((), tok_rows.dtype))
        picked = picked.reshape(ep_size, local_experts, cap_rows, d_model)
        return lax.all_to_all(picked, 'ep', 0, 0, tiled=True)

    def combine(expert_rows):
        returned = lax.all_to_all(expert_rows, 'ep', 1, 0, tiled=True)
        return returned.reshape(n_experts * cap_rows, d_model)[slot_tok]

    router_logit = jnp.dot(x_loc, w_gate, preferred_element_type=F32)
    router_prob = jax.nn.softmax(router_logit, axis=-1)
    gate_val = n_experts * jnp.sum(jnp.where(onehot, router_prob, 0.0), axis=1)
    recv_rows = dispatch(x_loc)
    gy_full = gy_loc.astype(F32)
    dy_tok = (gate_val[:, None] * gy_full).astype(BF16)
    recv_grad = dispatch(dy_tok)

    def one_expert(carry, per_expert):
        rows, grad, up, down = per_expert
        rows, grad = rows.reshape(-1, d_model), grad.reshape(-1, d_model)
        pre_act = dot(rows, up)
        hid_full, gelu_back = jax.vjp(jax.nn.gelu, pre_act)
        hidden = hid_full.astype(BF16)
        out_rows = dot(hidden, down).astype(BF16)
        d_pre = gelu_back(dot(grad, down, ((1,), (1,))))[0].astype(BF16)
        grad_down = dot(hidden, grad, ((0,), (0,)))
        grad_up = dot(rows, d_pre, ((0,), (0,)))
        d_rows = dot(d_pre, up, ((1,), (1,))).astype(BF16)
        shape = (ep_size, cap_rows, d_model)
        return carry, (out_rows.reshape(shape), d_rows.reshape(shape), grad_up, grad_down)

    swap = lambda rows: jnp.swapaxes(rows, 0, 1)
    _, (expert_out, d_rows, grad_up, grad_down) = lax.scan(
        one_expert, 0, (swap(recv_rows), swap(recv_grad), w_up, w_down))
    y_tok = combine(expert_out)
    moe_out = (gate_val[:, None] * y_tok.astype(F32)).astype(BF16)
    dx_expert = combine(d_rows)
    d_gate = jnp.sum(gy_full * y_tok.astype(F32), axis=1)
    d_logit = ((d_gate * gate_val)[:, None] * (onehot.astype(F32) - router_prob)).astype(BF16)
    dx_router = dot(d_logit, w_gate, ((1,), (1,)))
    grad_x = (dx_expert.astype(F32) + dx_router).astype(BF16)
    grad_gate = dot(x_loc, d_logit, ((0,), (0,)))

    def sum_dp(term):
        total = term
        for shift in range(1, dp_size):
            total = total + lax.ppermute(term, 'dp', [(i, (i + shift) % dp_size) for i in range(dp_size)])
        return total

    grad_gate = jnp.sum(lax.all_gather(grad_gate, ('dp', 'ep')), axis=0)
    return moe_out, grad_x, sum_dp(grad_up), sum_dp(grad_down), grad_gate


def solution(mesh):
    dp_size, ep_size = mesh.shape['dp'], mesh.shape['ep']
    tok_spec = P(('dp', 'ep'), None)
    idx_spec = P(('dp', 'ep'))
    rep_spec = P(None, None)
    exp_spec = P('ep', None, None)
    swap = [(i, (i + 1) % dp_size) for i in range(dp_size)]

    def local_step(x, gy, idx, w_gate, w_up, w_down):
        _, d_model = x.shape
        n_experts = w_gate.shape[1]
        local = w_up.shape[0]
        width = 2 * d_model
        base_rows = BASE_GROUPS * GROUP
        n_base = n_experts * base_rows
        n_over = OVER_GROUPS * GROUP
        ep = lax.axis_index('ep')
        first_expert = (ep * local).astype(I32).reshape(1)

        my_groups, pos = token_positions(idx, n_experts, local)
        chunk_rows = n_base // CHUNKS
        slots = (ep_size, local // CHUNKS, base_rows, width)
        base, base_z = [], []
        for c in range(CHUNKS):
            sent = permute_rows(pos, x, gy, c * chunk_rows, chunk_rows)
            base.append(lax.all_to_all(sent.reshape(ep_size, -1, width), 'ep', 0, 0, tiled=True))
            base_z.append(lax.ppermute(base[c], 'dp', swap).reshape(slots))
        marks = jnp.pad(my_groups.astype(BF16)[None, :], ((0, GROUP - 1), (0, width - n_experts)))
        over_sent = permute_rows(pos, x, gy, n_base, n_over, marks).reshape(SENT_GROUPS, GROUP, width)
        over = lax.all_gather(over_sent, 'ep')
        over_sent_z = lax.ppermute(over_sent, 'dp', swap)
        over_z = lax.all_gather(over_sent_z, 'ep')

        n_runs = MAX_OVER_TILES * RUNS * 3
        table, runs = plan_call(own_plan_kernel, local, first_expert, [over], [(5, MAX_OVER_TILES), (n_runs,)], 1)
        gtable, runs_z, fits = plan_call(grad_plan_kernel, local, first_expert, [over, over_z],
                                         [(8, 2 * (local + MAX_OVER_TILES)), (n_runs,), (1,)], 2)
        over_shape = (ep_size * SENT_GROUPS, GROUP, width)
        over = over.reshape(over_shape)
        over_z = over_z.reshape(over_shape)
        dwg = jnp.zeros((n_experts, d_model), F32)
        stores = None
        for c in range(CHUNKS):
            kept = own_base_pass(first_expert, c, base[c].reshape(slots), w_gate, w_up, w_down, dwg, stores, over_shape)
            dwg = kept[5]
            stores = kept[:5] + kept[6:]
        od, *base_store, zero_od = stores
        base_back = lax.all_to_all(od.reshape(ep_size, -1, width), 'ep', 0, 0, tiled=True)
        od_over, x_o, dy_o, h_o, da_o, dwg = own_over_pass(table, runs, first_expert, over, w_gate, w_up, w_down,
                                                          dwg, zero_od)
        over_back = lax.psum_scatter(od_over.reshape(ep_size, SENT_GROUPS, GROUP, width), 'ep', scatter_dimension=0)
        d_up, d_down = grad_pass(gtable, runs_z, first_expert, base_store, (x_o, dy_o, h_o, da_o), base_z, over_z,
                                 w_gate, w_up, w_down)
        d_gate = jnp.sum(lax.all_gather(dwg, ('dp', 'ep')), axis=0).T
        moe_out, grad_x = unpermute_rows(pos, base_back, over_back.reshape(-1, width))
        sparse = (moe_out, grad_x, d_up, d_down, d_gate)

        def dense(carry):
            del carry
            return (jnp.array(True),) + padded_step(x, gy, idx, w_gate, w_up, w_down, ep_size, dp_size)

        return lax.while_loop(lambda carry: jnp.logical_not(carry[0]), dense, (fits[0] == 1,) + sparse)[1:]

    return jax.shard_map(
        local_step, mesh=mesh, in_specs=(tok_spec, tok_spec, idx_spec, rep_spec, exp_spec, exp_spec),
        out_specs=(tok_spec, tok_spec, exp_spec, exp_spec, rep_spec), check_vma=False)
```

```python
import functools

import jax
import jax.numpy as jnp
from jax import lax
from jax.experimental import pallas as pl
from jax.experimental.pallas import tpu as pltpu
from jax.sharding import PartitionSpec as P


PAD_FACTOR = 4
GROUP = 8
BASE_GROUPS = 7
OVER_GROUPS = 50
SENT_GROUPS = OVER_GROUPS + 1
MAX_OVER_TILES = 8
RUNS = 8
RUN_SIZES = (16, 8, 4, 2, 1)
EXPERT, COUNT, STORE, LAST, N_RUNS = range(5)
TILE_GROUPS = 26
TILE = TILE_GROUPS * GROUP
PERM_TILE = 256
TOKEN_TILE = 512
CHUNK = 512
ROW_CHUNK = 256
CHUNKS = 2
SQRT_2_PI = 0.7978845608028654
CUBIC = 0.044715
VMEM_BYTES = 67_043_328

F32 = jnp.float32
BF16 = jnp.bfloat16
I32 = jnp.int32


BY_ROWS = ((0,), (0,))
BY_COLS = ((1,), (1,))


def dot(a, b, dims=((1,), (0,))):
    return lax.dot_general(a, b, (dims, ((), ())), preferred_element_type=F32)


def origin(*ids):
    return 0, 0


def step_id():
    return pl.program_id(0)


def step_count():
    return pl.num_programs(0)


def exclusive_cumsum(v, axis):
    return jnp.cumsum(v, axis=axis) - v


def token_positions(idx, n_experts, local):
    tok_count = idx.shape[0]
    block = 128
    base_rows = BASE_GROUPS * GROUP
    onehot = (idx[:, None] == jnp.arange(n_experts, dtype=I32)[None, :]).astype(BF16)
    blocks = onehot.reshape(tok_count // block, block, n_experts)
    lower = jnp.tril(jnp.ones((block, block), BF16))
    inclusive = jnp.einsum('ij,bje->bie', lower, blocks, preferred_element_type=F32)
    totals = jnp.sum(blocks.astype(F32), axis=1)
    counts = jnp.sum(totals, axis=0).astype(I32)
    groups = (counts + GROUP - 1) // GROUP
    over = jnp.maximum(groups - BASE_GROUPS, 0)
    over_start = exclusive_cumsum(over, 0)
    rank = inclusive + (exclusive_cumsum(totals, 0) - 1.0)[:, None, :]
    expert = jnp.arange(n_experts, dtype=I32)
    per_chunk = local // CHUNKS
    slot = (expert % local // per_chunk) * (n_experts // CHUNKS) + expert // local * per_chunk + expert % per_chunk
    base_at = (slot * base_rows).astype(F32)
    over_at = (n_experts * base_rows - base_rows + over_start * GROUP).astype(F32)
    row = jnp.sum(blocks.astype(F32) * (rank + jnp.where(rank < base_rows, base_at, over_at)), axis=2)
    last_row = n_experts * base_rows + OVER_GROUPS * GROUP - 1
    return groups, jnp.minimum(row, last_row).reshape(tok_count).astype(I32)


def permute_kernel(pos_ref, x_ref, gy_ref, *refs):
    *tail, out_ref = refs
    d_model = x_ref.shape[1]
    rows = out_ref.shape[0] - sum(t.shape[0] for t in tail)
    row_id = step_id() * rows + lax.broadcasted_iota(I32, (rows, x_ref.shape[0]), 0)
    select = jnp.where(row_id == pos_ref[...], 1.0, 0.0).astype(BF16)
    out_ref[:rows, :d_model] = dot(select, x_ref[...]).astype(BF16)
    out_ref[:rows, d_model:] = dot(select, gy_ref[...]).astype(BF16)
    for t in tail:
        out_ref[rows:, :] = t[...]


def permute_rows(pos, x, gy, first_row, n_rows, *tail):
    tok_count, d_model = x.shape
    tile = n_rows if n_rows % PERM_TILE else PERM_TILE
    extra = sum(t.shape[0] for t in tail)
    return pl.pallas_call(
        permute_kernel,
        grid=(n_rows // tile,),
        in_specs=[
            pl.BlockSpec((1, tok_count), origin),
            pl.BlockSpec((tok_count, d_model), origin),
            pl.BlockSpec((tok_count, d_model), origin),
        ] + [pl.BlockSpec(t.shape, origin) for t in tail],
        out_specs=pl.BlockSpec((tile + extra, 2 * d_model), lambda i: (i, 0)),
        out_shape=jax.ShapeDtypeStruct((n_rows + extra, 2 * d_model), BF16),
        cost_estimate=pl.CostEstimate(flops=4 * n_rows * tok_count * d_model, bytes_accessed=16_000_000, transcendentals=0),
        name='permute',
    )((pos - first_row).reshape(1, tok_count), x, gy, *tail)


def unpermute_kernel(pos_ref, base_ref, over_ref, out_ref, dx_ref, out_rows, dx_rows, out_tile, dx_tile):
    step = step_id()
    toks, d_model = out_ref.shape
    base_steps = 2 * CHUNKS
    block = base_ref.shape[0] * base_ref.shape[1]
    lanes = 128
    parts = d_model // lanes

    def spread(ref, first):
        n = ref.shape[0]
        size = max(k for k in range(GROUP, 65, GROUP) if n % k == 0)

        @pl.loop(0, n // size)
        def _(i):
            at = pl.multiple_of(i * size, 8)
            rows = ref[pl.ds(at, size), :].astype(F32)
            for c in range(parts):
                to = pl.ds((first + at) * 8 + c, size, stride=8)
                out_rows[to, :] = rows[:, c * lanes:(c + 1) * lanes]
                dx_rows[to, :] = rows[:, d_model + c * lanes:d_model + (c + 1) * lanes]

    @pl.when(step < base_steps)
    def _():
        for d in range(base_ref.shape[0]):
            spread(base_ref.at[d], step * block + d * base_ref.shape[1])

    @pl.when(step == base_steps)
    def _():
        spread(over_ref, base_steps * block)

    @pl.when(step > base_steps)
    def _():
        first = (step - base_steps - 1) * toks

        @pl.loop(0, toks // 16)
        def _(i):
            rows = [pl.multiple_of(pos_ref[first + i * 16 + u] * 8, 8) for u in range(16)]
            outs = [out_rows[pl.ds(r, 8), :] for r in rows]
            dxs = [dx_rows[pl.ds(r, 8), :] for r in rows]
            for u in range(16):
                to = pl.ds(pl.multiple_of((i * 16 + u) * 8, 8), 8)
                out_tile[to, :] = outs[u]
                dx_tile[to, :] = dxs[u]

        for c in range(parts):
            cols = slice(c * lanes, (c + 1) * lanes)
            out_ref[:, cols] = out_tile[pl.ds(c, toks, stride=8), :].astype(BF16)
            dx_ref[:, cols] = dx_tile[pl.ds(c, toks, stride=8), :].astype(BF16)


def unpermute_rows(pos, base, over):
    n_own, n_slot, width = base.shape
    tok_count = pos.shape[0]
    d_model = width // 2
    shape = jax.ShapeDtypeStruct((tok_count, d_model), BF16)
    base_steps = 2 * CHUNKS
    n_rows = n_own * n_slot + over.shape[0]
    token_tile = lambda i, pos: (jnp.maximum(i - base_steps - 1, 0), 0)
    part = lambda i: jnp.minimum(i, base_steps - 1)
    return pl.pallas_call(
        unpermute_kernel,
        grid_spec=pltpu.PrefetchScalarGridSpec(
            num_scalar_prefetch=1,
            grid=(base_steps + 1 + tok_count // TOKEN_TILE,),
            in_specs=[
                pl.BlockSpec((n_own // 2, n_slot // CHUNKS, width), lambda i, pos: (part(i) % 2, part(i) // 2, 0)),
                pl.BlockSpec(over.shape, origin),
            ],
            out_specs=[pl.BlockSpec((TOKEN_TILE, d_model), token_tile)] * 2,
            scratch_shapes=[pltpu.VMEM((n_rows * 8, 128), F32)] * 2 + [pltpu.VMEM((TOKEN_TILE * 8, 128), F32)] * 2,
        ),
        out_shape=[shape, shape],
        compiler_params=pltpu.CompilerParams(dimension_semantics=('arbitrary',)),
        cost_estimate=pl.CostEstimate(flops=10_000_000_000, bytes_accessed=16_000_000, transcendentals=0),
        name='unpermute',
    )(pos, base, over)


def gate(x, wg, expert):
    logit = dot(x, wg)
    unnorm = jnp.exp(logit - jnp.max(logit, axis=1, keepdims=True))
    prob = unnorm / jnp.sum(unnorm, axis=1, keepdims=True)
    onehot = lax.broadcasted_iota(I32, prob.shape, 1) == expert
    gate_val = prob.shape[1] * jnp.sum(jnp.where(onehot, prob, 0.0), axis=1, keepdims=True)
    return prob, onehot, gate_val


def activations(x, dy, w_up, w_down, cols):
    a = dot(x, w_up[:, cols])
    dh = dot(dy, w_down[cols, :], BY_COLS)
    cubic = (SQRT_2_PI * CUBIC) * (a * a)
    half = 0.5 + 0.5 * jnp.tanh(a * (SQRT_2_PI + cubic))
    h = a * half
    slope = half + (h - h * half) * (2.0 * SQRT_2_PI + 6.0 * cubic)
    return h.astype(BF16), (slope * dh).astype(BF16)


def own_rows_step(x, gy, expert, wg_ref, w_up, w_down, store, dwg_ref):
    dy_ref, h_ref, da_ref = store
    prob, onehot, gate_val = gate(x, wg_ref[...], expert)
    gy_full = gy.astype(F32)
    dy = (gate_val * gy_full).astype(BF16)
    dy_ref[...] = dy
    for lo in range(0, h_ref.shape[1], ROW_CHUNK):
        cols = pl.ds(lo, ROW_CHUNK)
        h, da = activations(x, dy, w_up, w_down, cols)
        h_ref[:, cols] = h
        da_ref[:, cols] = da
    y = dot(h_ref[...], w_down[...]).astype(BF16).astype(F32)
    dxe = dot(da_ref[...], w_up[...], BY_COLS).astype(BF16).astype(F32)
    d_gate = jnp.sum(gy_full * y, axis=1, keepdims=True)
    d_logit = ((d_gate * gate_val) * (onehot.astype(F32) - prob)).astype(BF16)
    dwg_ref[...] += dot(d_logit, x, BY_ROWS)
    out = (gate_val * y).astype(BF16)
    dx = (dxe + dot(d_logit, wg_ref[...], BY_COLS)).astype(BF16)
    return out, dx


def own_base_kernel(first_ref, rows_ref, wg_ref, up_ref, down_ref, dwg_in, *refs):
    od_ref, x_ref, dy_ref, h_ref, da_ref, dwg_ref, zero_ref = refs[-7:]
    step = step_id()
    d_model = wg_ref.shape[0]

    @pl.when(step == 0)
    def _():
        dwg_ref[...] = dwg_in[...]

    zero_ref[...] = jnp.zeros_like(zero_ref)
    rows = rows_ref[...].reshape(dy_ref.shape[0], 2 * d_model)
    x = rows[:, :d_model]
    x_ref[...] = x
    out, dx = own_rows_step(x, rows[:, d_model:], first_ref[0] + step, wg_ref, up_ref.at[0], down_ref.at[0],
                            (dy_ref, h_ref, da_ref), dwg_ref)
    block = od_ref.shape[:3] + (d_model,)
    od_ref[:, :, :, :d_model] = out.reshape(block)
    od_ref[:, :, :, d_model:] = dx.reshape(block)


def own_base_pass(first_expert, chunk, rows, wg, w_up, w_down, dwg, stores, over_shape):
    n_src, count, seg, width = rows.shape
    local, d_model, d_ff = w_up.shape
    tile = n_src * seg
    lead = chunk * count
    row_spec = lambda at: pl.BlockSpec((n_src, 1, seg, width), lambda e, first: (0, at + e, 0, 0))
    store_spec = lambda cols: pl.BlockSpec((tile, cols), lambda e, first: (lead + e, 0))
    rows_of = lambda cols: jax.ShapeDtypeStruct((local * tile, cols), BF16)
    zero_block = (over_shape[0] // local,) + over_shape[1:]
    kept = [] if stores is None else list(stores)
    return pl.pallas_call(
        own_base_kernel,
        grid_spec=pltpu.PrefetchScalarGridSpec(
            num_scalar_prefetch=1,
            grid=(count,),
            in_specs=[
                row_spec(0),
                pl.BlockSpec(wg.shape, origin),
                pl.BlockSpec((1, d_model, d_ff), lambda e, first: (lead + e, 0, 0)),
                pl.BlockSpec((1, d_ff, d_model), lambda e, first: (lead + e, 0, 0)),
                pl.BlockSpec(dwg.shape, origin),
            ] + [pl.BlockSpec(memory_space=pl.ANY)] * len(kept),
            out_specs=[row_spec(lead), store_spec(d_model), store_spec(d_model), store_spec(d_ff), store_spec(d_ff),
                       pl.BlockSpec(dwg.shape, origin), pl.BlockSpec(zero_block, lambda e, first: (lead + e, 0, 0))],
        ),
        out_shape=[jax.ShapeDtypeStruct((n_src, local, seg, width), BF16), rows_of(d_model), rows_of(d_model), rows_of(d_ff), rows_of(d_ff),
                   jax.ShapeDtypeStruct(dwg.shape, F32), jax.ShapeDtypeStruct(over_shape, BF16)],
        input_output_aliases={6 + i: o for i, o in zip(range(len(kept)), (0, 1, 2, 3, 4, 6))},
        compiler_params=pltpu.CompilerParams(vmem_limit_bytes=VMEM_BYTES, dimension_semantics=('arbitrary',)),
        cost_estimate=pl.CostEstimate(flops=8_500_000_000 * count, bytes_accessed=20_000_000 * count,
                                      transcendentals=1_500_000 * count),
        name='own_base',
    )(first_expert + lead, rows, wg, w_up, w_down, dwg, *kept)


def run_copies(runs_ref, tile, n_runs, hbm, buf, sem, to_hbm):
    def body(r, carry):
        at = (tile * RUNS + r) * 3
        first, left, slot = (runs_ref[at + k] for k in range(3))
        for size in RUN_SIZES:
            take = left >= size

            @pl.when(take)
            def _(first=first, slot=slot, size=size):
                ends = (hbm.at[pl.ds(first, size)], buf.at[pl.ds(slot, size)])
                pltpu.make_async_copy(*(ends[::-1] if to_hbm else ends), sem).start()

            step = jnp.where(take, size, 0)
            first, slot, left = first + step, slot + step, left - step
        return carry

    lax.fori_loop(0, n_runs, body, 0)


def run_waits(count, hbm, buf, sem, to_hbm):
    for size in RUN_SIZES:
        @pl.when((count & size) != 0)
        def _(size=size):
            ends = (hbm.at[pl.ds(0, size)], buf.at[pl.ds(0, size)])
            pltpu.make_async_copy(*(ends[::-1] if to_hbm else ends), sem).wait()


def tile_rows(buf, count):
    rows = buf[...].reshape(TILE, buf.shape[-1])
    row_id = lax.broadcasted_iota(I32, rows.shape, 0)
    return jnp.where(row_id < count * GROUP, rows, jnp.zeros((), rows.dtype))


def own_over_kernel(tab_ref, runs_ref, first_ref, rows_hbm, wg_ref, up_ref, down_ref, dwg_in, zero_od,
                    od_hbm, x_ref, dy_ref, h_ref, da_ref, dwg_ref, in_buf, out_buf, in_sem, out_sem):
    del zero_od
    step = step_id()
    d_model = wg_ref.shape[0]
    slot = step % 2
    count = tab_ref[COUNT, step]

    @pl.when(step == 0)
    def _():
        dwg_ref[...] = dwg_in[...]
        run_copies(runs_ref, 0, tab_ref[N_RUNS, 0], rows_hbm, in_buf.at[0], in_sem.at[0], False)

    @pl.when(count > 0)
    def _():
        run_waits(count, rows_hbm, in_buf.at[slot], in_sem.at[slot], False)

        @pl.when(step + 1 < step_count())
        def _():
            run_copies(runs_ref, step + 1, tab_ref[N_RUNS, step + 1], rows_hbm, in_buf.at[1 - slot], in_sem.at[1 - slot], False)

        rows = tile_rows(in_buf.at[slot], count)
        x = rows[:, :d_model]
        x_ref[...] = x
        out, dx = own_rows_step(x, rows[:, d_model:], first_ref[0] + tab_ref[EXPERT, step], wg_ref,
                                up_ref.at[0], down_ref.at[0], (dy_ref, h_ref, da_ref), dwg_ref)

        @pl.when(step > 0)
        def _():
            run_waits(tab_ref[COUNT, step - 1], od_hbm, out_buf, out_sem, True)

        out_buf[:, :, :d_model] = out.reshape(TILE_GROUPS, GROUP, d_model)
        out_buf[:, :, d_model:] = dx.reshape(TILE_GROUPS, GROUP, d_model)
        run_copies(runs_ref, step, tab_ref[N_RUNS, step], od_hbm, out_buf, out_sem, True)

        @pl.when(tab_ref[LAST, step] == 1)
        def _():
            run_waits(count, od_hbm, out_buf, out_sem, True)


def own_over_pass(table, runs, first_expert, rows, wg, w_up, w_down, dwg, zero_od):
    d_model, d_ff = w_up.shape[1], w_up.shape[2]
    width = rows.shape[-1]
    n_tiles = table.shape[1]
    hbm = pl.BlockSpec(memory_space=pl.ANY)
    store_spec = lambda cols: pl.BlockSpec((TILE, cols), lambda i, tab, runs, first: (tab[STORE, i], 0))
    rows_of = lambda cols: jax.ShapeDtypeStruct((n_tiles * TILE, cols), BF16)
    return pl.pallas_call(
        own_over_kernel,
        grid_spec=pltpu.PrefetchScalarGridSpec(
            num_scalar_prefetch=3,
            grid=(n_tiles,),
            in_specs=[
                hbm,
                pl.BlockSpec(wg.shape, origin),
                pl.BlockSpec((1, d_model, d_ff), lambda i, tab, runs, first: (tab[EXPERT, i], 0, 0)),
                pl.BlockSpec((1, d_ff, d_model), lambda i, tab, runs, first: (tab[EXPERT, i], 0, 0)),
                pl.BlockSpec(dwg.shape, origin),
                hbm,
            ],
            out_specs=[hbm, store_spec(d_model), store_spec(d_model), store_spec(d_ff), store_spec(d_ff),
                       pl.BlockSpec(dwg.shape, origin)],
            scratch_shapes=[
                pltpu.VMEM((2, TILE_GROUPS, GROUP, width), BF16),
                pltpu.VMEM((TILE_GROUPS, GROUP, width), BF16),
                pltpu.SemaphoreType.DMA((2,)),
                pltpu.SemaphoreType.DMA,
            ],
        ),
        out_shape=[jax.ShapeDtypeStruct(zero_od.shape, BF16), rows_of(d_model), rows_of(d_model), rows_of(d_ff),
                   rows_of(d_ff), jax.ShapeDtypeStruct(dwg.shape, F32)],
        input_output_aliases={8: 0},
        compiler_params=pltpu.CompilerParams(vmem_limit_bytes=VMEM_BYTES, dimension_semantics=('arbitrary',)),
        cost_estimate=pl.CostEstimate(flops=10_000_000_000, bytes_accessed=40_000_000, transcendentals=2_000_000),
        name='own_over',
    )(table, runs, first_expert, rows, wg, w_up, w_down, dwg, zero_od)


OWN_BASE, OWN_OVER, OTHER_BASE, OTHER_OVER = range(4)


def grad_kernel(tab_ref, runs_ref, first_ref, xb_ref, dyb_ref, hb_ref, dab_ref, xo_ref, dyo_ref, ho_ref, dao_ref, *refs):
    *base_hbm, over_hbm, wg_ref, up_hbm, down_hbm, dup_hbm, ddown_hbm = refs[:-12]
    dup, ddown, up_buf, down_buf, h_buf, da_buf, base_buf, in_buf, w_sems, base_sem, in_sem, out_sems = refs[-12:]
    step = step_id()
    d_model, d_ff = dup.shape
    expert, kind, last, _, count = (tab_ref[row, step] for row in range(5))
    n_local = dup_hbm.shape[0]
    base_rows = h_buf.shape[0]

    def weights(e):
        return (pltpu.make_async_copy(up_hbm.at[e], up_buf, w_sems.at[0]),
                pltpu.make_async_copy(down_hbm.at[e], down_buf, w_sems.at[1]))

    def flush_down(e):
        return pltpu.make_async_copy(ddown, ddown_hbm.at[e], out_sems.at[0])

    def flush_up(e):
        return pltpu.make_async_copy(dup, dup_hbm.at[e], out_sems.at[1])

    def add_down(dy, h_src, add):
        for lo in range(0, d_ff, CHUNK):
            cols = pl.ds(lo, CHUNK)
            term = dot(h_src[:, cols], dy, BY_ROWS)
            ddown[cols, :] = ddown[cols, :] + term if add else term

    def add_up(x, da_src, add):
        for lo in range(0, d_ff, CHUNK):
            cols = pl.ds(lo, CHUNK)
            term = dot(x, da_src[:, cols], BY_ROWS)
            dup[:, cols] = dup[:, cols] + term if add else term

    def accumulate(x, dy, h_src, da_src):
        add_down(dy, h_src, True)

        @pl.when(last == 1)
        def _():
            flush_down(expert).start()

        add_up(x, da_src, True)

        @pl.when(last == 1)
        def _():
            flush_up(expert).start()

            @pl.when(expert + 1 < n_local)
            def _():
                for copy in weights(expert + 1):
                    copy.start()

            @pl.when(expert + 1 == n_local)
            def _():
                flush_down(expert).wait()
                flush_up(expert).wait()

    def base_copy(e):
        chunk = base_hbm[e // base_hbm[0].shape[1]]
        return pltpu.make_async_copy(chunk.at[:, e % chunk.shape[1]], base_buf, base_sem)

    ahead = step + 1
    ahead_at = jnp.minimum(ahead, step_count() - 1)

    @pl.when((ahead < step_count()) & (tab_ref[1, ahead_at] == OTHER_OVER))
    def _():
        run_copies(runs_ref, tab_ref[5, ahead_at], tab_ref[7, ahead_at], over_hbm, in_buf.at[ahead % 2], in_sem.at[ahead % 2],
                   False)

    @pl.when(kind == OWN_BASE)
    def _():
        for e in range(n_local):
            @pl.when(expert == e)
            def _():
                base_copy(e).start()

        @pl.when(expert == 0)
        def _():
            for copy in weights(0):
                copy.start()

        @pl.when(expert > 0)
        def _():
            flush_down(expert - 1).wait()

        add_down(dyb_ref[...], hb_ref, False)

        @pl.when(expert > 0)
        def _():
            flush_up(expert - 1).wait()

        add_up(xb_ref[...], dab_ref, False)

    @pl.when(kind == OWN_OVER)
    def _():
        add_down(dyo_ref[...], ho_ref, True)
        add_up(xo_ref[...], dao_ref, True)

    def other_rows(rows, n_rows):
        x, gy = rows[:, :d_model], rows[:, d_model:]
        _, _, gate_val = gate(x, wg_ref[...], first_ref[0] + expert)
        dy = (gate_val * gy.astype(F32)).astype(BF16)
        h_dst, da_dst = h_buf.at[:n_rows], da_buf.at[:n_rows]
        for lo in range(0, d_ff, ROW_CHUNK):
            cols = pl.ds(lo, ROW_CHUNK)
            h, da = activations(x, dy, up_buf, down_buf, cols)
            h_dst[:, cols] = h
            da_dst[:, cols] = da
        accumulate(x, dy, h_dst, da_dst)

    @pl.when(kind == OTHER_BASE)
    def _():
        for copy in weights(expert):
            copy.wait()
        base_copy(0).wait()
        other_rows(base_buf[...].reshape(base_rows, 2 * d_model), base_rows)

    @pl.when(kind == OTHER_OVER)
    def _():
        run_waits(count, over_hbm, in_buf.at[step % 2], in_sem.at[step % 2], False)
        other_rows(tile_rows(in_buf.at[step % 2], count), TILE)


def grad_pass(table, ids, first_expert, base_store, over_store, base, over, wg, w_up, w_down):
    n_src, _, seg, width = base[0].shape
    d_model, d_ff = w_up.shape[1], w_up.shape[2]
    base_rows = n_src * seg
    base_spec = lambda cols: pl.BlockSpec((base_rows, cols), lambda i, tab, ids, first: (tab[6, i], 0))
    over_spec = lambda cols: pl.BlockSpec((TILE, cols), lambda i, tab, ids, first: (tab[3, i], 0))
    hbm = pl.BlockSpec(memory_space=pl.ANY)
    return pl.pallas_call(
        grad_kernel,
        grid_spec=pltpu.PrefetchScalarGridSpec(
            num_scalar_prefetch=3,
            grid=(table.shape[1],),
            in_specs=[
                base_spec(d_model),
                base_spec(d_model),
                base_spec(d_ff),
                base_spec(d_ff),
                over_spec(d_model),
                over_spec(d_model),
                over_spec(d_ff),
                over_spec(d_ff),
                *[hbm for _ in base],
                hbm,
                pl.BlockSpec(wg.shape, origin),
                hbm,
                hbm,
            ],
            out_specs=[hbm, hbm],
            scratch_shapes=[
                pltpu.VMEM((d_model, d_ff), F32),
                pltpu.VMEM((d_ff, d_model), F32),
                pltpu.VMEM((d_model, d_ff), BF16),
                pltpu.VMEM((d_ff, d_model), BF16),
                pltpu.VMEM((base_rows, d_ff), BF16),
                pltpu.VMEM((base_rows, d_ff), BF16),
                pltpu.VMEM((n_src, seg, width), BF16),
                pltpu.VMEM((2, TILE_GROUPS, GROUP, width), BF16),
                pltpu.SemaphoreType.DMA((2,)),
                pltpu.SemaphoreType.DMA,
                pltpu.SemaphoreType.DMA((2,)),
                pltpu.SemaphoreType.DMA((2,)),
            ],
        ),
        out_shape=[jax.ShapeDtypeStruct(w_up.shape, F32), jax.ShapeDtypeStruct(w_down.shape, F32)],
        compiler_params=pltpu.CompilerParams(vmem_limit_bytes=VMEM_BYTES, dimension_semantics=('arbitrary',)),
        cost_estimate=pl.CostEstimate(flops=70_000_000_000, bytes_accessed=150_000_000, transcendentals=8_000_000),
        name='grad_pass',
    )(table, ids, first_expert, *base_store, *over_store, *base, over, wg, w_up, w_down)


def overflow_spans(count_ref, local):
    groups = jnp.sum(count_ref[...].astype(F32), axis=(1, 2))
    over = jnp.maximum(groups - BASE_GROUPS, 0.0)
    lanes = over.shape[1]
    row, col = (lax.broadcasted_iota(I32, (lanes, lanes), d) for d in (0, 1))
    start = dot(over.astype(BF16), jnp.where(row < col, 1.0, 0.0).astype(BF16))
    tiles = jnp.ceil(jnp.sum(over, axis=0, keepdims=True) * (1.0 / TILE_GROUPS) - 1e-3)
    owner = dot(jnp.broadcast_to(tiles, over.shape).astype(BF16), jnp.where(row // local == col, 1.0, 0.0).astype(BF16))
    excess = jnp.max(jnp.maximum(start + over - OVER_GROUPS, owner - MAX_OVER_TILES))
    first = jnp.minimum(start, OVER_GROUPS)
    size = jnp.minimum(start + over, OVER_GROUPS) - first
    return size.astype(I32), first.astype(I32), excess


def fill_tiles(n_src, local, lead, size, first, runs, n_runs, count):
    for t in range(MAX_OVER_TILES):
        n_runs[t] = 0
        count[t] = 0

    def put(tile, slot, begin, groups):
        @pl.when((groups > 0) & (tile < MAX_OVER_TILES))
        def _():
            at = (tile * RUNS + n_runs[tile]) * 3
            for k, value in enumerate((begin, groups, slot)):
                runs[at + k] = value
            n_runs[tile] = n_runs[tile] + 1
            count[tile] = count[tile] + groups

    spans, tile = [], jnp.int32(0)
    for e in range(local):
        def per_source(s, where, e=e):
            tile, slot = where
            groups = size[s, lead + e]
            begin = s * SENT_GROUPS + first[s, lead + e]
            head = jnp.minimum(groups, TILE_GROUPS - slot)
            rest = groups - head
            put(tile, slot, begin, head)
            put(tile + 1, 0, begin + head, rest)
            full = (slot + head == TILE_GROUPS).astype(I32)
            return tile + full, jnp.where(full == 1, rest, slot + head)

        end, slot = lax.fori_loop(0, n_src, per_source, (tile, jnp.int32(0)))
        end = jnp.minimum(end + (slot > 0).astype(I32), MAX_OVER_TILES)
        spans.append((tile, end - tile))
        tile = end
    return spans, tile


def to_scalars(pairs, sems):
    copies = [pltpu.make_async_copy(v, m, sems.at[i]) for i, (v, m) in enumerate(pairs)]
    for copy in copies:
        copy.start()
    for copy in copies:
        copy.wait()


def own_plan_kernel(local, lead_ref, count_ref, tab_ref, runs_ref, size_v, first_v, size_s, first_s, n_runs, count, sems):
    size_v[...], first_v[...], _ = overflow_spans(count_ref, local)
    to_scalars([(size_v, size_s), (first_v, first_s)], sems)
    spans, n_tiles = fill_tiles(count_ref.shape[0], local, lead_ref[0], size_s, first_s, runs_ref, n_runs.at[0], count.at[0])
    last = jnp.maximum(n_tiles - 1, 0)
    for t in range(MAX_OVER_TILES):
        row = (local - 1, count[0, t], jnp.minimum(t, last), (last == t).astype(I32), n_runs[0, t])
        for k, value in enumerate(row):
            tab_ref[k, t] = value
    for e, (tile, tiles) in enumerate(spans):
        def body(k, c, e=e, tile=tile):
            tab_ref[EXPERT, tile + k] = e
            return c

        lax.fori_loop(0, tiles, body, 0)


def grad_plan_kernel(local, lead_ref, own_ref, other_ref, tab_ref, runs_ref, fits_ref, size_v, first_v, size_s, first_s,
                     n_runs, count, sems):
    n_src = own_ref.shape[0]
    size_v[0], first_v[0], own_excess = overflow_spans(own_ref, local)
    size_v[1], first_v[1], other_excess = overflow_spans(other_ref, local)
    to_scalars([(size_v, size_s), (first_v, first_s)], sems)
    fits_ref[0] = (jnp.maximum(own_excess, other_excess) <= 0.0).astype(I32)
    lead = lead_ref[0]
    own, n_tiles = fill_tiles(n_src, local, lead, size_s.at[0], first_s.at[0], runs_ref, n_runs.at[0], count.at[0])
    other, _ = fill_tiles(n_src, local, lead, size_s.at[1], first_s.at[1], runs_ref, n_runs.at[1], count.at[1])
    max_steps = tab_ref.shape[1]

    def emit(step, expert, kind, own_tile, other_tile, next_base):
        over = int(kind == OTHER_OVER)
        row = (expert, kind, 0, jnp.clip(own_tile, 0, MAX_OVER_TILES - 1), count[1, other_tile] * over, other_tile, next_base,
               n_runs[1, other_tile] * over)
        for k, value in enumerate(row):
            tab_ref[k, step] = value

    step = jnp.int32(0)
    for e in range(local):
        own_tile, own_tiles = own[e]
        other_tile, other_tiles = other[e]
        after = min(e + 1, local - 1)
        emit(step, e, OWN_BASE, own_tile, 0, e)

        def own_body(k, c, e=e, step=step, own_tile=own_tile, after=after):
            emit(step + 1 + k, e, OWN_OVER, own_tile + k, 0, after)
            return c

        lax.fori_loop(0, own_tiles, own_body, 0)
        step = step + 1 + own_tiles
        own_at = own_tile + own_tiles
        emit(step, e, OTHER_BASE, own_at, 0, after)

        def other_body(k, c, e=e, step=step, own_at=own_at, other_tile=other_tile, after=after):
            emit(step + 1 + k, e, OTHER_OVER, own_at, other_tile + k, after)
            return c

        lax.fori_loop(0, other_tiles, other_body, 0)
        step = step + 1 + other_tiles
        tab_ref[2, step - 1] = 1

    def dead(t, c):
        emit(t, local - 1, -1, n_tiles - 1, 0, local - 1)
        return c

    lax.fori_loop(step, max_steps, dead, 0)


def plan_call(kernel, local, lead, counts, out_shapes, planes):
    n_src = counts[0].shape[0]
    smem = pl.BlockSpec(memory_space=pltpu.SMEM)
    spec = pl.BlockSpec((n_src, 1, GROUP, 128), lambda i: (0, OVER_GROUPS, 0, 0))
    shape = (n_src, 128) if planes == 1 else (planes, n_src, 128)
    return pl.pallas_call(
        functools.partial(kernel, local),
        grid=(1,),
        in_specs=[smem] + [spec] * len(counts),
        out_specs=[smem] * len(out_shapes),
        out_shape=[jax.ShapeDtypeStruct(o, I32) for o in out_shapes],
        scratch_shapes=[pltpu.VMEM(shape, I32), pltpu.VMEM(shape, I32), pltpu.SMEM(shape, I32), pltpu.SMEM(shape, I32),
                        pltpu.SMEM((planes, MAX_OVER_TILES), I32), pltpu.SMEM((planes, MAX_OVER_TILES), I32),
                        pltpu.SemaphoreType.DMA((2,))],
    )(lead, *counts)


def padded_step(x_loc, gy_loc, idx_loc, w_gate, w_up, w_down, ep_size, dp_size):
    tok_count, d_model = x_loc.shape
    n_experts = w_gate.shape[1]
    local_experts = w_up.shape[0]
    cap_rows = PAD_FACTOR * tok_count // n_experts
    onehot = idx_loc[:, None] == jnp.arange(n_experts, dtype=I32)[None, :]
    expert_count = jnp.sum(onehot, axis=0, dtype=I32)
    sort_order = jnp.argsort(idx_loc, stable=True)
    sorted_pos = jnp.argsort(sort_order)
    expert_start = jnp.cumsum(expert_count) - expert_count
    slot_k = jnp.arange(cap_rows, dtype=I32)
    slot_valid = slot_k[None, :] < expert_count[:, None]
    src_tok = sort_order[jnp.minimum(expert_start[:, None] + slot_k[None, :], tok_count - 1)]
    slot_tok = idx_loc * cap_rows + sorted_pos - expert_start[idx_loc]

    def dispatch(tok_rows):
        picked = jnp.where(slot_valid[:, :, None], tok_rows[src_tok], jnp.zeros((), tok_rows.dtype))
        picked = picked.reshape(ep_size, local_experts, cap_rows, d_model)
        return lax.all_to_all(picked, 'ep', 0, 0, tiled=True)

    def combine(expert_rows):
        returned = lax.all_to_all(expert_rows, 'ep', 1, 0, tiled=True)
        return returned.reshape(n_experts * cap_rows, d_model)[slot_tok]

    router_logit = jnp.dot(x_loc, w_gate, preferred_element_type=F32)
    router_prob = jax.nn.softmax(router_logit, axis=-1)
    gate_val = n_experts * jnp.sum(jnp.where(onehot, router_prob, 0.0), axis=1)
    recv_rows = dispatch(x_loc)
    gy_full = gy_loc.astype(F32)
    dy_tok = (gate_val[:, None] * gy_full).astype(BF16)
    recv_grad = dispatch(dy_tok)

    def one_expert(carry, per_expert):
        rows, grad, up, down = per_expert
        rows, grad = rows.reshape(-1, d_model), grad.reshape(-1, d_model)
        pre_act = dot(rows, up)
        hid_full, gelu_back = jax.vjp(jax.nn.gelu, pre_act)
        hidden = hid_full.astype(BF16)
        out_rows = dot(hidden, down).astype(BF16)
        d_pre = gelu_back(dot(grad, down, BY_COLS))[0].astype(BF16)
        grad_down = dot(hidden, grad, BY_ROWS)
        grad_up = dot(rows, d_pre, BY_ROWS)
        d_rows = dot(d_pre, up, BY_COLS).astype(BF16)
        shape = (ep_size, cap_rows, d_model)
        return carry, (out_rows.reshape(shape), d_rows.reshape(shape), grad_up, grad_down)

    swap = lambda rows: jnp.swapaxes(rows, 0, 1)
    _, (expert_out, d_rows, grad_up, grad_down) = lax.scan(
        one_expert, 0, (swap(recv_rows), swap(recv_grad), w_up, w_down))
    y_tok = combine(expert_out)
    moe_out = (gate_val[:, None] * y_tok.astype(F32)).astype(BF16)
    dx_expert = combine(d_rows)
    d_gate = jnp.sum(gy_full * y_tok.astype(F32), axis=1)
    d_logit = ((d_gate * gate_val)[:, None] * (onehot.astype(F32) - router_prob)).astype(BF16)
    dx_router = dot(d_logit, w_gate, BY_COLS)
    grad_x = (dx_expert.astype(F32) + dx_router).astype(BF16)
    grad_gate = dot(x_loc, d_logit, BY_ROWS)

    def sum_dp(term):
        total = term
        for shift in range(1, dp_size):
            total = total + lax.ppermute(term, 'dp', [(i, (i + shift) % dp_size) for i in range(dp_size)])
        return total

    grad_gate = jnp.sum(lax.all_gather(grad_gate, ('dp', 'ep')), axis=0)
    return moe_out, grad_x, sum_dp(grad_up), sum_dp(grad_down), grad_gate


def solution(mesh):
    dp_size, ep_size = mesh.shape['dp'], mesh.shape['ep']
    tok_spec = P(('dp', 'ep'), None)
    idx_spec = P(('dp', 'ep'))
    rep_spec = P(None, None)
    exp_spec = P('ep', None, None)
    swap = [(i, (i + 1) % dp_size) for i in range(dp_size)]

    def local_step(x, gy, idx, w_gate, w_up, w_down):
        _, d_model = x.shape
        n_experts = w_gate.shape[1]
        local = w_up.shape[0]
        width = 2 * d_model
        base_rows = BASE_GROUPS * GROUP
        n_base = n_experts * base_rows
        n_over = OVER_GROUPS * GROUP
        ep = lax.axis_index('ep')
        first_expert = (ep * local).astype(I32).reshape(1)

        my_groups, pos = token_positions(idx, n_experts, local)
        chunk_rows = n_base // CHUNKS
        slots = (ep_size, local // CHUNKS, base_rows, width)
        base, base_z = [], []
        for c in range(CHUNKS):
            sent = permute_rows(pos, x, gy, c * chunk_rows, chunk_rows)
            base.append(lax.all_to_all(sent.reshape(ep_size, -1, width), 'ep', 0, 0, tiled=True))
            base_z.append(lax.ppermute(base[c], 'dp', swap).reshape(slots))
        marks = jnp.pad(my_groups.astype(BF16)[None, :], ((0, GROUP - 1), (0, width - n_experts)))
        over_sent = permute_rows(pos, x, gy, n_base, n_over, marks).reshape(SENT_GROUPS, GROUP, width)
        over = lax.all_gather(over_sent, 'ep')
        over_sent_z = lax.ppermute(over_sent, 'dp', swap)
        over_z = lax.all_gather(over_sent_z, 'ep')

        n_runs = MAX_OVER_TILES * RUNS * 3
        table, runs = plan_call(own_plan_kernel, local, first_expert, [over], [(5, MAX_OVER_TILES), (n_runs,)], 1)
        gtable, runs_z, fits = plan_call(grad_plan_kernel, local, first_expert, [over, over_z],
                                         [(8, 2 * (local + MAX_OVER_TILES)), (n_runs,), (1,)], 2)
        over_shape = (ep_size * SENT_GROUPS, GROUP, width)
        over = over.reshape(over_shape)
        over_z = over_z.reshape(over_shape)
        dwg = jnp.zeros((n_experts, d_model), F32)
        stores = None
        for c in range(CHUNKS):
            kept = own_base_pass(first_expert, c, base[c].reshape(slots), w_gate, w_up, w_down, dwg, stores, over_shape)
            dwg = kept[5]
            stores = kept[:5] + kept[6:]
        od, *base_store, zero_od = stores
        base_back = lax.all_to_all(od.reshape(ep_size, -1, width), 'ep', 0, 0, tiled=True)
        od_over, x_o, dy_o, h_o, da_o, dwg = own_over_pass(table, runs, first_expert, over, w_gate, w_up, w_down,
                                                          dwg, zero_od)
        over_back = lax.psum_scatter(od_over.reshape(ep_size, SENT_GROUPS, GROUP, width), 'ep', scatter_dimension=0)
        d_up, d_down = grad_pass(gtable, runs_z, first_expert, base_store, (x_o, dy_o, h_o, da_o), base_z, over_z,
                                 w_gate, w_up, w_down)

        def from_peer(axis, bits, value):
            return lax.ppermute(value, axis, [(i, i ^ bits) for i in range(mesh.shape[axis])])

        pair = dwg + from_peer('ep', 1, dwg)
        near = pair + from_peer('ep', 2, pair)
        far = from_peer('ep', 4, pair) + from_peer('ep', 6, pair)
        plane = near + far
        d_gate = (plane + from_peer('dp', 1, plane)).T
        moe_out, grad_x = unpermute_rows(pos, base_back, over_back.reshape(-1, width))
        sparse = (moe_out, grad_x, d_up, d_down, d_gate)

        def dense(carry):
            del carry
            return (jnp.array(True),) + padded_step(x, gy, idx, w_gate, w_up, w_down, ep_size, dp_size)

        return lax.while_loop(lambda carry: jnp.logical_not(carry[0]), dense, (fits[0] == 1,) + sparse)[1:]

    return jax.shard_map(
        local_step, mesh=mesh, in_specs=(tok_spec, tok_spec, idx_spec, rep_spec, exp_spec, exp_spec),
        out_specs=(tok_spec, tok_spec, exp_spec, exp_spec, rep_spec), check_vma=False)
```

```python
import functools

import jax
import jax.numpy as jnp
from jax import lax
from jax.experimental import pallas as pl
from jax.experimental.pallas import tpu as pltpu
from jax.sharding import PartitionSpec as P


PAD_FACTOR = 4
GROUP = 8
BASE_GROUPS = 7
OVER_GROUPS = 50
SENT_GROUPS = OVER_GROUPS + 1
MAX_OVER_TILES = 8
RUNS = 8
RUN_SIZES = (16, 8, 4, 2, 1)
EXPERT, COUNT, STORE, LAST, N_RUNS = range(5)
TILE_GROUPS = 26
TILE = TILE_GROUPS * GROUP
PERM_TILE = 256
TOKEN_TILE = 512
CHUNK = 512
ROW_CHUNK = 256
CHUNKS = 2
SQRT_2_PI = 0.7978845608028654
CUBIC = 0.044715
VMEM_BYTES = 67_043_328

F32 = jnp.float32
BF16 = jnp.bfloat16
I32 = jnp.int32


BY_ROWS = ((0,), (0,))
BY_COLS = ((1,), (1,))


def dot(a, b, dims=((1,), (0,))):
    return lax.dot_general(a, b, (dims, ((), ())), preferred_element_type=F32)


def origin(*ids):
    return 0, 0


def step_id():
    return pl.program_id(0)


def step_count():
    return pl.num_programs(0)


def exclusive_cumsum(v, axis):
    return jnp.cumsum(v, axis=axis) - v


def token_positions(idx, n_experts, local):
    tok_count = idx.shape[0]
    block = 128
    base_rows = BASE_GROUPS * GROUP
    onehot = (idx[:, None] == jnp.arange(n_experts, dtype=I32)[None, :]).astype(BF16)
    blocks = onehot.reshape(tok_count // block, block, n_experts)
    lower = jnp.tril(jnp.ones((block, block), BF16))
    inclusive = jnp.einsum('ij,bje->bie', lower, blocks, preferred_element_type=F32)
    totals = jnp.sum(blocks.astype(F32), axis=1)
    counts = jnp.sum(totals, axis=0).astype(I32)
    groups = (counts + GROUP - 1) // GROUP
    over = jnp.maximum(groups - BASE_GROUPS, 0)
    over_start = exclusive_cumsum(over, 0)
    rank = inclusive + (exclusive_cumsum(totals, 0) - 1.0)[:, None, :]
    expert = jnp.arange(n_experts, dtype=I32)
    per_chunk = local // CHUNKS
    slot = (expert % local // per_chunk) * (n_experts // CHUNKS) + expert // local * per_chunk + expert % per_chunk
    base_at = (slot * base_rows).astype(F32)
    over_at = (n_experts * base_rows - base_rows + over_start * GROUP).astype(F32)
    row = jnp.sum(blocks.astype(F32) * (rank + jnp.where(rank < base_rows, base_at, over_at)), axis=2)
    last_row = n_experts * base_rows + OVER_GROUPS * GROUP - 1
    return groups, jnp.minimum(row, last_row).reshape(tok_count).astype(I32)


def permute_kernel(pos_ref, x_ref, gy_ref, *refs):
    *tail, out_ref = refs
    d_model = x_ref.shape[1]
    rows = out_ref.shape[0] - sum(t.shape[0] for t in tail)
    row_id = step_id() * rows + lax.broadcasted_iota(I32, (rows, x_ref.shape[0]), 0)
    select = jnp.where(row_id == pos_ref[...], 1.0, 0.0).astype(BF16)
    out_ref[:rows, :d_model] = dot(select, x_ref[...]).astype(BF16)
    out_ref[:rows, d_model:] = dot(select, gy_ref[...]).astype(BF16)
    for t in tail:
        out_ref[rows:, :] = t[...]


def permute_rows(pos, x, gy, first_row, n_rows, *tail):
    tok_count, d_model = x.shape
    tile = n_rows if n_rows % PERM_TILE else PERM_TILE
    extra = sum(t.shape[0] for t in tail)
    return pl.pallas_call(
        permute_kernel,
        grid=(n_rows // tile,),
        in_specs=[
            pl.BlockSpec((1, tok_count), origin),
            pl.BlockSpec((tok_count, d_model), origin),
            pl.BlockSpec((tok_count, d_model), origin),
        ] + [pl.BlockSpec(t.shape, origin) for t in tail],
        out_specs=pl.BlockSpec((tile + extra, 2 * d_model), lambda i: (i, 0)),
        out_shape=jax.ShapeDtypeStruct((n_rows + extra, 2 * d_model), BF16),
        cost_estimate=pl.CostEstimate(flops=4 * n_rows * tok_count * d_model, bytes_accessed=16_000_000, transcendentals=0),
        name='permute',
    )((pos - first_row).reshape(1, tok_count), x, gy, *tail)


def unpermute_kernel(pos_ref, base_ref, over_ref, out_ref, dx_ref, out_rows, dx_rows, out_tile, dx_tile):
    step = step_id()
    toks, d_model = out_ref.shape
    base_steps = 2 * CHUNKS
    block = base_ref.shape[0] * base_ref.shape[1]
    lanes = 128
    parts = d_model // lanes

    def spread(ref, first):
        n = ref.shape[0]
        size = max(k for k in range(GROUP, 65, GROUP) if n % k == 0)

        @pl.loop(0, n // size)
        def _(i):
            at = pl.multiple_of(i * size, 8)
            rows = ref[pl.ds(at, size), :].astype(F32)
            for c in range(parts):
                to = pl.ds((first + at) * 8 + c, size, stride=8)
                out_rows[to, :] = rows[:, c * lanes:(c + 1) * lanes]
                dx_rows[to, :] = rows[:, d_model + c * lanes:d_model + (c + 1) * lanes]

    @pl.when(step < base_steps)
    def _():
        for d in range(base_ref.shape[0]):
            spread(base_ref.at[d], step * block + d * base_ref.shape[1])

    @pl.when(step == base_steps)
    def _():
        spread(over_ref, base_steps * block)

    @pl.when(step > base_steps)
    def _():
        first = (step - base_steps - 1) * toks

        @pl.loop(0, toks // 16)
        def _(i):
            rows = [pl.multiple_of(pos_ref[first + i * 16 + u] * 8, 8) for u in range(16)]
            outs = [out_rows[pl.ds(r, 8), :] for r in rows]
            dxs = [dx_rows[pl.ds(r, 8), :] for r in rows]
            for u in range(16):
                to = pl.ds(pl.multiple_of((i * 16 + u) * 8, 8), 8)
                out_tile[to, :] = outs[u]
                dx_tile[to, :] = dxs[u]

        for c in range(parts):
            cols = slice(c * lanes, (c + 1) * lanes)
            out_ref[:, cols] = out_tile[pl.ds(c, toks, stride=8), :].astype(BF16)
            dx_ref[:, cols] = dx_tile[pl.ds(c, toks, stride=8), :].astype(BF16)


def unpermute_rows(pos, base, over):
    n_own, n_slot, width = base.shape
    tok_count = pos.shape[0]
    d_model = width // 2
    shape = jax.ShapeDtypeStruct((tok_count, d_model), BF16)
    base_steps = 2 * CHUNKS
    n_rows = n_own * n_slot + over.shape[0]
    token_tile = lambda i, pos: (jnp.maximum(i - base_steps - 1, 0), 0)
    part = lambda i: jnp.minimum(i, base_steps - 1)
    return pl.pallas_call(
        unpermute_kernel,
        grid_spec=pltpu.PrefetchScalarGridSpec(
            num_scalar_prefetch=1,
            grid=(base_steps + 1 + tok_count // TOKEN_TILE,),
            in_specs=[
                pl.BlockSpec((n_own // 2, n_slot // CHUNKS, width), lambda i, pos: (part(i) % 2, part(i) // 2, 0)),
                pl.BlockSpec(over.shape, origin),
            ],
            out_specs=[pl.BlockSpec((TOKEN_TILE, d_model), token_tile)] * 2,
            scratch_shapes=[pltpu.VMEM((n_rows * 8, 128), F32)] * 2 + [pltpu.VMEM((TOKEN_TILE * 8, 128), F32)] * 2,
        ),
        out_shape=[shape, shape],
        compiler_params=pltpu.CompilerParams(dimension_semantics=('arbitrary',)),
        cost_estimate=pl.CostEstimate(flops=10_000_000_000, bytes_accessed=16_000_000, transcendentals=0),
        name='unpermute',
    )(pos, base, over)


def gate(x, wg, expert):
    logit = dot(x, wg)
    unnorm = jnp.exp(logit - jnp.max(logit, axis=1, keepdims=True))
    prob = unnorm / jnp.sum(unnorm, axis=1, keepdims=True)
    onehot = lax.broadcasted_iota(I32, prob.shape, 1) == expert
    gate_val = prob.shape[1] * jnp.sum(jnp.where(onehot, prob, 0.0), axis=1, keepdims=True)
    return prob, onehot, gate_val


def activations(x, dy, w_up, w_down, cols):
    a = dot(x, w_up[:, cols])
    dh = dot(dy, w_down[cols, :], BY_COLS)
    cubic = (SQRT_2_PI * CUBIC) * (a * a)
    half = 0.5 + 0.5 * jnp.tanh(a * (SQRT_2_PI + cubic))
    h = a * half
    slope = half + (h - h * half) * (2.0 * SQRT_2_PI + 6.0 * cubic)
    return h.astype(BF16), (slope * dh).astype(BF16)


def own_rows_step(x, gy, expert, wg_ref, w_up, w_down, store, dwg_ref):
    dy_ref, h_ref, da_ref = store
    prob, onehot, gate_val = gate(x, wg_ref[...], expert)
    gy_full = gy.astype(F32)
    dy = (gate_val * gy_full).astype(BF16)
    dy_ref[...] = dy
    for lo in range(0, h_ref.shape[1], ROW_CHUNK):
        cols = pl.ds(lo, ROW_CHUNK)
        h, da = activations(x, dy, w_up, w_down, cols)
        h_ref[:, cols] = h
        da_ref[:, cols] = da
    y = dot(h_ref[...], w_down[...]).astype(BF16).astype(F32)
    dxe = dot(da_ref[...], w_up[...], BY_COLS).astype(BF16).astype(F32)
    d_gate = jnp.sum(gy_full * y, axis=1, keepdims=True)
    d_logit = ((d_gate * gate_val) * (onehot.astype(F32) - prob)).astype(BF16)
    dwg_ref[...] += dot(d_logit, x, BY_ROWS)
    out = (gate_val * y).astype(BF16)
    dx = (dxe + dot(d_logit, wg_ref[...], BY_COLS)).astype(BF16)
    return out, dx


def own_base_kernel(first_ref, rows_ref, wg_ref, up_ref, down_ref, dwg_in, *refs):
    od_ref, x_ref, dy_ref, h_ref, da_ref, dwg_ref, zero_ref = refs[-7:]
    step = step_id()
    d_model = wg_ref.shape[0]

    @pl.when(step == 0)
    def _():
        dwg_ref[...] = dwg_in[...]

    zero_ref[...] = jnp.zeros_like(zero_ref)
    rows = rows_ref[...].reshape(dy_ref.shape[0], 2 * d_model)
    x = rows[:, :d_model]
    x_ref[...] = x
    out, dx = own_rows_step(x, rows[:, d_model:], first_ref[0] + step, wg_ref, up_ref.at[0], down_ref.at[0],
                            (dy_ref, h_ref, da_ref), dwg_ref)
    block = od_ref.shape[:3] + (d_model,)
    od_ref[:, :, :, :d_model] = out.reshape(block)
    od_ref[:, :, :, d_model:] = dx.reshape(block)


def own_base_pass(first_expert, chunk, rows, wg, w_up, w_down, dwg, stores, over_shape):
    n_src, count, seg, width = rows.shape
    local, d_model, d_ff = w_up.shape
    tile = n_src * seg
    lead = chunk * count
    row_spec = lambda at: pl.BlockSpec((n_src, 1, seg, width), lambda e, first: (0, at + e, 0, 0))
    store_spec = lambda cols: pl.BlockSpec((tile, cols), lambda e, first: (lead + e, 0))
    rows_of = lambda cols: jax.ShapeDtypeStruct((local * tile, cols), BF16)
    zero_block = (over_shape[0] // local,) + over_shape[1:]
    kept = [] if stores is None else list(stores)
    return pl.pallas_call(
        own_base_kernel,
        grid_spec=pltpu.PrefetchScalarGridSpec(
            num_scalar_prefetch=1,
            grid=(count,),
            in_specs=[
                row_spec(0),
                pl.BlockSpec(wg.shape, origin),
                pl.BlockSpec((1, d_model, d_ff), lambda e, first: (lead + e, 0, 0)),
                pl.BlockSpec((1, d_ff, d_model), lambda e, first: (lead + e, 0, 0)),
                pl.BlockSpec(dwg.shape, origin),
            ] + [pl.BlockSpec(memory_space=pl.ANY)] * len(kept),
            out_specs=[row_spec(lead), store_spec(d_model), store_spec(d_model), store_spec(d_ff), store_spec(d_ff),
                       pl.BlockSpec(dwg.shape, origin), pl.BlockSpec(zero_block, lambda e, first: (lead + e, 0, 0))],
        ),
        out_shape=[jax.ShapeDtypeStruct((n_src, local, seg, width), BF16), rows_of(d_model), rows_of(d_model), rows_of(d_ff), rows_of(d_ff),
                   jax.ShapeDtypeStruct(dwg.shape, F32), jax.ShapeDtypeStruct(over_shape, BF16)],
        input_output_aliases={6 + i: o for i, o in zip(range(len(kept)), (0, 1, 2, 3, 4, 6))},
        compiler_params=pltpu.CompilerParams(vmem_limit_bytes=VMEM_BYTES, dimension_semantics=('arbitrary',)),
        cost_estimate=pl.CostEstimate(flops=8_500_000_000 * count, bytes_accessed=20_000_000 * count,
                                      transcendentals=1_500_000 * count),
        name='own_base',
    )(first_expert + lead, rows, wg, w_up, w_down, dwg, *kept)


def run_copies(runs_ref, tile, n_runs, hbm, buf, sem, to_hbm):
    def body(r, carry):
        at = (tile * RUNS + r) * 3
        first, left, slot = (runs_ref[at + k] for k in range(3))
        for size in RUN_SIZES:
            take = left >= size

            @pl.when(take)
            def _(first=first, slot=slot, size=size):
                ends = (hbm.at[pl.ds(first, size)], buf.at[pl.ds(slot, size)])
                pltpu.make_async_copy(*(ends[::-1] if to_hbm else ends), sem).start()

            step = jnp.where(take, size, 0)
            first, slot, left = first + step, slot + step, left - step
        return carry

    lax.fori_loop(0, n_runs, body, 0)


def run_waits(count, hbm, buf, sem, to_hbm):
    for size in RUN_SIZES:
        @pl.when((count & size) != 0)
        def _(size=size):
            ends = (hbm.at[pl.ds(0, size)], buf.at[pl.ds(0, size)])
            pltpu.make_async_copy(*(ends[::-1] if to_hbm else ends), sem).wait()


def tile_rows(buf, count):
    rows = buf[...].reshape(TILE, buf.shape[-1])
    row_id = lax.broadcasted_iota(I32, rows.shape, 0)
    return jnp.where(row_id < count * GROUP, rows, jnp.zeros((), rows.dtype))


def own_over_kernel(tab_ref, runs_ref, first_ref, rows_hbm, wg_ref, up_ref, down_ref, dwg_in, zero_od,
                    od_hbm, x_ref, dy_ref, h_ref, da_ref, dwg_ref, in_buf, out_buf, in_sem, out_sem):
    del zero_od
    step = step_id()
    d_model = wg_ref.shape[0]
    slot = step % 2
    count = tab_ref[COUNT, step]

    @pl.when(step == 0)
    def _():
        dwg_ref[...] = dwg_in[...]
        run_copies(runs_ref, 0, tab_ref[N_RUNS, 0], rows_hbm, in_buf.at[0], in_sem.at[0], False)

    @pl.when(count > 0)
    def _():
        run_waits(count, rows_hbm, in_buf.at[slot], in_sem.at[slot], False)

        @pl.when(step + 1 < step_count())
        def _():
            run_copies(runs_ref, step + 1, tab_ref[N_RUNS, step + 1], rows_hbm, in_buf.at[1 - slot], in_sem.at[1 - slot], False)

        rows = tile_rows(in_buf.at[slot], count)
        x = rows[:, :d_model]
        x_ref[...] = x
        out, dx = own_rows_step(x, rows[:, d_model:], first_ref[0] + tab_ref[EXPERT, step], wg_ref,
                                up_ref.at[0], down_ref.at[0], (dy_ref, h_ref, da_ref), dwg_ref)

        @pl.when(step > 0)
        def _():
            run_waits(tab_ref[COUNT, step - 1], od_hbm, out_buf, out_sem, True)

        out_buf[:, :, :d_model] = out.reshape(TILE_GROUPS, GROUP, d_model)
        out_buf[:, :, d_model:] = dx.reshape(TILE_GROUPS, GROUP, d_model)
        run_copies(runs_ref, step, tab_ref[N_RUNS, step], od_hbm, out_buf, out_sem, True)

        @pl.when(tab_ref[LAST, step] == 1)
        def _():
            run_waits(count, od_hbm, out_buf, out_sem, True)


def own_over_pass(table, runs, first_expert, rows, wg, w_up, w_down, dwg, zero_od):
    d_model, d_ff = w_up.shape[1], w_up.shape[2]
    width = rows.shape[-1]
    n_tiles = table.shape[1]
    hbm = pl.BlockSpec(memory_space=pl.ANY)
    store_spec = lambda cols: pl.BlockSpec((TILE, cols), lambda i, tab, runs, first: (tab[STORE, i], 0))
    rows_of = lambda cols: jax.ShapeDtypeStruct((n_tiles * TILE, cols), BF16)
    return pl.pallas_call(
        own_over_kernel,
        grid_spec=pltpu.PrefetchScalarGridSpec(
            num_scalar_prefetch=3,
            grid=(n_tiles,),
            in_specs=[
                hbm,
                pl.BlockSpec(wg.shape, origin),
                pl.BlockSpec((1, d_model, d_ff), lambda i, tab, runs, first: (tab[EXPERT, i], 0, 0)),
                pl.BlockSpec((1, d_ff, d_model), lambda i, tab, runs, first: (tab[EXPERT, i], 0, 0)),
                pl.BlockSpec(dwg.shape, origin),
                hbm,
            ],
            out_specs=[hbm, store_spec(d_model), store_spec(d_model), store_spec(d_ff), store_spec(d_ff),
                       pl.BlockSpec(dwg.shape, origin)],
            scratch_shapes=[
                pltpu.VMEM((2, TILE_GROUPS, GROUP, width), BF16),
                pltpu.VMEM((TILE_GROUPS, GROUP, width), BF16),
                pltpu.SemaphoreType.DMA((2,)),
                pltpu.SemaphoreType.DMA,
            ],
        ),
        out_shape=[jax.ShapeDtypeStruct(zero_od.shape, BF16), rows_of(d_model), rows_of(d_model), rows_of(d_ff),
                   rows_of(d_ff), jax.ShapeDtypeStruct(dwg.shape, F32)],
        input_output_aliases={8: 0},
        compiler_params=pltpu.CompilerParams(vmem_limit_bytes=VMEM_BYTES, dimension_semantics=('arbitrary',)),
        cost_estimate=pl.CostEstimate(flops=10_000_000_000, bytes_accessed=40_000_000, transcendentals=2_000_000),
        name='own_over',
    )(table, runs, first_expert, rows, wg, w_up, w_down, dwg, zero_od)


OWN_BASE, OWN_OVER, OTHER_BASE, OTHER_OVER = range(4)


def grad_kernel(tab_ref, runs_ref, first_ref, xb_ref, dyb_ref, hb_ref, dab_ref, xo_ref, dyo_ref, ho_ref, dao_ref, *refs):
    *base_hbm, over_hbm, wg_ref, up_hbm, down_hbm, dup_hbm, ddown_hbm = refs[:-12]
    dup, ddown, up_buf, down_buf, h_buf, da_buf, base_buf, in_buf, w_sems, base_sem, in_sem, out_sems = refs[-12:]
    step = step_id()
    d_model, d_ff = dup.shape
    expert, kind, last, _, count = (tab_ref[row, step] for row in range(5))
    n_local = dup_hbm.shape[0]
    base_rows = h_buf.shape[0]

    def weights(e):
        return (pltpu.make_async_copy(up_hbm.at[e], up_buf, w_sems.at[0]),
                pltpu.make_async_copy(down_hbm.at[e], down_buf, w_sems.at[1]))

    def flush_down(e):
        return pltpu.make_async_copy(ddown, ddown_hbm.at[e], out_sems.at[0])

    def flush_up(e):
        return pltpu.make_async_copy(dup, dup_hbm.at[e], out_sems.at[1])

    def add_down(dy, h_src, add):
        for lo in range(0, d_ff, CHUNK):
            cols = pl.ds(lo, CHUNK)
            term = dot(h_src[:, cols], dy, BY_ROWS)
            ddown[cols, :] = ddown[cols, :] + term if add else term

    def add_up(x, da_src, add):
        for lo in range(0, d_ff, CHUNK):
            cols = pl.ds(lo, CHUNK)
            term = dot(x, da_src[:, cols], BY_ROWS)
            dup[:, cols] = dup[:, cols] + term if add else term

    def accumulate(x, dy, h_src, da_src):
        add_down(dy, h_src, True)

        @pl.when(last == 1)
        def _():
            flush_down(expert).start()

        add_up(x, da_src, True)

        @pl.when(last == 1)
        def _():
            flush_up(expert).start()

            @pl.when(expert + 1 < n_local)
            def _():
                for copy in weights(expert + 1):
                    copy.start()

            @pl.when(expert + 1 == n_local)
            def _():
                flush_down(expert).wait()
                flush_up(expert).wait()

    def base_copy(e):
        chunk = base_hbm[e // base_hbm[0].shape[1]]
        return pltpu.make_async_copy(chunk.at[:, e % chunk.shape[1]], base_buf, base_sem)

    ahead = step + 1
    ahead_at = jnp.minimum(ahead, step_count() - 1)

    @pl.when((ahead < step_count()) & (tab_ref[1, ahead_at] == OTHER_OVER))
    def _():
        run_copies(runs_ref, tab_ref[5, ahead_at], tab_ref[7, ahead_at], over_hbm, in_buf.at[ahead % 2], in_sem.at[ahead % 2],
                   False)

    @pl.when(kind == OWN_BASE)
    def _():
        for e in range(n_local):
            @pl.when(expert == e)
            def _():
                base_copy(e).start()

        @pl.when(expert == 0)
        def _():
            for copy in weights(0):
                copy.start()

        @pl.when(expert > 0)
        def _():
            flush_down(expert - 1).wait()

        add_down(dyb_ref[...], hb_ref, False)

        @pl.when(expert > 0)
        def _():
            flush_up(expert - 1).wait()

        add_up(xb_ref[...], dab_ref, False)

    @pl.when(kind == OWN_OVER)
    def _():
        add_down(dyo_ref[...], ho_ref, True)
        add_up(xo_ref[...], dao_ref, True)

    def other_rows(rows, n_rows):
        x, gy = rows[:, :d_model], rows[:, d_model:]
        _, _, gate_val = gate(x, wg_ref[...], first_ref[0] + expert)
        dy = (gate_val * gy.astype(F32)).astype(BF16)
        h_dst, da_dst = h_buf.at[:n_rows], da_buf.at[:n_rows]
        for lo in range(0, d_ff, ROW_CHUNK):
            cols = pl.ds(lo, ROW_CHUNK)
            h, da = activations(x, dy, up_buf, down_buf, cols)
            h_dst[:, cols] = h
            da_dst[:, cols] = da
        accumulate(x, dy, h_dst, da_dst)

    @pl.when(kind == OTHER_BASE)
    def _():
        for copy in weights(expert):
            copy.wait()
        base_copy(0).wait()
        other_rows(base_buf[...].reshape(base_rows, 2 * d_model), base_rows)

    @pl.when(kind == OTHER_OVER)
    def _():
        run_waits(count, over_hbm, in_buf.at[step % 2], in_sem.at[step % 2], False)
        other_rows(tile_rows(in_buf.at[step % 2], count), TILE)


def grad_pass(table, ids, first_expert, base_store, over_store, base, over, wg, w_up, w_down):
    n_src, _, seg, width = base[0].shape
    d_model, d_ff = w_up.shape[1], w_up.shape[2]
    base_rows = n_src * seg
    base_spec = lambda cols: pl.BlockSpec((base_rows, cols), lambda i, tab, ids, first: (tab[6, i], 0))
    over_spec = lambda cols: pl.BlockSpec((TILE, cols), lambda i, tab, ids, first: (tab[3, i], 0))
    hbm = pl.BlockSpec(memory_space=pl.ANY)
    return pl.pallas_call(
        grad_kernel,
        grid_spec=pltpu.PrefetchScalarGridSpec(
            num_scalar_prefetch=3,
            grid=(table.shape[1],),
            in_specs=[
                base_spec(d_model),
                base_spec(d_model),
                base_spec(d_ff),
                base_spec(d_ff),
                over_spec(d_model),
                over_spec(d_model),
                over_spec(d_ff),
                over_spec(d_ff),
                *[hbm for _ in base],
                hbm,
                pl.BlockSpec(wg.shape, origin),
                hbm,
                hbm,
            ],
            out_specs=[hbm, hbm],
            scratch_shapes=[
                pltpu.VMEM((d_model, d_ff), F32),
                pltpu.VMEM((d_ff, d_model), F32),
                pltpu.VMEM((d_model, d_ff), BF16),
                pltpu.VMEM((d_ff, d_model), BF16),
                pltpu.VMEM((base_rows, d_ff), BF16),
                pltpu.VMEM((base_rows, d_ff), BF16),
                pltpu.VMEM((n_src, seg, width), BF16),
                pltpu.VMEM((2, TILE_GROUPS, GROUP, width), BF16),
                pltpu.SemaphoreType.DMA((2,)),
                pltpu.SemaphoreType.DMA,
                pltpu.SemaphoreType.DMA((2,)),
                pltpu.SemaphoreType.DMA((2,)),
            ],
        ),
        out_shape=[jax.ShapeDtypeStruct(w_up.shape, F32), jax.ShapeDtypeStruct(w_down.shape, F32)],
        compiler_params=pltpu.CompilerParams(vmem_limit_bytes=VMEM_BYTES, dimension_semantics=('arbitrary',)),
        cost_estimate=pl.CostEstimate(flops=70_000_000_000, bytes_accessed=150_000_000, transcendentals=8_000_000),
        name='grad_pass',
    )(table, ids, first_expert, *base_store, *over_store, *base, over, wg, w_up, w_down)


def overflow_spans(count_ref, local):
    groups = jnp.sum(count_ref[...].astype(F32), axis=(1, 2))
    over = jnp.maximum(groups - BASE_GROUPS, 0.0)
    lanes = over.shape[1]
    row, col = (lax.broadcasted_iota(I32, (lanes, lanes), d) for d in (0, 1))
    start = dot(over.astype(BF16), jnp.where(row < col, 1.0, 0.0).astype(BF16))
    tiles = jnp.ceil(jnp.sum(over, axis=0, keepdims=True) * (1.0 / TILE_GROUPS) - 1e-3)
    owner = dot(jnp.broadcast_to(tiles, over.shape).astype(BF16), jnp.where(row // local == col, 1.0, 0.0).astype(BF16))
    excess = jnp.max(jnp.maximum(start + over - OVER_GROUPS, owner - MAX_OVER_TILES))
    first = jnp.minimum(start, OVER_GROUPS)
    size = jnp.minimum(start + over, OVER_GROUPS) - first
    return size.astype(I32), first.astype(I32), excess


def fill_tiles(n_src, local, lead, size, first, runs, n_runs, count):
    for t in range(MAX_OVER_TILES):
        n_runs[t] = 0
        count[t] = 0

    def put(tile, slot, begin, groups):
        @pl.when((groups > 0) & (tile < MAX_OVER_TILES))
        def _():
            at = (tile * RUNS + n_runs[tile]) * 3
            for k, value in enumerate((begin, groups, slot)):
                runs[at + k] = value
            n_runs[tile] = n_runs[tile] + 1
            count[tile] = count[tile] + groups

    spans, tile = [], jnp.int32(0)
    for e in range(local):
        def per_source(s, where, e=e):
            tile, slot = where
            groups = size[s, lead + e]
            begin = s * SENT_GROUPS + first[s, lead + e]
            head = jnp.minimum(groups, TILE_GROUPS - slot)
            rest = groups - head
            put(tile, slot, begin, head)
            put(tile + 1, 0, begin + head, rest)
            full = (slot + head == TILE_GROUPS).astype(I32)
            return tile + full, jnp.where(full == 1, rest, slot + head)

        end, slot = lax.fori_loop(0, n_src, per_source, (tile, jnp.int32(0)))
        end = jnp.minimum(end + (slot > 0).astype(I32), MAX_OVER_TILES)
        spans.append((tile, end - tile))
        tile = end
    return spans, tile


def to_scalars(pairs, sems):
    copies = [pltpu.make_async_copy(v, m, sems.at[i]) for i, (v, m) in enumerate(pairs)]
    for copy in copies:
        copy.start()
    for copy in copies:
        copy.wait()


def own_plan_kernel(local, lead_ref, count_ref, tab_ref, runs_ref, span_ref, size_v, first_v, size_s, first_s, n_runs, count,
                    sems):
    size_v[0], first_v[0], excess = overflow_spans(count_ref, local)
    to_scalars([(size_v, size_s), (first_v, first_s)], sems)
    spans, n_tiles = fill_tiles(count_ref.shape[0], local, lead_ref[0], size_s.at[0], first_s.at[0], runs_ref, n_runs.at[0],
                                count.at[0])
    for e, (tile, tiles) in enumerate(spans):
        span_ref[e] = tile
        span_ref[local + e] = tiles
    span_ref[2 * local] = (excess <= 0.0).astype(I32)
    last = jnp.maximum(n_tiles - 1, 0)
    for t in range(MAX_OVER_TILES):
        row = (local - 1, count[0, t], jnp.minimum(t, last), (last == t).astype(I32), n_runs[0, t])
        for k, value in enumerate(row):
            tab_ref[k, t] = value
    for e, (tile, tiles) in enumerate(spans):
        def body(k, c, e=e, tile=tile):
            tab_ref[EXPERT, tile + k] = e
            return c

        lax.fori_loop(0, tiles, body, 0)


def grad_plan_kernel(local, lead_ref, span_ref, other_ref, tab_ref, runs_ref, fits_ref, size_v, first_v, size_s, first_s,
                     n_runs, count, sems):
    n_src = other_ref.shape[0]
    size_v[0], first_v[0], excess = overflow_spans(other_ref, local)
    to_scalars([(size_v, size_s), (first_v, first_s)], sems)
    fits_ref[0] = span_ref[2 * local] * (excess <= 0.0).astype(I32)
    lead = lead_ref[0]
    own = [(span_ref[e], span_ref[local + e]) for e in range(local)]
    n_tiles = own[-1][0] + own[-1][1]
    other, _ = fill_tiles(n_src, local, lead, size_s.at[0], first_s.at[0], runs_ref, n_runs.at[0], count.at[0])
    max_steps = tab_ref.shape[1]

    def emit(step, expert, kind, own_tile, other_tile, next_base):
        over = int(kind == OTHER_OVER)
        row = (expert, kind, 0, jnp.clip(own_tile, 0, MAX_OVER_TILES - 1), count[0, other_tile] * over, other_tile, next_base,
               n_runs[0, other_tile] * over)
        for k, value in enumerate(row):
            tab_ref[k, step] = value

    step = jnp.int32(0)
    for e in range(local):
        own_tile, own_tiles = own[e]
        other_tile, other_tiles = other[e]
        after = min(e + 1, local - 1)
        emit(step, e, OWN_BASE, own_tile, 0, e)

        def own_body(k, c, e=e, step=step, own_tile=own_tile, after=after):
            emit(step + 1 + k, e, OWN_OVER, own_tile + k, 0, after)
            return c

        lax.fori_loop(0, own_tiles, own_body, 0)
        step = step + 1 + own_tiles
        own_at = own_tile + own_tiles
        emit(step, e, OTHER_BASE, own_at, 0, after)

        def other_body(k, c, e=e, step=step, own_at=own_at, other_tile=other_tile, after=after):
            emit(step + 1 + k, e, OTHER_OVER, own_at, other_tile + k, after)
            return c

        lax.fori_loop(0, other_tiles, other_body, 0)
        step = step + 1 + other_tiles
        tab_ref[2, step - 1] = 1

    def dead(t, c):
        emit(t, local - 1, -1, n_tiles - 1, 0, local - 1)
        return c

    lax.fori_loop(step, max_steps, dead, 0)


def plan_call(kernel, local, scalars, counts, out_shapes):
    n_src = counts.shape[0]
    smem = pl.BlockSpec(memory_space=pltpu.SMEM)
    shape = (1, n_src, 128)
    return pl.pallas_call(
        functools.partial(kernel, local),
        grid=(1,),
        in_specs=[smem] * len(scalars) + [pl.BlockSpec((n_src, 1, GROUP, 128), lambda i: (0, OVER_GROUPS, 0, 0))],
        out_specs=[smem] * len(out_shapes),
        out_shape=[jax.ShapeDtypeStruct(o, I32) for o in out_shapes],
        scratch_shapes=[pltpu.VMEM(shape, I32)] * 2 + [pltpu.SMEM(shape, I32)] * 2
        + [pltpu.SMEM((1, MAX_OVER_TILES), I32)] * 2 + [pltpu.SemaphoreType.DMA((2,))],
    )(*scalars, counts)


def padded_step(x_loc, gy_loc, idx_loc, w_gate, w_up, w_down, ep_size, dp_size):
    tok_count, d_model = x_loc.shape
    n_experts = w_gate.shape[1]
    local_experts = w_up.shape[0]
    cap_rows = PAD_FACTOR * tok_count // n_experts
    onehot = idx_loc[:, None] == jnp.arange(n_experts, dtype=I32)[None, :]
    expert_count = jnp.sum(onehot, axis=0, dtype=I32)
    sort_order = jnp.argsort(idx_loc, stable=True)
    sorted_pos = jnp.argsort(sort_order)
    expert_start = jnp.cumsum(expert_count) - expert_count
    slot_k = jnp.arange(cap_rows, dtype=I32)
    slot_valid = slot_k[None, :] < expert_count[:, None]
    src_tok = sort_order[jnp.minimum(expert_start[:, None] + slot_k[None, :], tok_count - 1)]
    slot_tok = idx_loc * cap_rows + sorted_pos - expert_start[idx_loc]

    def dispatch(tok_rows):
        picked = jnp.where(slot_valid[:, :, None], tok_rows[src_tok], jnp.zeros((), tok_rows.dtype))
        picked = picked.reshape(ep_size, local_experts, cap_rows, d_model)
        return lax.all_to_all(picked, 'ep', 0, 0, tiled=True)

    def combine(expert_rows):
        returned = lax.all_to_all(expert_rows, 'ep', 1, 0, tiled=True)
        return returned.reshape(n_experts * cap_rows, d_model)[slot_tok]

    router_logit = jnp.dot(x_loc, w_gate, preferred_element_type=F32)
    router_prob = jax.nn.softmax(router_logit, axis=-1)
    gate_val = n_experts * jnp.sum(jnp.where(onehot, router_prob, 0.0), axis=1)
    recv_rows = dispatch(x_loc)
    gy_full = gy_loc.astype(F32)
    dy_tok = (gate_val[:, None] * gy_full).astype(BF16)
    recv_grad = dispatch(dy_tok)

    def one_expert(carry, per_expert):
        rows, grad, up, down = per_expert
        rows, grad = rows.reshape(-1, d_model), grad.reshape(-1, d_model)
        pre_act = dot(rows, up)
        hid_full, gelu_back = jax.vjp(jax.nn.gelu, pre_act)
        hidden = hid_full.astype(BF16)
        out_rows = dot(hidden, down).astype(BF16)
        d_pre = gelu_back(dot(grad, down, BY_COLS))[0].astype(BF16)
        grad_down = dot(hidden, grad, BY_ROWS)
        grad_up = dot(rows, d_pre, BY_ROWS)
        d_rows = dot(d_pre, up, BY_COLS).astype(BF16)
        shape = (ep_size, cap_rows, d_model)
        return carry, (out_rows.reshape(shape), d_rows.reshape(shape), grad_up, grad_down)

    swap = lambda rows: jnp.swapaxes(rows, 0, 1)
    _, (expert_out, d_rows, grad_up, grad_down) = lax.scan(
        one_expert, 0, (swap(recv_rows), swap(recv_grad), w_up, w_down))
    y_tok = combine(expert_out)
    moe_out = (gate_val[:, None] * y_tok.astype(F32)).astype(BF16)
    dx_expert = combine(d_rows)
    d_gate = jnp.sum(gy_full * y_tok.astype(F32), axis=1)
    d_logit = ((d_gate * gate_val)[:, None] * (onehot.astype(F32) - router_prob)).astype(BF16)
    dx_router = dot(d_logit, w_gate, BY_COLS)
    grad_x = (dx_expert.astype(F32) + dx_router).astype(BF16)
    grad_gate = dot(x_loc, d_logit, BY_ROWS)

    def sum_dp(term):
        total = term
        for shift in range(1, dp_size):
            total = total + lax.ppermute(term, 'dp', [(i, (i + shift) % dp_size) for i in range(dp_size)])
        return total

    grad_gate = jnp.sum(lax.all_gather(grad_gate, ('dp', 'ep')), axis=0)
    return moe_out, grad_x, sum_dp(grad_up), sum_dp(grad_down), grad_gate


def solution(mesh):
    dp_size, ep_size = mesh.shape['dp'], mesh.shape['ep']
    tok_spec = P(('dp', 'ep'), None)
    idx_spec = P(('dp', 'ep'))
    rep_spec = P(None, None)
    exp_spec = P('ep', None, None)
    swap = [(i, (i + 1) % dp_size) for i in range(dp_size)]

    def local_step(x, gy, idx, w_gate, w_up, w_down):
        _, d_model = x.shape
        n_experts = w_gate.shape[1]
        local = w_up.shape[0]
        width = 2 * d_model
        base_rows = BASE_GROUPS * GROUP
        n_base = n_experts * base_rows
        n_over = OVER_GROUPS * GROUP
        ep = lax.axis_index('ep')
        first_expert = (ep * local).astype(I32).reshape(1)

        my_groups, pos = token_positions(idx, n_experts, local)
        chunk_rows = n_base // CHUNKS
        slots = (ep_size, local // CHUNKS, base_rows, width)
        base, base_z = [], []
        for c in range(CHUNKS):
            sent = permute_rows(pos, x, gy, c * chunk_rows, chunk_rows)
            base.append(lax.all_to_all(sent.reshape(ep_size, -1, width), 'ep', 0, 0, tiled=True))
            base_z.append(lax.ppermute(base[c], 'dp', swap).reshape(slots))
        marks = jnp.pad(my_groups.astype(BF16)[None, :], ((0, GROUP - 1), (0, width - n_experts)))
        over_sent = permute_rows(pos, x, gy, n_base, n_over, marks).reshape(SENT_GROUPS, GROUP, width)
        over = lax.all_gather(over_sent, 'ep')
        over_sent_z = lax.ppermute(over_sent, 'dp', swap)
        over_z = lax.all_gather(over_sent_z, 'ep')

        n_runs = MAX_OVER_TILES * RUNS * 3
        table, runs, spans = plan_call(own_plan_kernel, local, [first_expert], over,
                                       [(5, MAX_OVER_TILES), (n_runs,), (2 * local + 1,)])
        gtable, runs_z, fits = plan_call(grad_plan_kernel, local, [first_expert, spans], over_z,
                                         [(8, 2 * (local + MAX_OVER_TILES)), (n_runs,), (1,)])
        over_shape = (ep_size * SENT_GROUPS, GROUP, width)
        over = over.reshape(over_shape)
        over_z = over_z.reshape(over_shape)
        dwg = jnp.zeros((n_experts, d_model), F32)
        stores = None
        for c in range(CHUNKS):
            kept = own_base_pass(first_expert, c, base[c].reshape(slots), w_gate, w_up, w_down, dwg, stores, over_shape)
            dwg = kept[5]
            stores = kept[:5] + kept[6:]
        od, *base_store, zero_od = stores
        base_back = lax.all_to_all(od.reshape(ep_size, -1, width), 'ep', 0, 0, tiled=True)
        od_over, x_o, dy_o, h_o, da_o, dwg = own_over_pass(table, runs, first_expert, over, w_gate, w_up, w_down,
                                                          dwg, zero_od)
        over_back = lax.psum_scatter(od_over.reshape(ep_size, SENT_GROUPS, GROUP, width), 'ep', scatter_dimension=0)
        d_up, d_down = grad_pass(gtable, runs_z, first_expert, base_store, (x_o, dy_o, h_o, da_o), base_z, over_z,
                                 w_gate, w_up, w_down)
        d_gate = jnp.sum(lax.all_gather(dwg, ('dp', 'ep')), axis=0).T
        moe_out, grad_x = unpermute_rows(pos, base_back, over_back.reshape(-1, width))
        sparse = (moe_out, grad_x, d_up, d_down, d_gate)

        def dense(carry):
            del carry
            return (jnp.array(True),) + padded_step(x, gy, idx, w_gate, w_up, w_down, ep_size, dp_size)

        return lax.while_loop(lambda carry: jnp.logical_not(carry[0]), dense, (fits[0] == 1,) + sparse)[1:]

    return jax.shard_map(
        local_step, mesh=mesh, in_specs=(tok_spec, tok_spec, idx_spec, rep_spec, exp_spec, exp_spec),
        out_specs=(tok_spec, tok_spec, exp_spec, exp_spec, rep_spec), check_vma=False)
```
